256 devices in a mesh: seq: 16 (over z, x_lo), img: 8 (over y, x_hi), fsdp: 2 (over core).
Axes of the slice: x: 4 (x_hi: 2, x_lo: 2; x = x_hi * 2 + x_lo), y: 4, z: 8, core: 2. Of those that a mesh axis runs over, the one named last changes fastest.
Arguments:
- vision_feats: bfloat16 [8, 2304, 1024], P('img', ('seq', 'fsdp')), may hold values from -6 to 6
- ln_gain: float32 [1024], replicated, may hold values from 0.5 to 1.5
- ln_bias: float32 [1024], replicated, may hold values from -3 to 3
- w_in: bfloat16 [1024, 4096], P('fsdp', 'seq'), may hold values from -0.1875 to 0.1875
- b_in: float32 [4096], P('seq'), may hold values from -3 to 3
- w_out: bfloat16 [4096, 4096], P('seq', 'fsdp'), may hold values from -0.09375 to 0.09375
- lm_grad: bfloat16 [8, 4096, 4096], P('img', 'seq', 'fsdp'), may hold values from -0.079589844 to 0.079589844
- image_counts: int32 [8, 2], P('img'), may hold values from 1 to 3, as said below
- token_pos: int32 [8, 2304], P('img'), may hold values from 0 to 2047, as said below
Outputs:
- w_in_grad: float32 [1024, 4096], P(('img', 'fsdp'), 'seq')
- b_in_grad: float32 [4096], replicated
- w_out_grad: float32 [4096, 4096], P(('seq', 'img'), 'fsdp')
- b_out_grad: float32 [4096], replicated
- ln_gain_grad: float32 [1024], replicated
- ln_bias_grad: float32 [1024], replicated
The draws below stay inside these ranges and needn't reach their ends.
Inputs may be any that keep to these rules, and one draw needn't show every extreme that they name: `image_counts`: in each group the 2 samples hold 4 images together, each sample one or more. `token_pos`: each image's 576 tokens take consecutive positions of its sample's sequence in order; a sample's images come in order without intersection, and images are numbered sample by sample as image_counts gives.
All inputs are finite; a program needn't handle non-finite values.
Results may differ from the reference program's by a relative error of at most 0.0047.
Values may be sent and summed in bfloat16 or wider, within the bound.
A program may use at most 128 MiB of HBM per device.

```python
import jax
import jax.numpy as jnp
from jax import lax

D = 4096
DV = 1024
HID = 4096
PATCH = 576
IMGS = 4
LEN = 2048
IMG_ROWS = 2304
POS = 4096
GROUPS = 8


def image_layout(key):
    base_key = jax.random.fold_in(key, 311)
    count_key, place_key = jax.random.split(base_key)
    first_count = 1 + jax.random.randint(count_key, (GROUPS,), 0, 3)
    counts = jnp.stack([first_count, IMGS - first_count], axis=1).astype(jnp.int32)
    text_room = LEN - counts * PATCH
    marks = jax.random.randint(place_key, (GROUPS, 2, 3), 0, 1 + text_room[:, :, None])
    marks = jnp.sort(marks, axis=2).astype(jnp.int32)
    pieces = []
    for image_index in range(IMGS):
        in_second = image_index >= first_count
        sample = in_second.astype(jnp.int32)
        slot_index = jnp.where(in_second, image_index - first_count, image_index).astype(jnp.int32)
        mark_row = jnp.take_along_axis(marks, sample[:, None, None], axis=1)[:, 0, :]
        begin_pos = jnp.take_along_axis(mark_row, slot_index[:, None], axis=1)[:, 0] + slot_index * PATCH
        pieces.append(begin_pos[:, None] + jnp.arange(PATCH, dtype=jnp.int32)[None, :])
    positions = jnp.concatenate(pieces, axis=1).astype(jnp.int32)
    return (counts, positions)


def draw_image_counts(key, part):
    counts, positions = image_layout(key)
    return counts


def draw_token_pos(key, part):
    counts, positions = image_layout(key)
    return positions


def shard_levels(key, shape, cuts, low, top_value):
    def one(position, parts):
        draws = jax.random.uniform(jax.random.fold_in(jax.random.fold_in(key, 6), position), (parts,), jnp.float32, low / len(cuts), top_value / len(cuts))
        return jnp.repeat(jnp.exp(draws), shape[position] // parts).reshape((-1,) + (1,) * (len(shape) - position - 1))

    loudness = one(*cuts[0])
    for cut in cuts[1:]:
        loudness = loudness * one(*cut)
    return loudness


def normal_values(stream_key, extent, deviation, limit, cuts=(), held_as=jnp.bfloat16):
    entries = jax.random.normal(stream_key, extent, jnp.float32) * deviation
    if len(cuts) > 0:
        entries = shard_levels(stream_key, extent, cuts, -0.22, 0.18) * entries
    return jnp.clip(entries, min=-limit, max=limit).astype(held_as)


def setup_inputs(seed: int = 0) -> dict:
    arg_keys = jax.random.split(jax.random.key(seed), 10)
    return {
        "vision_feats": normal_values(arg_keys[0], (GROUPS, IMG_ROWS, DV), 1.0, 6.0, ((0, 8), (1, 32))),
        "ln_gain": jnp.clip(1.0 + 0.1 * jax.random.normal(arg_keys[1], (DV,), jnp.float32), 0.5, 1.5),
        "ln_bias": normal_values(arg_keys[2], (DV,), 0.5, 3.0, (), jnp.float32),
        "w_in": normal_values(arg_keys[3], (DV, HID), DV ** -0.5, 0.1875, ((0, 2), (1, 16))),
        "b_in": normal_values(arg_keys[4], (HID,), 0.5, 3.0, ((0, 16),), jnp.float32),
        "w_out": normal_values(arg_keys[5], (HID, D), HID ** -0.5, 0.09375, ((0, 16), (1, 2))),
        "lm_grad": normal_values(arg_keys[6], (GROUPS, POS, D), 0.01, 0.079589844, ((0, 8), (1, 16), (2, 2))),
        "image_counts": draw_image_counts(jax.random.fold_in(arg_keys[9], 71), 0),
        "token_pos": draw_token_pos(jax.random.fold_in(arg_keys[9], 71), 0),
    }


def gelu_parts(preact):
    cumul = 0.5 * (1.0 + lax.erf(preact * 0.7071067811865476))
    density = jnp.exp(-0.5 * preact * preact) * 0.3989422804014327
    return (preact * cumul, cumul + preact * density)

def layer_norm(features, ln_gain, ln_bias):
    values = features.astype(jnp.float32)
    row_mean = lax.optimization_barrier(jnp.mean(values, axis=1, keepdims=True))
    centred = values - row_mean
    row_var = lax.optimization_barrier(jnp.mean(centred * centred, axis=1, keepdims=True))
    normed = centred * lax.rsqrt(row_var + 1e-05)
    return (normed, (normed * ln_gain + ln_bias).astype(jnp.bfloat16))

def absolute_positions(counts, positions):
    row_count = positions.shape[0]
    image_index = jnp.arange(row_count, dtype=jnp.int32) // PATCH
    bounds = jnp.cumsum(counts).astype(jnp.int32)
    sample = lax.optimization_barrier(jnp.sum((image_index[:, None] >= bounds[None, :]).astype(jnp.int32), axis=1))
    return (sample * LEN + positions).astype(jnp.int32)

def contract(left, right, left_dim, right_dim):
    return lax.dot_general(left, right, (((left_dim,), (right_dim,)), ((), ())), preferred_element_type=jnp.float32)

def reference(vision_feats, ln_gain, ln_bias, w_in, b_in, w_out, lm_grad, image_counts, token_pos):

    def one_group(totals, inputs):
        features, cotangent, counts, positions = inputs
        normed, normed_in = layer_norm(features, ln_gain, ln_bias)
        preact = jnp.dot(normed_in, w_in, preferred_element_type=jnp.float32) + b_in
        activ, slope = gelu_parts(preact)
        hidden = activ.astype(jnp.bfloat16)
        picked = cotangent[absolute_positions(counts, positions)]
        hidden_grad = contract(picked, w_out, 1, 1)
        preact_grad = (hidden_grad * slope).astype(jnp.bfloat16)
        normed_grad = contract(preact_grad, w_in, 1, 1)
        terms = (contract(normed_in, preact_grad, 0, 0), lax.optimization_barrier(jnp.sum(preact_grad, axis=0, dtype=jnp.float32)), contract(hidden, picked, 0, 0), lax.optimization_barrier(jnp.sum(picked, axis=0, dtype=jnp.float32)), lax.optimization_barrier(jnp.sum(normed_grad * normed, axis=0)), lax.optimization_barrier(jnp.sum(normed_grad, axis=0)))
        return (tuple((left + right for left, right in zip(totals, terms))), None)
    start_state = (jnp.zeros((DV, HID), jnp.float32), jnp.zeros((HID,), jnp.float32), jnp.zeros((HID, D), jnp.float32), jnp.zeros((D,), jnp.float32), jnp.zeros((DV,), jnp.float32), jnp.zeros((DV,), jnp.float32))
    totals, unused = lax.scan(one_group, start_state, (vision_feats, lm_grad, image_counts, token_pos))
    return (totals[0], totals[1], totals[2], totals[3], totals[4], totals[5])
```

```python
import jax
import jax.numpy as jnp
from jax import lax
from jax.experimental import pallas as pl
from jax.experimental.pallas import tpu as pltpu
from jax.sharding import Mesh
from jax.sharding import PartitionSpec as P

PATCH = 576
LEN = 2048
SEQ = ("seq_0", "seq_1")
IMG = ("img_0", "img_1")
SEQ_FSDP = ("seq_0", "seq_1", "fsdp")
IMG_FSDP = ("img_0", "img_1", "fsdp")
SEQ_IMG = ("seq_0", "seq_1", "img_0", "img_1")
MESH = pl.DeviceIdType.MESH
BF16 = jnp.bfloat16
F32 = jnp.float32
VMEM = pl.BlockSpec(memory_space=pltpu.VMEM)
DMA = pltpu.SemaphoreType.DMA
LIMIT = 60 * 1024 * 1024


def remote(src, dst, send, recv, device):
    return pltpu.make_async_remote_copy(
        src_ref=src, dst_ref=dst, send_sem=send, recv_sem=recv, device_id=device, device_id_type=MESH
    )


def greet(devices):
    barrier = pltpu.get_barrier_semaphore()
    for device in devices:
        pl.semaphore_signal(barrier, inc=1, device_id=device, device_id_type=MESH)
    pl.semaphore_wait(barrier, len(devices))


def call(kernel, outs, scratch, number, args, flops):
    return pl.pallas_call(
        kernel,
        out_shape=outs,
        in_specs=[VMEM] * len(args),
        out_specs=jax.tree.map(lambda _: VMEM, outs),
        scratch_shapes=scratch,
        compiler_params=pltpu.CompilerParams(
            collective_id=number, has_side_effects=True, vmem_limit_bytes=LIMIT
        ),
        cost_estimate=pl.CostEstimate(flops=flops, bytes_accessed=1 << 20, transcendentals=0),
    )(*args)


def swap_kernel(lm, out, send, recv):
    other = 1 - lax.axis_index("seq_1")
    neighbour = {"seq_1": other}
    greet([neighbour])
    width = out.shape[1]
    columns = pl.ds(pl.multiple_of(other * width, 128), width)
    copy = remote(lm.at[:, columns], out, send, recv, neighbour)
    copy.start()
    copy.wait()


def swap_columns(lm):
    rows, width = lm.shape
    out = jax.ShapeDtypeStruct((rows, width // 2), lm.dtype)
    return call(swap_kernel, out, [DMA, DMA], 0, (lm,), 1 << 30)


def exchange_kernel(v, wo, wi, bi, vs, wos, wis, bis, up_s, up_r, dn_s, dn_r, x_s, x_r, c_s, c_r, w_s, w_r, local):
    layers = vs.shape[0]
    z, xl, c = lax.axis_index("seq_0"), lax.axis_index("seq_1"), lax.axis_index("fsdp")
    other, peer = 1 - xl, 1 - c
    up, down = {"seq_0": (z + 1) % layers}, {"seq_0": (z + layers - 1) % layers}
    across, twin = {"seq_1": other}, {"fsdp": peer}
    greet([up, down, across, twin])
    width = wos.shape[2]
    mine = pl.ds(pl.multiple_of(xl * width, 128), width)
    theirs = pl.ds(pl.multiple_of(other * width, 128), width)
    started = []

    def go(copy):
        copy.start()
        started.append(copy)
        return copy

    n_up, n_down = layers // 2, layers // 2 - 1
    ups = {0: go(remote(v, vs.at[z, xl, c], up_s.at[0], up_r.at[0], up))}
    downs = {0: go(remote(v, vs.at[z, xl, c], dn_s.at[0], dn_r.at[0], down))}
    xs = [go(remote(v, vs.at[z, xl, c], x_s.at[0], x_r.at[0], across))]
    cs = [go(remote(v, vs.at[z, xl, c], c_s.at[0], c_r.at[0], twin))]
    w_x = [
        go(remote(wi, wis.at[c, xl], w_s.at[0], w_r.at[0], across)),
        go(remote(bi, bis.at[xl], w_s.at[1], w_r.at[1], across)),
        go(remote(wo.at[:, theirs], wos.at[xl], w_s.at[2], w_r.at[2], across)),
    ]
    w_c = [go(remote(wi, wis.at[c, xl], w_s.at[3], w_r.at[3], twin))]
    locals_ = [
        pltpu.make_async_copy(v, vs.at[z, xl, c], local.at[0]),
        pltpu.make_async_copy(wo.at[:, mine], wos.at[xl], local.at[1]),
        pltpu.make_async_copy(wi, wis.at[c, xl], local.at[2]),
        pltpu.make_async_copy(bi, bis.at[xl], local.at[3]),
    ]
    for copy in locals_:
        copy.start()
    blocks = [z]

    def arrived(zb):
        j = len(blocks)
        blocks.append(zb)
        xs.append(go(remote(vs.at[zb, xl, c], vs.at[zb, xl, c], x_s.at[j], x_r.at[j], across)))
        cs.append(go(remote(vs.at[zb, xl, c], vs.at[zb, xl, c], c_s.at[j], c_r.at[j], twin)))

    done = 0

    def pass_on(limit):
        nonlocal done
        while done < limit:
            xs[done].wait_recv()
            zb = blocks[done]
            j = layers + done
            cs.append(go(remote(vs.at[zb, other, c], vs.at[zb, other, c], c_s.at[j], c_r.at[j], twin)))
            done += 1

    for s in range(n_up):
        held = len(blocks)
        ups[s].wait_recv()
        zb = (z + layers - 1 - s) % layers
        if s + 1 < n_up:
            ups[s + 1] = go(remote(vs.at[zb, xl, c], vs.at[zb, xl, c], up_s.at[s + 1], up_r.at[s + 1], up))
        arrived(zb)
        if s < n_down:
            downs[s].wait_recv()
            zb = (z + 1 + s) % layers
            if s + 1 < n_down:
                downs[s + 1] = go(
                    remote(vs.at[zb, xl, c], vs.at[zb, xl, c], dn_s.at[s + 1], dn_r.at[s + 1], down)
                )
            arrived(zb)
        pass_on(held)
    w_x[0].wait_recv()
    w_c.append(go(remote(wis.at[c, other], wis.at[c, other], w_s.at[4], w_r.at[4], twin)))
    pass_on(layers)
    for copy in w_x[1:] + w_c + cs:
        copy.wait_recv()
    for copy in started:
        copy.wait_send()
    for copy in locals_:
        copy.wait()


def exchange(v, wo, wi, bi, layers):
    outs = (
        jax.ShapeDtypeStruct((layers, 2, 2, *v.shape), v.dtype),
        jax.ShapeDtypeStruct((2, wo.shape[0], wo.shape[1] // 2), wo.dtype),
        jax.ShapeDtypeStruct((2, 2, *wi.shape), wi.dtype),
        jax.ShapeDtypeStruct((2, *bi.shape), bi.dtype),
    )
    half = layers // 2
    sems = [half, half, half - 1, half - 1, layers, layers, 2 * layers, 2 * layers, 5, 5, 4]
    return call(exchange_kernel, outs, [DMA((n,)) for n in sems], 1, (v, wo, wi, bi), 1 << 33)


CHUNKS = 3


def middle_kernel(hp, slope, wo, pg, ws, r1, keep, give, r2, ry, c_s, c_r, x_s, x_r, y_s, y_r):
    y, xl, c = lax.axis_index("img_0"), lax.axis_index("seq_1"), lax.axis_index("fsdp")
    other, peer = 1 - xl, 1 - c
    ny = wo.shape[1]
    across, twin = {"seq_1": other}, {"fsdp": peer}
    ys = [{"img_0": (y + k) % ny} for k in range(1, ny)]
    greet([across, twin] + ys)
    rows, width = pg.shape
    step = rows // CHUNKS

    def lanes(a, b):
        return pl.ds(pl.multiple_of((a * 2 + b) * width, 128), width)

    firsts, seconds, thirds = [], [], []
    for k in range(CHUNKS):
        part = pl.ds(k * step, step)
        for p in range(2):
            side = other if p == 0 else xl
            copy = remote(hp.at[part, lanes(side, peer)], r1.at[p, part], c_s.at[p, k], c_r.at[p, k], twin)
            copy.start()
            firsts.append(copy)
    for k in range(1, ny):
        copy = remote(wo.at[:, (y + k) % ny], ry.at[k - 1], y_s.at[k - 1], y_r.at[k - 1], ys[k - 1])
        copy.start()
        thirds.append(copy)
    for k in range(CHUNKS):
        part = pl.ds(k * step, step)
        firsts[2 * k].wait_recv()
        give[part, :] = (hp[part, lanes(other, c)].astype(F32) + r1[0, part, :].astype(F32)).astype(BF16)
        copy = remote(give.at[part], r2.at[part], x_s.at[k], x_r.at[k], across)
        copy.start()
        seconds.append(copy)
        firsts[2 * k + 1].wait_recv()
        keep[part, :] = hp[part, lanes(xl, c)].astype(F32) + r1[1, part, :].astype(F32)
    for k in range(CHUNKS):
        part = pl.ds(k * step, step)
        seconds[k].wait_recv()
        pg[part, :] = ((keep[part, :] + r2[part, :].astype(F32)) * slope[part, :]).astype(BF16)
    total = wo[:, y].astype(F32)
    for k in range(1, ny):
        thirds[k - 1].wait_recv()
        total = total + ry[k - 1].astype(F32)
    ws[...] = total.astype(BF16)
    for copy in firsts + seconds + thirds:
        copy.wait_send()


def middle(hp, slope, wo):
    rows, width = slope.shape
    ny = wo.shape[1]
    outs = (
        jax.ShapeDtypeStruct((rows, width), BF16),
        jax.ShapeDtypeStruct((2, *wo.shape[2:]), BF16),
    )
    scratch = [
        pltpu.VMEM((2, rows, width), BF16),
        pltpu.VMEM((rows, width), F32),
        pltpu.VMEM((rows, width), BF16),
        pltpu.VMEM((rows, width), BF16),
        pltpu.VMEM((ny - 1, 2, *wo.shape[2:]), BF16),
        DMA((2, CHUNKS)),
        DMA((2, CHUNKS)),
        DMA((CHUNKS,)),
        DMA((CHUNKS,)),
        DMA((ny - 1,)),
        DMA((ny - 1,)),
    ]
    return call(middle_kernel, outs, scratch, 2, (hp, slope, wo), 1 << 32)


def last_kernel(
    ws, wi, vec, w_out, w_in, gain, bias, b_out, b_in, rx, ri, v1, t1, v2, t2, v3, x_s, x_r, i_s, i_r, a_s, a_r, b_s, b_r, d_s, d_r
):
    layers, ny = v3.shape[0], wi.shape[0]
    z, xl, c = lax.axis_index("seq_0"), lax.axis_index("seq_1"), lax.axis_index("fsdp")
    y, xh = lax.axis_index("img_0"), lax.axis_index("img_1")

    def flip(me, bit):
        return 1 - me if bit else me

    plane = []
    for dy in range(ny):
        for dx in range(2):
            for dc in range(2):
                if (dy, dx, dc) != (0, 0, 0):
                    plane.append((dy, dx, dc))
    plane_ids = [((y + dy) % ny, flip(xh, dx), flip(c, dc)) for dy, dx, dc in plane]
    plane_dev = [{"img_0": a, "img_1": b, "fsdp": d} for a, b, d in plane_ids]
    side_dev = [{"seq_1": 1 - xl}, {"seq_1": 1 - xl, "img_1": 1 - xh}]
    corner = {"seq_1": 1 - xl, "fsdp": 1 - c}
    stack = [{"seq_0": (z + k) % layers} for k in range(1, layers)]
    greet(plane_dev + side_dev + [corner] + stack)
    started = []

    def go(copy):
        copy.start()
        started.append(copy)
        return copy

    stage_a = []
    for n, (dy, dx, dc) in enumerate(plane):
        if dc == 0:
            k = len(stage_a)
            stage_a.append(go(remote(vec, v1.at[k], a_s.at[k], a_r.at[k], plane_dev[n])))
    ins = []
    for n, (dy, dx, dc) in enumerate(plane):
        a, b, d = plane_ids[n]
        ins.append((go(remote(wi.at[a, b, d], ri.at[n], i_s.at[n], i_r.at[n], plane_dev[n])), n, dc))
    outs = [
        (go(remote(ws.at[1 - xl, xh], rx.at[0], x_s.at[0], x_r.at[0], side_dev[0])), 0, 1),
        (go(remote(ws.at[1 - xl, 1 - xh], rx.at[1], x_s.at[1], x_r.at[1], side_dev[1])), 1, 1),
        (go(remote(ws.at[xl, 1 - xh], rx.at[2], x_s.at[2], x_r.at[2], {"img_1": 1 - xh})), 2, 0),
    ]
    total = vec[...]
    for k, copy in enumerate(stage_a):
        copy.wait_recv()
        total = total + v1[k]
    t1[...] = total
    q = xl * 2 + c
    stage_b = []
    for k, (dx, dc) in enumerate(((0, 1), (1, 0), (1, 1))):
        device = {"seq_1": flip(xl, dx), "fsdp": flip(c, dc)}
        stage_b.append(go(remote(t1, v2.at[q], b_s.at[k], b_r.at[k], device)))
    v2[q] = total
    for copy in stage_b:
        copy.wait_recv()
    t2[0:16] = v2[0, 0:16] + v2[1, 0:16] + v2[2, 0:16] + v2[3, 0:16]
    t2[16:32] = v2[0, 16:32] + v2[2, 16:32]
    t2[32:48] = v2[1, 16:32] + v2[3, 16:32]
    for j in range(4):
        t2[48 + j : 49 + j] = v2[j, 32:33]
    t2[52:56] = jnp.zeros((4, 128), F32)
    stage_d = []
    for k in range(1, layers):
        stage_d.append(go(remote(t2, v3.at[z], d_s.at[k - 1], d_r.at[k - 1], stack[k - 1])))
    v3[z] = t2[...]

    same = wi[y, xh, c].astype(F32)
    cross = jnp.zeros_like(same)
    for copy, n, dc in ins:
        copy.wait_recv()
        if dc:
            cross = cross + ri[n].astype(F32)
        else:
            same = same + ri[n].astype(F32)
    width = same.shape[1]
    w_in[:, pl.ds(pl.multiple_of(c * width, 128), width)] = same
    w_in[:, pl.ds(pl.multiple_of((1 - c) * width, 128), width)] = cross
    near = ws[xl, xh].astype(F32)
    outs[2][0].wait_recv()
    near = near + rx[2].astype(F32)
    outs[0][0].wait_recv()
    outs[1][0].wait_recv()
    far = rx[0].astype(F32) + rx[1].astype(F32)
    width = near.shape[1]
    w_out[:, pl.ds(pl.multiple_of(xl * width, 128), width)] = near
    w_out[:, pl.ds(pl.multiple_of((1 - xl) * width, 128), width)] = far

    for copy in stage_d:
        copy.wait_recv()
    total = v3[0]
    for j in range(1, layers):
        total = total + v3[j]
    gain[...] = total[0:8]
    bias[...] = total[8:16]
    b_out[...] = total[16:48]
    for j in range(layers):
        b_in[4 * j : 4 * j + 4, :] = v3[j, 48:52]
    for copy in started:
        copy.wait_send()


def last(ws, wi, vec, layers):
    ny = wi.shape[0]
    members = ny * 4 - 1
    block = wi.shape[3:]
    outs = (
        jax.ShapeDtypeStruct((ws.shape[2], 2 * ws.shape[3]), F32),
        jax.ShapeDtypeStruct((block[0], 2 * block[1]), F32),
        jax.ShapeDtypeStruct((8, 128), F32),
        jax.ShapeDtypeStruct((8, 128), F32),
        jax.ShapeDtypeStruct((32, 128), F32),
        jax.ShapeDtypeStruct((4 * layers, 128), F32),
    )
    scratch = [
        pltpu.VMEM((3, *ws.shape[2:]), BF16),
        pltpu.VMEM((members, *block), BF16),
        pltpu.VMEM((2 * ny - 1, 40, 128), F32),
        pltpu.VMEM((40, 128), F32),
        pltpu.VMEM((4, 40, 128), F32),
        pltpu.VMEM((56, 128), F32),
        pltpu.VMEM((layers, 56, 128), F32),
    ]
    for n in (3, members, 2 * ny - 1, 3, layers - 1):
        scratch += [DMA((n,)), DMA((n,))]
    return call(last_kernel, outs, scratch, 3, (ws, wi, vec), 1 << 32)


def gelu_parts(preact):
    cumul = 0.5 * (1.0 + lax.erf(preact * 0.7071067811865476))
    density = jnp.exp(-0.5 * preact * preact) * 0.3989422804014327
    return (preact * cumul, cumul + preact * density)


def contract(left, right, left_dim, right_dim, out=F32):
    return lax.dot_general(left, right, (((left_dim,), (right_dim,)), ((), ())), preferred_element_type=out)


def per_device(vision_feats, ln_gain, ln_bias, w_in, b_in, w_out, lm_grad, image_counts, token_pos):
    layers = lax.axis_size("seq_0")
    xl, c = lax.axis_index("seq_1"), lax.axis_index("fsdp")
    seq_index = lax.axis_index(SEQ)
    lm = lm_grad[0]
    block_rows, half = lm.shape
    quarter = half // 2
    own_hid = b_in.shape[0]
    unit = own_hid // 2
    layer_hid = 2 * own_hid

    own = lax.dynamic_slice_in_dim(lm, xl * quarter, quarter, 1)
    gathered_a = lax.all_gather(own, "seq_0", axis=0)
    swapped = swap_columns(lax.optimization_barrier((lm, own))[0])
    gathered_b = lax.all_gather(swapped, "seq_0", axis=0)

    counts, positions = image_counts[0], token_pos[0]
    images = positions.shape[0] // PATCH
    starts = []
    for i in range(images):
        starts.append(jnp.where(i >= counts[0], LEN, 0) + positions[i * PATCH])

    v_all, w_out_q, w_in_all, b_in_all = exchange(
        vision_feats[0], w_out, w_in, b_in.reshape(-1, 128), layers
    )
    w_out_q = w_out_q.reshape(layer_hid, quarter)
    w_in_layer = jnp.moveaxis(w_in_all, 1, 2).reshape(-1, layer_hid)
    b_in_layer = b_in_all.reshape(layer_hid)
    values = v_all.reshape(-1, *v_all.shape[3:]).astype(F32)
    row_mean = jnp.mean(values, axis=-1, keepdims=True)
    centred = values - row_mean
    row_var = jnp.mean(centred * centred, axis=-1, keepdims=True)
    normed = centred * lax.rsqrt(row_var + 1e-05)
    rows = normed.shape[0] * normed.shape[1]
    normed_in = (normed * ln_gain + ln_bias).astype(BF16).reshape(rows, -1)
    normed = normed.astype(BF16).reshape(rows, -1)
    preact = contract(normed_in, w_in_layer, 1, 0) + b_in_layer
    hidden = gelu_parts(preact)[0].astype(BF16)
    at = (2 * xl + c) * unit
    slope = gelu_parts(lax.dynamic_slice_in_dim(preact, at, unit, 1))[1]
    w_in_own = lax.dynamic_slice_in_dim(w_in_layer, at, unit, 1).astype(F32)
    hidden_pos = jnp.zeros((layers * 2 * block_rows, layer_hid), BF16)
    for i, start in enumerate(starts):
        hidden_pos = lax.dynamic_update_slice(hidden_pos, hidden[i * PATCH : (i + 1) * PATCH], (start, 0))
    hidden_pos = hidden_pos.reshape(layers, 2, block_rows, layer_hid)

    position = seq_index * block_rows + jnp.arange(block_rows, dtype=jnp.int32)
    taken = sum(((position >= s) & (position < s + PATCH)).astype(BF16) for s in starts)
    out_bias = jnp.dot(taken[None, :], lm, preferred_element_type=F32)[0]

    pa = gathered_a.reshape(-1, quarter)
    pb = gathered_b.reshape(-1, quarter)
    ha = lax.dynamic_index_in_dim(hidden_pos, xl, 1, keepdims=False).reshape(-1, layer_hid)
    hb = lax.dynamic_index_in_dim(hidden_pos, 1 - xl, 1, keepdims=False).reshape(-1, layer_hid)
    part_a = contract(pa, w_out_q, 1, 1, BF16)
    w_part_a = contract(ha, pa, 0, 0)
    part_b = contract(pb, w_out_q, 1, 1, BF16)
    w_part = (w_part_a + contract(hb, pb, 0, 0)).astype(BF16)
    shape = (layers, 1, block_rows, layer_hid)
    hp = jnp.zeros((layers, 2, block_rows, layer_hid), BF16)
    hp = lax.dynamic_update_slice(hp, part_a.reshape(shape), (0, xl, 0, 0))
    hp = lax.dynamic_update_slice(hp, part_b.reshape(shape), (0, 1 - xl, 0, 0)).reshape(-1, layer_hid)
    hp = jnp.concatenate([lax.dynamic_slice_in_dim(hp, s, PATCH, 0) for s in starts], axis=0)

    ny = lax.axis_size("img_0")
    block = layer_hid // (2 * ny)
    pg, w_sum = middle(hp, slope, w_part.reshape(2, ny, block, quarter))
    w_sum = w_sum.reshape(2, 2, block // 2, quarter)
    w_in_part = contract(normed_in, pg, 0, 0, BF16)
    moment = contract(normed, pg, 0, 0)
    b_in_part = jnp.sum(pg.astype(F32), axis=0)
    gain_part = jnp.sum(moment * w_in_own, axis=1)
    bias_part = jnp.sum(w_in_own * b_in_part, axis=1)
    vec = jnp.concatenate([gain_part, bias_part, out_bias, b_in_part, jnp.zeros((7 * 128,), F32)])
    w_out_grad, w_in_grad, gain, bias, b_out, b_in_grad = last(
        w_sum, w_in_part.reshape(ny, 2, 2, -1, unit), vec.reshape(-1, 128), layers
    )
    return (w_in_grad, b_in_grad.reshape(-1), w_out_grad, b_out.reshape(-1), gain.reshape(-1), bias.reshape(-1))


def solution(mesh):
    finer = Mesh(
        mesh.devices.reshape(8, 2, 4, 2, mesh.shape["fsdp"]),
        ("seq_0", "seq_1", "img_0", "img_1", "fsdp"),
    )
    placed = (
        P(IMG, SEQ_FSDP, None),
        P(),
        P(),
        P("fsdp", SEQ),
        P(SEQ),
        P(SEQ, "fsdp"),
        P(IMG, SEQ, "fsdp"),
        P(IMG, None),
        P(IMG, None),
    )
    return jax.shard_map(
        per_device,
        mesh=finer,
        in_specs=placed,
        out_specs=(P(IMG_FSDP, SEQ), P(), P(SEQ_IMG, "fsdp"), P(), P(), P()),
        check_vma=False,
    )
```

```python
import jax
import jax.numpy as jnp
from jax import lax
from jax.experimental import pallas as pl
from jax.experimental.pallas import tpu as pltpu
from jax.sharding import Mesh
from jax.sharding import PartitionSpec as P

PATCH = 576
LEN = 2048
SEQ = ("seq_0", "seq_1")
IMG = ("img_0", "img_1")
SEQ_FSDP = ("seq_0", "seq_1", "fsdp")
IMG_FSDP = ("img_0", "img_1", "fsdp")
SEQ_IMG = ("seq_0", "seq_1", "img_0", "img_1")
MESH = pl.DeviceIdType.MESH
BF16 = jnp.bfloat16
F32 = jnp.float32
VMEM = pl.BlockSpec(memory_space=pltpu.VMEM)
SMEM = pl.BlockSpec(memory_space=pltpu.SMEM)
ANY = pl.BlockSpec(memory_space=pl.ANY)
DMA = pltpu.SemaphoreType.DMA
LIMIT = 63 * 1024 * 1024
WINDOW = 640


def remote(src, dst, send, recv, device):
    return pltpu.make_async_remote_copy(
        src_ref=src, dst_ref=dst, send_sem=send, recv_sem=recv, device_id=device, device_id_type=MESH
    )


def greet(devices):
    barrier = pltpu.get_barrier_semaphore()
    for device in devices:
        pl.semaphore_signal(barrier, inc=1, device_id=device, device_id_type=MESH)
    pl.semaphore_wait(barrier, len(devices))


def call(kernel, outs, scratch, number, args, flops, specs=None):
    ins, results = specs or ([VMEM] * len(args), [VMEM] * len(outs))
    return pl.pallas_call(
        kernel,
        out_shape=tuple(outs),
        in_specs=ins,
        out_specs=tuple(results),
        scratch_shapes=scratch,
        compiler_params=pltpu.CompilerParams(
            collective_id=number, has_side_effects=number is not None, vmem_limit_bytes=LIMIT
        ),
        cost_estimate=pl.CostEstimate(flops=flops, bytes_accessed=1 << 20, transcendentals=0),
    )(*args)


def gelu_parts(preact):
    cumul = 0.5 * (1.0 + lax.erf(preact * 0.7071067811865476))
    density = jnp.exp(-0.5 * preact * preact) * 0.3989422804014327
    return (preact * cumul, cumul + preact * density)


def contract(left, right, left_dim, right_dim):
    return lax.dot_general(left, right, (((left_dim,), (right_dim,)), ((), ())), preferred_element_type=F32)


def image_starts(counts, token_pos):
    images = token_pos.shape[1] // PATCH
    return [jnp.where(counts[0, 0] <= i, LEN, 0) + token_pos[0, i * PATCH] for i in range(images)]


def main_kernel(
    counts, token_pos, v, wo, wi, bi, lm, gain, bias,
    grads_out, hid_out, slope_out, nrm_out, nin_out, hg_out, turned, b_out,
    grads, vs, wq, wis, bis, mine, r1, give, r2, hg, nrm, nin, hid, slope, pre, nf,
    vu_s, vu_r, vd_s, vd_r, vx_s, vx_r, vc_s, vc_r,
    pu_s, pu_r, pd_s, pd_r, px_s, px_r, wx_s, wx_r, wc_s, wc_r,
    h1_s, h1_r, h2_s, h2_r, local, put_p, put_v, put_h,
):
    layers = vs.shape[0]
    block_rows = lm.shape[0]
    chunk = block_rows // 2
    quarter = grads.shape[1]
    own_hid = wo.shape[0]
    unit = own_hid // 2
    layer_rows = 4 * v.shape[0]
    z, xl, c = lax.axis_index("seq_0"), lax.axis_index("seq_1"), lax.axis_index("fsdp")
    other, peer = 1 - xl, 1 - c
    up, down = {"seq_0": (z + 1) % layers}, {"seq_0": (z + layers - 1) % layers}
    across, twin = {"seq_1": other}, {"fsdp": peer}
    mine_cols = pl.ds(pl.multiple_of(xl * quarter, 128), quarter)
    their_cols = pl.ds(pl.multiple_of(other * quarter, 128), quarter)

    def below(s):
        return (z + layers - s) % layers

    def above(s):
        return (z + s) % layers

    def rows(zb, xq, k):
        return pl.ds(pl.multiple_of((zb * 2 + xq) * block_rows + k * chunk, 128), chunk)

    def ring_p(s, t, upward):
        xq = xl if t == 0 else other
        if upward:
            r = rows(below(s), xq, 0)
            return lambda n: remote(grads.at[r], grads.at[r], pu_s.at[n, t], pu_r.at[n, t], up)
        r = rows(above(s), xq, 1)
        return lambda n: remote(grads.at[r], grads.at[r], pd_s.at[n, t], pd_r.at[n, t], down)

    def ring_v(s, upward):
        zb = below(s) if upward else above(s)
        ref = vs.at[zb, xl, c]
        if upward:
            return lambda n: remote(ref, ref, vu_s.at[n], vu_r.at[n], up)
        return lambda n: remote(ref, ref, vd_s.at[n], vd_r.at[n], down)

    def v_across(s, d, xq):
        ref = vs.at[below(s) if d == 0 else above(s), xq, c]
        return remote(ref, ref, vx_s.at[d, s], vx_r.at[d, s], across)

    def v_twin(s, d, xq, t, cq):
        ref = vs.at[below(s) if d == 0 else above(s), xq, cq]
        return remote(ref, ref, vc_s.at[t, d, s], vc_r.at[t, d, s], twin)

    def p_swap(k, xq):
        r = rows(z, xq, k)
        source = lm.at[pl.ds(k * chunk, chunk), their_cols]
        return remote(source, grads.at[r], px_s.at[k], px_r.at[k], across)

    def w_in_at(cq, xq):
        size = wi.shape[0]
        return wis.at[pl.ds(pl.multiple_of(cq * size, 128), size), pl.ds(pl.multiple_of(xq * own_hid, 128), own_hid)]

    def w_out_at(xq):
        return wq.at[pl.ds(pl.multiple_of(xq * own_hid, 128), own_hid)]

    def w_swap(n, xq):
        source = (wo.at[:, their_cols], wi, bi)[n]
        target = (w_out_at(xq), w_in_at(c, xq), bis.at[xq])[n]
        return remote(source, target, wx_s.at[n], wx_r.at[n], across)

    def w_twin(t, cq):
        ref = w_in_at(cq, xl if t == 0 else other)
        return remote(ref, ref, wc_s.at[t], wc_r.at[t], twin)

    def lanes(xq, cq):
        return pl.ds(pl.multiple_of((xq * 2 + cq) * unit, 128), unit)

    def h_twin(s, xq):
        return remote(mine.at[s, :, :, lanes(xq, peer)], r1.at[s, xq], h1_s.at[s, xq], h1_r.at[s, xq], twin)

    def h_across(s):
        return remote(give.at[s], r2.at[s], h2_s.at[s], h2_r.at[s], across)

    greet([up, down, across, twin])
    locals_ = [
        pltpu.make_async_copy(lm.at[pl.ds(0, chunk), mine_cols], grads.at[rows(z, xl, 0)], local.at[0]),
        pltpu.make_async_copy(lm.at[pl.ds(chunk, chunk), mine_cols], grads.at[rows(z, xl, 1)], local.at[1]),
        pltpu.make_async_copy(v, vs.at[z, xl, c], local.at[2]),
        pltpu.make_async_copy(wo.at[:, mine_cols], w_out_at(xl), local.at[3]),
        pltpu.make_async_copy(wi, w_in_at(c, xl), local.at[4]),
        pltpu.make_async_copy(bi, bis.at[xl], local.at[5]),
    ]
    for copy in locals_:
        copy.start()
    p_swap(0, xl).start()
    p_swap(1, xl).start()
    for n in range(3):
        w_swap(n, xl).start()
    locals_[2].wait()
    ring_v(0, True)(0).start()
    ring_v(0, False)(0).start()
    for copy in locals_[:2]:
        copy.wait()
    ring_p(0, 0, True)(0).start()
    ring_p(0, 0, False)(0).start()
    v_across(0, 0, xl).start()
    v_twin(0, 0, xl, 0, c).start()
    for copy in locals_[3:]:
        copy.wait()
    w_twin(0, c).start()

    starts = image_starts(counts, token_pos)
    here = (z * 2 + xl) * block_rows + lax.broadcasted_iota(jnp.int32, (block_rows, 1), 0)
    taken = jnp.zeros((block_rows, 1), F32)
    for start in starts:
        taken = taken + jnp.where((here >= start) & (here < start + PATCH), 1.0, 0.0)
    for j in range(lm.shape[1] // 128):
        column = lm[:, j * 128 : (j + 1) * 128].astype(F32) * taken
        b_out[j : j + 1, :] = jnp.sum(column, axis=0, keepdims=True)
    def put_chunk(s, t, upward):
        r = rows(below(s) if upward else above(s), xl if t == 0 else other, 0 if upward else 1)
        return pltpu.make_async_copy(grads.at[r], grads_out.at[r], put_p.at[s, t, 0 if upward else 1])

    def put_layer(s, d, n):
        r = pl.ds(pl.multiple_of((below(s) if d == 0 else above(s)) * layer_rows, 32), layer_rows)
        source = (hid, slope, nrm, nin)[n]
        target = (hid_out, slope_out, nrm_out, nin_out)[n]
        return pltpu.make_async_copy(source.at[r], target.at[r], put_v.at[s, d, n])

    def put_sum(s, xq, k):
        r = rows(below(s) if k == 0 else above(s), xq, k)
        return pltpu.make_async_copy(hg.at[r], hg_out.at[r], put_h.at[s, xq, k])

    put_chunk(0, 0, True).start()
    put_chunk(0, 0, False).start()
    p_swap(0, other).wait_recv()
    ring_p(0, 1, True)(0).start()
    put_chunk(0, 1, True).start()
    p_swap(1, other).wait_recv()
    ring_p(0, 1, False)(0).start()
    put_chunk(0, 1, False).start()

    def multiply(s):
        for xq in range(2):
            for k in range(2):
                r = rows(below(s) if k == 0 else above(s), xq, k)
                mine[s, xq * 2 + k] = contract(grads[r, :], wq[...], 1, 1)
        for xq in range(2):
            h_twin(s, xq).start()

    def add_twin(s):
        for xq in range(2):
            h_twin(s, xq).wait_recv()
        give[s] = (mine[s, :, :, lanes(other, c)] + r1[s, other]).astype(BF16)
        h_across(s).start()
        for xq in range(2):
            for k in range(2):
                r = rows(below(s) if k == 0 else above(s), xq, k)
                n = xq * 2 + k
                hg[r, :] = mine[s, n, :, lanes(xl, c)] + r1[s, xl, n]

    def add_across(s):
        h_across(s).wait_recv()
        for xq in range(2):
            for k in range(2):
                r = rows(below(s) if k == 0 else above(s), xq, k)
                hg[r, :] = hg[r, :] + r2[s, xq * 2 + k].astype(F32)
                put_sum(s, xq, k).start()

    def span(body, lo, hi):
        def step(s, carry):
            body(s)
            return carry

        lax.fori_loop(lo, hi, step, 0)

    def normalise(zb):
        for n in range(4):
            values = vs[zb, n // 2, n % 2].astype(F32)
            mean = jnp.mean(values, axis=1, keepdims=True)
            centred = values - mean
            var = jnp.mean(centred * centred, axis=1, keepdims=True)
            size = values.shape[0]
            nf[n * size : (n + 1) * size, :] = centred * lax.rsqrt(var + 1e-05)
        r = pl.ds(pl.multiple_of(zb * layer_rows, 32), layer_rows)
        normed = nf[...]
        nrm[r, :] = normed.astype(BF16)
        nin[r, :] = (normed * gain[...] + bias[...]).astype(BF16)
        pre[...] = contract(nin[r, :], wis[...], 1, 0)
        for xq in range(2):
            for half in range(2):
                at = xq * own_hid + half * unit
                pre[:, at : at + unit] = pre[:, at : at + unit] + bis[xq, half : half + 1, :]
        hid[r, :] = gelu_parts(pre[...])[0].astype(BF16)
        slope[r, :] = gelu_parts(pre[:, lanes(xl, c)])[1]

    v_up, v_down = layers // 2, layers // 2 - 1

    def serve_v(s):
        @pl.when(s <= v_up)
        def _():
            ring_v(s, True)(s - 1).wait_recv()

            @pl.when(s < v_up)
            def _():
                ring_v(s, True)(s).start()

            v_across(s, 0, xl).start()
            v_twin(s, 0, xl, 0, c).start()

        @pl.when(s <= v_down)
        def _():
            ring_v(s, False)(s - 1).wait_recv()

            @pl.when(s < v_down)
            def _():
                ring_v(s, False)(s).start()

            v_across(s, 1, xl).start()
            v_twin(s, 1, xl, 0, c).start()

        @pl.when(s - 1 <= v_up)
        def _():
            v_across(s - 1, 0, other).wait_recv()
            v_twin(s - 1, 0, other, 1, c).start()

        @pl.when((s >= 2) & (s - 1 <= v_down))
        def _():
            v_across(s - 1, 1, other).wait_recv()
            v_twin(s - 1, 1, other, 1, c).start()

    def serve_p(s, t):
        for upward in (True, False):
            ring_p(s, t, upward)(s - 1).wait_recv()

            @pl.when(s < layers - 1)
            def _():
                ring_p(s, t, upward)(s).start()

            put_chunk(s, t, upward).start()

    def use_v(s):
        @pl.when(s <= v_up)
        def _():
            v_twin(s, 0, xl, 0, peer).wait_recv()
            v_twin(s, 0, other, 1, peer).wait_recv()
            normalise(below(s))
            for n in range(4):
                put_layer(s, 0, n).start()

        @pl.when((s >= 1) & (s <= v_down))
        def _():
            v_twin(s, 1, xl, 0, peer).wait_recv()
            v_twin(s, 1, other, 1, peer).wait_recv()
            normalise(above(s))
            for n in range(4):
                put_layer(s, 1, n).start()

    def count(s):
        return jnp.maximum(jnp.minimum(2 * s - 3, s), 0)

    def step(s, carry):
        serve_v(s)
        serve_p(s, 0)

        @pl.when(s == 1)
        def _():
            w_swap(1, other).wait_recv()
            w_twin(1, c).start()

        @pl.when(s == 2)
        def _():
            w_swap(0, other).wait_recv()
            w_swap(2, other).wait_recv()
            for t in range(2):
                w_twin(t, peer).wait_recv()
            turned[...] = wis[:, lanes(xl, c)].astype(F32).T

        span(add_across, count(s - 3), count(s - 2))
        span(add_twin, count(s - 2), count(s - 1))
        span(multiply, count(s - 1), count(s))
        serve_p(s, 1)

        @pl.when(s >= 3)
        def _():
            use_v(s - 3)

        return carry

    lax.fori_loop(1, layers, step, 0)
    span(multiply, layers - 1, layers)
    span(add_twin, layers - 2, layers)
    span(add_across, layers - 3, layers)

    for k in range(2):
        p_swap(k, xl).wait_send()
    for n in range(3):
        w_swap(n, xl).wait_send()
    for t in range(2):
        w_twin(t, c).wait_send()

    def sent_p(s, carry):
        for t in range(2):
            for upward in (True, False):
                ring_p(s, t, upward)(s).wait_send()
        return carry

    lax.fori_loop(0, layers - 1, sent_p, 0)

    def put_done(s, carry):
        for t in range(2):
            for k in range(2):
                put_chunk(s, t, k == 0).wait()
                put_sum(s, t, k).wait()
        return carry

    lax.fori_loop(0, layers, put_done, 0)
    def sent_h(s):
        for xq in range(2):
            h_twin(s, xq).wait_send()
        h_across(s).wait_send()

    span(sent_h, 0, layers)
    for s in range(v_up):
        ring_v(s, True)(s).wait_send()
    for s in range(v_down):
        ring_v(s, False)(s).wait_send()
    for s in range(v_up + 1):
        for d in range(2):
            if d == 0 or 1 <= s <= v_down:
                for n in range(4):
                    put_layer(s, d, n).wait()
                v_across(s, d, xl).wait_send()
                v_twin(s, d, xl, 0, c).wait_send()
                v_twin(s, d, other, 1, c).wait_send()


def main(counts, token_pos, v, wo, wi, bi, lm, gain, bias, layers):
    rows, width = lm.shape
    quarter = width // 2
    own = wo.shape[0]
    unit = own // 2
    hid = 2 * own
    tokens = token_pos.shape[1]
    features = v.shape[1]
    layer_rows = 4 * v.shape[0]
    chunk = rows // 2
    places = layers * 2 * rows
    shapes = [
        ((places, quarter), BF16),
        ((tokens, hid), BF16),
        ((tokens, unit), F32),
        ((tokens, features), BF16),
        ((tokens, features), BF16),
        ((places, unit), F32),
    ]
    outs = [jax.ShapeDtypeStruct(*shape) for shape in shapes]
    outs += [jax.ShapeDtypeStruct((unit, features), F32), jax.ShapeDtypeStruct((width // 128, 128), F32)]
    scratch = [
        pltpu.VMEM((places, quarter), BF16),
        pltpu.VMEM((layers, 2, 2, *v.shape), BF16),
        pltpu.VMEM((hid, quarter), BF16),
        pltpu.VMEM((features, hid), BF16),
        pltpu.VMEM((2, *bi.shape), F32),
        pltpu.VMEM((layers, 4, chunk, hid), F32),
        pltpu.VMEM((layers, 2, 4, chunk, unit), F32),
        pltpu.VMEM((layers, 4, chunk, unit), BF16),
        pltpu.VMEM((layers, 4, chunk, unit), BF16),
        pltpu.VMEM((places, unit), F32),
        pltpu.VMEM((tokens, features), BF16),
        pltpu.VMEM((tokens, features), BF16),
        pltpu.VMEM((tokens, hid), BF16),
        pltpu.VMEM((tokens, unit), F32),
        pltpu.VMEM((layer_rows, hid), F32),
        pltpu.VMEM((layer_rows, features), F32),
    ]
    half = layers // 2
    sems = [(half,), (half - 1,), (2, half + 1), (2, 2, half + 1), (layers - 1, 2), (layers - 1, 2), (2,), (3,), (2,)]
    sems += [(layers, 2), (layers,)]
    for shape in sems:
        scratch += [DMA(shape), DMA(shape)]
    scratch += [DMA((6,)), DMA((layers, 2, 2)), DMA((half + 1, 2, 4)), DMA((layers, 2, 2))]
    specs = [SMEM] * 2 + [VMEM] * 7, [ANY] * 6 + [VMEM] * 2
    return call(main_kernel, outs, scratch, 0, (counts, token_pos, v, wo, wi, bi, lm, gain, bias), 1 << 34, specs)


def product_kernel(
    counts, token_pos, grads, hid, slope, nrm, nin, hg, turned, b_out,
    w_out_part, w_in_part, vec,
    pw, hv, hw, sv, rv, nv, acc, shift, pgs, got, got_p, got_h,
):
    starts = image_starts(counts, token_pos)
    size = PATCH + 8
    places = grads.shape[0]
    windows, sums, bases, lows = [], [], [], []
    for i, start in enumerate(starts):
        base = jnp.minimum((start // 16) * 16, places - WINDOW)
        low = jnp.minimum((start // 8) * 8, places - size)
        bases.append(base)
        lows.append(low)
        windows.append(
            pltpu.make_async_copy(grads.at[pl.ds(pl.multiple_of(base, 16), WINDOW)], pw.at[i], got_p.at[i])
        )
        sums.append(pltpu.make_async_copy(hg.at[pl.ds(pl.multiple_of(low, 8), size)], hw.at[i], got_h.at[i]))
    others = [pltpu.make_async_copy(a, b, got.at[n]) for n, (a, b) in enumerate(((hid, hv), (slope, sv), (nin, rv), (nrm, nv)))]
    for copy in [others[0], windows[0], others[1]] + sums + windows[1:] + others[2:]:
        copy.start()
    shift[PATCH:, :] = jnp.zeros((WINDOW - PATCH, shift.shape[1]), F32)
    vec[16:32, :] = b_out[...]
    vec[33:40, :] = jnp.zeros((7, 128), F32)
    others[0].wait()
    for i, start in enumerate(starts):
        shift[0:PATCH, :] = hv[i * PATCH : (i + 1) * PATCH, :].astype(F32)
        left = pltpu.roll(shift[...], start - bases[i], 0).astype(BF16)
        windows[i].wait()
        product = contract(left, pw[i], 0, 0)
        acc[...] = product if i == 0 else acc[...] + product
    w_out_part[...] = acc[...].astype(BF16)
    unit = sv.shape[1]
    total = jnp.zeros((1, unit), F32)
    others[1].wait()
    for i, start in enumerate(starts):
        r = slice(i * PATCH, (i + 1) * PATCH)
        sums[i].wait()
        back = jnp.where(start == lows[i], 0, size - (start - lows[i]))
        window = pltpu.roll(hw[i], back, 0)[0:PATCH]
        pg = (window * sv[r, :]).astype(BF16)
        pgs[r, :] = pg
        total = total + jnp.sum(pg.astype(F32), axis=0, keepdims=True)
    vec[32:33, :] = total
    others[2].wait()
    w_in_part[...] = contract(pgs[...], rv[...], 0, 0).T
    others[3].wait()
    moment = contract(pgs[...], nv[...], 0, 0)
    column = contract(pgs[...], jnp.ones((pgs.shape[0], 128), BF16), 0, 0)
    for j in range(nv.shape[1] // 128):
        at = slice(j * 128, (j + 1) * 128)
        vec[j : j + 1, :] = jnp.sum(moment[:, at] * turned[:, at], axis=0, keepdims=True)
        vec[8 + j : 9 + j, :] = jnp.sum(column * turned[:, at], axis=0, keepdims=True)


def products(counts, token_pos, grads, hid, slope, nrm, nin, hg, turned, b_out):
    images = token_pos.shape[1] // PATCH
    features, unit, quarter = nrm.shape[1], hg.shape[1], grads.shape[1]
    width = hid.shape[1]
    outs = (
        jax.ShapeDtypeStruct((width, quarter), BF16),
        jax.ShapeDtypeStruct((features, unit), F32),
        jax.ShapeDtypeStruct((40, 128), F32),
    )
    scratch = [
        pltpu.VMEM((images, WINDOW, quarter), BF16),
        pltpu.VMEM(hid.shape, BF16),
        pltpu.VMEM((images, PATCH + 8, unit), F32),
        pltpu.VMEM(slope.shape, F32),
        pltpu.VMEM(nin.shape, BF16),
        pltpu.VMEM(nrm.shape, BF16),
        pltpu.VMEM((width, quarter), F32),
        pltpu.VMEM((WINDOW, width), F32),
        pltpu.VMEM(slope.shape, BF16),
        DMA((4,)),
        DMA((images,)),
        DMA((images,)),
    ]
    specs = [SMEM] * 2 + [ANY] * 6 + [VMEM] * 2, [VMEM] * 3
    return call(product_kernel, outs, scratch, None, (counts, token_pos, grads, hid, slope, nrm, nin, hg, turned, b_out), 1 << 34, specs)


def last_kernel(
    wo, wi, vec, w_out, w_in, gain, bias, b_out, b_in, ry, ws, rx, ri, v1, t1, v2, t2, v3,
    y_s, y_r, x_s, x_r, i_s, i_r, a_s, a_r, b_s, b_r, d_s, d_r,
):
    layers, ny = v3.shape[0], wi.shape[0]
    z, xl, c = lax.axis_index("seq_0"), lax.axis_index("seq_1"), lax.axis_index("fsdp")
    y, xh = lax.axis_index("img_0"), lax.axis_index("img_1")

    def flip(me, bit):
        return 1 - me if bit else me

    plane = []
    for dy in range(ny):
        for dx in range(2):
            for dc in range(2):
                if (dy, dx, dc) != (0, 0, 0):
                    plane.append((dy, dx, dc))
    plane_ids = [((y + dy) % ny, flip(xh, dx), flip(c, dc)) for dy, dx, dc in plane]
    plane_dev = [{"img_0": a, "img_1": b, "fsdp": d} for a, b, d in plane_ids]
    side_dev = [{"seq_1": 1 - xl}, {"seq_1": 1 - xl, "img_1": 1 - xh}]
    corner = {"seq_1": 1 - xl, "fsdp": 1 - c}
    stack = [{"seq_0": (z + k) % layers} for k in range(1, layers)]
    greet(plane_dev + side_dev + [corner] + stack)
    ys = [{"img_0": (y + k) % ny} for k in range(1, ny)]
    started = []

    def go(copy):
        copy.start()
        started.append(copy)
        return copy

    stage_a = []
    for n, (dy, dx, dc) in enumerate(plane):
        if dc == 0:
            k = len(stage_a)
            stage_a.append(go(remote(vec, v1.at[k], a_s.at[k], a_r.at[k], plane_dev[n])))
    firsts = []
    for k in range(1, ny):
        firsts.append(go(remote(wo.at[:, (y + k) % ny], ry.at[k - 1], y_s.at[k - 1], y_r.at[k - 1], ys[k - 1])))
    ins = []
    for n, (dy, dx, dc) in enumerate(plane):
        a, b, d = plane_ids[n]
        ins.append((go(remote(wi.at[a, b, d], ri.at[n], i_s.at[n], i_r.at[n], plane_dev[n])), n, dc))
    total = vec[...]
    for k, copy in enumerate(stage_a):
        copy.wait_recv()
        total = total + v1[k]
    t1[...] = total
    q = xl * 2 + c
    stage_b = []
    for k, (dx, dc) in enumerate(((0, 1), (1, 0), (1, 1))):
        device = {"seq_1": flip(xl, dx), "fsdp": flip(c, dc)}
        stage_b.append(go(remote(t1, v2.at[q], b_s.at[k], b_r.at[k], device)))
    v2[q] = total
    for copy in stage_b:
        copy.wait_recv()
    t2[0:16] = v2[0, 0:16] + v2[1, 0:16] + v2[2, 0:16] + v2[3, 0:16]
    t2[16:32] = v2[0, 16:32] + v2[2, 16:32]
    t2[32:48] = v2[1, 16:32] + v2[3, 16:32]
    for j in range(4):
        t2[48 + j : 49 + j] = v2[j, 32:33]
    t2[52:56] = jnp.zeros((4, 128), F32)
    stage_d = []
    for k in range(1, layers):
        stage_d.append(go(remote(t2, v3.at[z], d_s.at[k - 1], d_r.at[k - 1], stack[k - 1])))
    v3[z] = t2[...]

    summed = wo[:, y].astype(F32)
    for k, copy in enumerate(firsts):
        copy.wait_recv()
        summed = summed + ry[k].astype(F32)
    block = ws.shape[2]
    for j in range(2):
        ws[:, j] = summed[:, j * block : (j + 1) * block].astype(BF16)
    outs = [
        (go(remote(ws.at[1 - xl, xh], rx.at[0], x_s.at[0], x_r.at[0], side_dev[0])), 0, 1),
        (go(remote(ws.at[1 - xl, 1 - xh], rx.at[1], x_s.at[1], x_r.at[1], side_dev[1])), 1, 1),
        (go(remote(ws.at[xl, 1 - xh], rx.at[2], x_s.at[2], x_r.at[2], {"img_1": 1 - xh})), 2, 0),
    ]

    same = wi[y, xh, c].astype(F32)
    cross = jnp.zeros_like(same)
    for copy, n, dc in ins:
        copy.wait_recv()
        if dc:
            cross = cross + ri[n].astype(F32)
        else:
            same = same + ri[n].astype(F32)
    width = same.shape[1]
    w_in[:, pl.ds(pl.multiple_of(c * width, 128), width)] = same
    w_in[:, pl.ds(pl.multiple_of((1 - c) * width, 128), width)] = cross
    near = ws[xl, xh].astype(F32)
    outs[2][0].wait_recv()
    near = near + rx[2].astype(F32)
    outs[0][0].wait_recv()
    outs[1][0].wait_recv()
    far = rx[0].astype(F32) + rx[1].astype(F32)
    width = near.shape[1]
    w_out[:, pl.ds(pl.multiple_of(xl * width, 128), width)] = near
    w_out[:, pl.ds(pl.multiple_of((1 - xl) * width, 128), width)] = far

    for copy in stage_d:
        copy.wait_recv()
    total = v3[0]
    for j in range(1, layers):
        total = total + v3[j]
    gain[...] = total[0:8]
    bias[...] = total[8:16]
    b_out[...] = total[16:48]
    for j in range(layers):
        b_in[4 * j : 4 * j + 4, :] = v3[j, 48:52]
    for copy in started:
        copy.wait_send()


def last(wo, wi, vec, layers):
    ny = wi.shape[0]
    members = ny * 4 - 1
    block = wi.shape[3:]
    outs = (
        jax.ShapeDtypeStruct((wo.shape[2] // 2, 2 * wo.shape[3]), F32),
        jax.ShapeDtypeStruct((block[0], 2 * block[1]), F32),
        jax.ShapeDtypeStruct((8, 128), F32),
        jax.ShapeDtypeStruct((8, 128), F32),
        jax.ShapeDtypeStruct((32, 128), F32),
        jax.ShapeDtypeStruct((4 * layers, 128), F32),
    )
    scratch = [
        pltpu.VMEM((ny - 1, 2, *wo.shape[2:]), BF16),
        pltpu.VMEM((2, 2, wo.shape[2] // 2, wo.shape[3]), BF16),
        pltpu.VMEM((3, wo.shape[2] // 2, wo.shape[3]), BF16),
        pltpu.VMEM((members, *block), F32),
        pltpu.VMEM((2 * ny - 1, 40, 128), F32),
        pltpu.VMEM((40, 128), F32),
        pltpu.VMEM((4, 40, 128), F32),
        pltpu.VMEM((56, 128), F32),
        pltpu.VMEM((layers, 56, 128), F32),
    ]
    for n in (ny - 1, 3, members, 2 * ny - 1, 3, layers - 1):
        scratch += [DMA((n,)), DMA((n,))]
    return call(last_kernel, outs, scratch, 1, (wo, wi, vec), 1 << 32)


def per_device(vision_feats, ln_gain, ln_bias, w_in, b_in, w_out, lm_grad, image_counts, token_pos):
    layers, ny = lax.axis_size("seq_0"), lax.axis_size("img_0")
    pieces = main(
        image_counts,
        token_pos,
        vision_feats[0],
        w_out,
        w_in,
        b_in.reshape(2, -1),
        lm_grad[0],
        ln_gain[None],
        ln_bias[None],
        layers,
    )
    w_out_part, w_in_part, vec = products(image_counts, token_pos, *pieces)
    quarter, unit = w_out_part.shape[1], w_in_part.shape[1]
    w_out_grad, w_in_grad, gain, bias, b_out, b_in_grad = last(
        w_out_part.reshape(2, ny, -1, quarter), w_in_part.reshape(ny, 2, 2, -1, unit), vec, layers
    )
    return (w_in_grad, b_in_grad.reshape(-1), w_out_grad, b_out.reshape(-1), gain.reshape(-1), bias.reshape(-1))


def solution(mesh):
    finer = Mesh(
        mesh.devices.reshape(8, 2, 4, 2, mesh.shape["fsdp"]),
        ("seq_0", "seq_1", "img_0", "img_1", "fsdp"),
    )
    placed = (
        P(IMG, SEQ_FSDP, None),
        P(),
        P(),
        P("fsdp", SEQ),
        P(SEQ),
        P(SEQ, "fsdp"),
        P(IMG, SEQ, "fsdp"),
        P(IMG, None),
        P(IMG, None),
    )
    return jax.shard_map(
        per_device,
        mesh=finer,
        in_specs=placed,
        out_specs=(P(IMG_FSDP, SEQ), P(), P(SEQ_IMG, "fsdp"), P(), P(), P()),
        check_vma=False,
    )
```

```python
import jax
import jax.numpy as jnp
from jax import lax
from jax.experimental import pallas as pl
from jax.experimental.pallas import tpu as pltpu
from jax.sharding import Mesh
from jax.sharding import PartitionSpec as P

PATCH = 576
LEN = 2048
SEQ = ("seq_0", "seq_1")
IMG = ("img_0", "img_1")
SEQ_FSDP = ("seq_0", "seq_1", "fsdp")
IMG_FSDP = ("img_0", "img_1", "fsdp")
SEQ_IMG = ("seq_0", "seq_1", "img_0", "img_1")
MESH = pl.DeviceIdType.MESH
BF16 = jnp.bfloat16
F32 = jnp.float32
VMEM = pl.BlockSpec(memory_space=pltpu.VMEM)
SMEM = pl.BlockSpec(memory_space=pltpu.SMEM)
ANY = pl.BlockSpec(memory_space=pl.ANY)
DMA = pltpu.SemaphoreType.DMA
LIMIT = 63 * 1024 * 1024
WINDOW = 640
SUB = 2


def remote(src, dst, send, recv, device):
    return pltpu.make_async_remote_copy(
        src_ref=src, dst_ref=dst, send_sem=send, recv_sem=recv, device_id=device, device_id_type=MESH
    )


def signal(devices):
    barrier = pltpu.get_barrier_semaphore()
    for device in devices:
        pl.semaphore_signal(barrier, inc=1, device_id=device, device_id_type=MESH)


def greet(devices):
    signal(devices)
    pl.semaphore_wait(pltpu.get_barrier_semaphore(), len(devices))


def call(kernel, outs, scratch, number, args, flops, specs=None):
    ins, results = specs or ([VMEM] * len(args), [VMEM] * len(outs))
    return pl.pallas_call(
        kernel,
        out_shape=tuple(outs),
        in_specs=ins,
        out_specs=tuple(results),
        scratch_shapes=scratch,
        compiler_params=pltpu.CompilerParams(
            collective_id=number, has_side_effects=number is not None, vmem_limit_bytes=LIMIT
        ),
        cost_estimate=pl.CostEstimate(flops=flops, bytes_accessed=1 << 20, transcendentals=0),
    )(*args)


def gelu_parts(preact):
    cumul = 0.5 * (1.0 + lax.erf(preact * 0.7071067811865476))
    density = jnp.exp(-0.5 * preact * preact) * 0.3989422804014327
    return (preact * cumul, cumul + preact * density)


def contract(left, right, left_dim, right_dim):
    return lax.dot_general(left, right, (((left_dim,), (right_dim,)), ((), ())), preferred_element_type=F32)


def image_starts(counts, token_pos):
    images = token_pos.shape[1] // PATCH
    return [jnp.where(counts[0, 0] <= i, LEN, 0) + token_pos[0, i * PATCH] for i in range(images)]


def main_kernel(
    counts, token_pos, v, wo, wi, bi, lm, gain, bias,
    grads_out, hid_out, slope_out, nrm_out, nin_out, hg_out, turned, b_out,
    grads, vs, wq, wis, bis, mine, r1, give, r2, hg, nrm, nin, hid, slope, pre, nf, held,
    vu_s, vu_r, vd_s, vd_r, vx_s, vx_r, vc_s, vc_r,
    pu_s, pu_r, pd_s, pd_r, px_s, px_r, wx_s, wx_r, wc_s, wc_r,
    h1_s, h1_r, h2_s, h2_r, local, put_p, put_v, put_h,
):
    layers = vs.shape[0]
    block_rows = lm.shape[0]
    chunk = block_rows // 2
    quarter = grads.shape[1]
    own_hid = wo.shape[0]
    unit = own_hid // 2
    layer_rows = 4 * v.shape[0]
    z, xl, c = lax.axis_index("seq_0"), lax.axis_index("seq_1"), lax.axis_index("fsdp")
    other, peer = 1 - xl, 1 - c
    up, down = {"seq_0": (z + 1) % layers}, {"seq_0": (z + layers - 1) % layers}
    across, twin = {"seq_1": other}, {"fsdp": peer}
    mine_cols = pl.ds(pl.multiple_of(xl * quarter, 128), quarter)
    their_cols = pl.ds(pl.multiple_of(other * quarter, 128), quarter)

    def below(s):
        return (z + layers - s) % layers

    def above(s):
        return (z + s) % layers

    def rows(zb, xq, k):
        return pl.ds(pl.multiple_of((zb * 2 + xq) * block_rows + k * chunk, 128), chunk)

    def ring_p(s, t, upward, u):
        xq = xl if t == 0 else other
        size = chunk // SUB
        zb, k = (below(s), 0) if upward else (above(s), 1)
        r = pl.ds(pl.multiple_of((zb * 2 + xq) * block_rows + k * chunk + u * size, 16), size)
        if upward:
            return lambda n: remote(grads.at[r], grads.at[r], pu_s.at[n, t, u], pu_r.at[n, t, u], up)
        return lambda n: remote(grads.at[r], grads.at[r], pd_s.at[n, t, u], pd_r.at[n, t, u], down)

    def ring_v(s, upward):
        zb = below(s) if upward else above(s)
        ref = vs.at[zb, xl, c]
        if upward:
            return lambda n: remote(ref, ref, vu_s.at[n], vu_r.at[n], up)
        return lambda n: remote(ref, ref, vd_s.at[n], vd_r.at[n], down)

    def v_across(s, d, xq):
        ref = vs.at[below(s) if d == 0 else above(s), xq, c]
        return remote(ref, ref, vx_s.at[d, s], vx_r.at[d, s], across)

    def v_twin(s, d, xq, t, cq):
        ref = vs.at[below(s) if d == 0 else above(s), xq, cq]
        return remote(ref, ref, vc_s.at[t, d, s], vc_r.at[t, d, s], twin)

    def p_swap(u, k, xq):
        size = chunk // SUB
        r = pl.ds(pl.multiple_of((z * 2 + xq) * block_rows + k * chunk + u * size, 16), size)
        source = lm.at[pl.ds(k * chunk + u * size, size), their_cols]
        return remote(source, grads.at[r], px_s.at[u, k], px_r.at[u, k], across)

    def w_in_at(cq, xq):
        size = wi.shape[0]
        return wis.at[pl.ds(pl.multiple_of(cq * size, 128), size), pl.ds(pl.multiple_of(xq * own_hid, 128), own_hid)]

    def w_out_at(xq):
        return wq.at[pl.ds(pl.multiple_of(xq * own_hid, 128), own_hid)]

    def w_swap(n, xq):
        source = (wo.at[:, their_cols], wi, bi)[n]
        target = (w_out_at(xq), w_in_at(c, xq), bis.at[xq])[n]
        return remote(source, target, wx_s.at[n], wx_r.at[n], across)

    def w_twin(t, cq):
        ref = w_in_at(cq, xl if t == 0 else other)
        return remote(ref, ref, wc_s.at[t], wc_r.at[t], twin)

    def lanes(xq, cq):
        return pl.ds(pl.multiple_of((xq * 2 + cq) * unit, 128), unit)

    def h_twin(s, xq):
        return remote(mine.at[s, :, :, lanes(xq, peer)], r1.at[s, xq], h1_s.at[s, xq], h1_r.at[s, xq], twin)

    def h_across(s):
        return remote(give.at[s], r2.at[s], h2_s.at[s], h2_r.at[s], across)

    signal([up, down, across, twin])
    locals_ = [
        pltpu.make_async_copy(v, vs.at[z, xl, c], local.at[2]),
        pltpu.make_async_copy(lm.at[pl.ds(0, chunk), mine_cols], grads.at[rows(z, xl, 0)], local.at[0]),
        pltpu.make_async_copy(lm.at[pl.ds(chunk, chunk), mine_cols], grads.at[rows(z, xl, 1)], local.at[1]),
        pltpu.make_async_copy(wi, w_in_at(c, xl), local.at[4]),
        pltpu.make_async_copy(wo.at[:, mine_cols], w_out_at(xl), local.at[3]),
        pltpu.make_async_copy(bi, bis.at[xl], local.at[5]),
        pltpu.make_async_copy(lm, held, local.at[6]),
    ]
    for copy in locals_:
        copy.start()
    pl.semaphore_wait(pltpu.get_barrier_semaphore(), 4)
    for u in range(SUB):
        for k in range(2):
            p_swap(u, k, xl).start()
    locals_[0].wait()
    ring_v(0, True)(0).start()
    ring_v(0, False)(0).start()
    for copy in locals_[1:3]:
        copy.wait()
    for u in range(SUB):
        ring_p(0, 0, True, u)(0).start()
        ring_p(0, 0, False, u)(0).start()
    v_across(0, 0, xl).start()
    for n in (1, 2, 0):
        w_swap(n, xl).start()
    v_twin(0, 0, xl, 0, c).start()
    for copy in locals_[3:6]:
        copy.wait()
    w_twin(0, c).start()

    def put_chunk(s, t, upward):
        r = rows(below(s) if upward else above(s), xl if t == 0 else other, 0 if upward else 1)
        return pltpu.make_async_copy(grads.at[r], grads_out.at[r], put_p.at[s, t, 0 if upward else 1])

    def put_layer(s, d, n):
        r = pl.ds(pl.multiple_of((below(s) if d == 0 else above(s)) * layer_rows, 32), layer_rows)
        source = (hid, slope, nrm, nin)[n]
        target = (hid_out, slope_out, nrm_out, nin_out)[n]
        return pltpu.make_async_copy(source.at[r], target.at[r], put_v.at[s, d, n])

    def put_sum(s, xq, k):
        r = rows(below(s) if k == 0 else above(s), xq, k)
        return pltpu.make_async_copy(hg.at[r], hg_out.at[r], put_h.at[s, xq, k])

    for u in range(SUB):
        p_swap(u, 0, other).wait_recv()
        ring_p(0, 1, True, u)(0).start()
        p_swap(u, 1, other).wait_recv()
        ring_p(0, 1, False, u)(0).start()
    for t in range(2):
        put_chunk(0, t, True).start()
        put_chunk(0, t, False).start()
    locals_[6].wait()
    starts = image_starts(counts, token_pos)
    here = (z * 2 + xl) * block_rows + lax.broadcasted_iota(jnp.int32, (block_rows, 1), 0)
    taken = jnp.zeros((block_rows, 1), F32)
    for start in starts:
        taken = taken + jnp.where((here >= start) & (here < start + PATCH), 1.0, 0.0)
    for j in range(lm.shape[1] // 128):
        column = held[:, j * 128 : (j + 1) * 128].astype(F32) * taken
        b_out[j : j + 1, :] = jnp.sum(column, axis=0, keepdims=True)
    def multiply(s):
        for xq in range(2):
            for k in range(2):
                r = rows(below(s) if k == 0 else above(s), xq, k)
                mine[s, xq * 2 + k] = contract(grads[r, :], wq[...], 1, 1)
        for xq in range(2):
            h_twin(s, xq).start()

    def add_twin(s):
        for xq in range(2):
            h_twin(s, xq).wait_recv()
        give[s] = (mine[s, :, :, lanes(other, c)] + r1[s, other]).astype(BF16)
        h_across(s).start()
        for xq in range(2):
            for k in range(2):
                r = rows(below(s) if k == 0 else above(s), xq, k)
                n = xq * 2 + k
                hg[r, :] = mine[s, n, :, lanes(xl, c)] + r1[s, xl, n]

    def add_across(s):
        h_across(s).wait_recv()
        for xq in range(2):
            for k in range(2):
                r = rows(below(s) if k == 0 else above(s), xq, k)
                hg[r, :] = hg[r, :] + r2[s, xq * 2 + k].astype(F32)
                put_sum(s, xq, k).start()

    def span(body, lo, hi):
        def step(s, carry):
            body(s)
            return carry

        lax.fori_loop(lo, hi, step, 0)

    def normalise(zb):
        for n in range(4):
            values = vs[zb, n // 2, n % 2].astype(F32)
            mean = jnp.mean(values, axis=1, keepdims=True)
            centred = values - mean
            var = jnp.mean(centred * centred, axis=1, keepdims=True)
            size = values.shape[0]
            nf[n * size : (n + 1) * size, :] = centred * lax.rsqrt(var + 1e-05)
        r = pl.ds(pl.multiple_of(zb * layer_rows, 32), layer_rows)
        normed = nf[...]
        nrm[r, :] = normed.astype(BF16)
        nin[r, :] = (normed * gain[...] + bias[...]).astype(BF16)
        pre[...] = contract(nin[r, :], wis[...], 1, 0)
        for xq in range(2):
            for half in range(2):
                at = xq * own_hid + half * unit
                pre[:, at : at + unit] = pre[:, at : at + unit] + bis[xq, half : half + 1, :]
        hid[r, :] = gelu_parts(pre[...])[0].astype(BF16)
        slope[r, :] = gelu_parts(pre[:, lanes(xl, c)])[1]

    v_up, v_down = layers // 2, layers // 2 - 1

    def serve_v(s):
        @pl.when(s <= v_up)
        def _():
            ring_v(s, True)(s - 1).wait_recv()

            @pl.when(s < v_up)
            def _():
                ring_v(s, True)(s).start()

            v_across(s, 0, xl).start()
            v_twin(s, 0, xl, 0, c).start()

        @pl.when(s <= v_down)
        def _():
            ring_v(s, False)(s - 1).wait_recv()

            @pl.when(s < v_down)
            def _():
                ring_v(s, False)(s).start()

            v_across(s, 1, xl).start()
            v_twin(s, 1, xl, 0, c).start()

        @pl.when((s >= 2) & (s - 2 <= v_up))
        def _():
            v_across(s - 2, 0, other).wait_recv()
            v_twin(s - 2, 0, other, 1, c).start()

        @pl.when((s >= 3) & (s - 2 <= v_down))
        def _():
            v_across(s - 2, 1, other).wait_recv()
            v_twin(s - 2, 1, other, 1, c).start()

    def serve_p(s, t):
        for u in range(SUB):
            for upward in (True, False):
                ring_p(s, t, upward, u)(s - 1).wait_recv()

                @pl.when(s < layers - 1)
                def _():
                    ring_p(s, t, upward, u)(s).start()

        for upward in (True, False):
            put_chunk(s, t, upward).start()

    def use_v(s):
        @pl.when(s <= v_up)
        def _():
            v_twin(s, 0, xl, 0, peer).wait_recv()
            v_twin(s, 0, other, 1, peer).wait_recv()
            normalise(below(s))
            for n in range(4):
                put_layer(s, 0, n).start()

        @pl.when((s >= 1) & (s <= v_down))
        def _():
            v_twin(s, 1, xl, 0, peer).wait_recv()
            v_twin(s, 1, other, 1, peer).wait_recv()
            normalise(above(s))
            for n in range(4):
                put_layer(s, 1, n).start()

    def count(s):
        return jnp.maximum(jnp.minimum(2 * s - 4, s), 0)

    def step(s, carry):
        serve_v(s)
        serve_p(s, 0)

        @pl.when(s == 2)
        def _():
            w_swap(1, other).wait_recv()
            w_twin(1, c).start()

        @pl.when(s == 3)
        def _():
            w_swap(0, other).wait_recv()
            w_swap(2, other).wait_recv()
            for t in range(2):
                w_twin(t, peer).wait_recv()
            turned[...] = wis[:, lanes(xl, c)].astype(F32).T

        span(add_across, count(s - 3), count(s - 2))
        span(add_twin, count(s - 2), count(s - 1))
        span(multiply, count(s - 1), count(s))
        serve_p(s, 1)

        @pl.when(s >= 3)
        def _():
            use_v(s - 3)

        return carry

    lax.fori_loop(1, layers, step, 0)
    span(multiply, layers - 1, layers)
    span(add_twin, layers - 2, layers)
    span(add_across, layers - 3, layers)

    for u in range(SUB):
        for k in range(2):
            p_swap(u, k, xl).wait_send()
    for n in range(3):
        w_swap(n, xl).wait_send()
    for t in range(2):
        w_twin(t, c).wait_send()

    def sent_p(s, carry):
        for t in range(2):
            for upward in (True, False):
                for u in range(SUB):
                    ring_p(s, t, upward, u)(s).wait_send()
        return carry

    lax.fori_loop(0, layers - 1, sent_p, 0)

    def put_done(s, carry):
        for t in range(2):
            for k in range(2):
                put_chunk(s, t, k == 0).wait()
                put_sum(s, t, k).wait()
        return carry

    lax.fori_loop(0, layers, put_done, 0)
    def sent_h(s):
        for xq in range(2):
            h_twin(s, xq).wait_send()
        h_across(s).wait_send()

    span(sent_h, 0, layers)
    for s in range(v_up):
        ring_v(s, True)(s).wait_send()
    for s in range(v_down):
        ring_v(s, False)(s).wait_send()
    for s in range(v_up + 1):
        for d in range(2):
            if d == 0 or 1 <= s <= v_down:
                for n in range(4):
                    put_layer(s, d, n).wait()
                v_across(s, d, xl).wait_send()
                v_twin(s, d, xl, 0, c).wait_send()
                v_twin(s, d, other, 1, c).wait_send()


def main(counts, token_pos, v, wo, wi, bi, lm, gain, bias, layers):
    rows, width = lm.shape
    quarter = width // 2
    own = wo.shape[0]
    unit = own // 2
    hid = 2 * own
    tokens = token_pos.shape[1]
    features = v.shape[1]
    layer_rows = 4 * v.shape[0]
    chunk = rows // 2
    places = layers * 2 * rows
    shapes = [
        ((places, quarter), BF16),
        ((tokens, hid), BF16),
        ((tokens, unit), F32),
        ((tokens, features), BF16),
        ((tokens, features), BF16),
        ((places, unit), F32),
    ]
    outs = [jax.ShapeDtypeStruct(*shape) for shape in shapes]
    outs += [jax.ShapeDtypeStruct((unit, features), F32), jax.ShapeDtypeStruct((width // 128, 128), F32)]
    scratch = [
        pltpu.VMEM((places, quarter), BF16),
        pltpu.VMEM((layers, 2, 2, *v.shape), BF16),
        pltpu.VMEM((hid, quarter), BF16),
        pltpu.VMEM((features, hid), BF16),
        pltpu.VMEM((2, *bi.shape), F32),
        pltpu.VMEM((layers, 4, chunk, hid), F32),
        pltpu.VMEM((layers, 2, 4, chunk, unit), F32),
        pltpu.VMEM((layers, 4, chunk, unit), BF16),
        pltpu.VMEM((layers, 4, chunk, unit), BF16),
        pltpu.VMEM((places, unit), F32),
        pltpu.VMEM((tokens, features), BF16),
        pltpu.VMEM((tokens, features), BF16),
        pltpu.VMEM((tokens, hid), BF16),
        pltpu.VMEM((tokens, unit), F32),
        pltpu.VMEM((layer_rows, hid), F32),
        pltpu.VMEM((layer_rows, features), F32),
        pltpu.VMEM((rows, width), BF16),
    ]
    half = layers // 2
    sems = [(half,), (half - 1,), (2, half + 1), (2, 2, half + 1), (layers - 1, 2, SUB), (layers - 1, 2, SUB), (SUB, 2), (3,), (2,)]
    sems += [(layers, 2), (layers,)]
    for shape in sems:
        scratch += [DMA(shape), DMA(shape)]
    scratch += [DMA((7,)), DMA((layers, 2, 2)), DMA((half + 1, 2, 4)), DMA((layers, 2, 2))]
    specs = [SMEM] * 2 + [ANY] * 5 + [VMEM] * 2, [ANY] * 6 + [VMEM] * 2
    return call(main_kernel, outs, scratch, 0, (counts, token_pos, v, wo, wi, bi, lm, gain, bias), 1 << 34, specs)


def product_kernel(
    counts, token_pos, grads, hid, slope, nrm, nin, hg, turned, b_out,
    w_out_part, w_in_part, vec,
    pw, hv, hw, sv, rv, nv, acc, shift, pgs, got, got_p, got_h,
):
    starts = image_starts(counts, token_pos)
    size = PATCH + 8
    places = grads.shape[0]
    windows, sums, bases, lows = [], [], [], []
    for i, start in enumerate(starts):
        base = jnp.minimum((start // 16) * 16, places - WINDOW)
        low = jnp.minimum((start // 8) * 8, places - size)
        bases.append(base)
        lows.append(low)
        windows.append(
            pltpu.make_async_copy(grads.at[pl.ds(pl.multiple_of(base, 16), WINDOW)], pw.at[i], got_p.at[i])
        )
        sums.append(pltpu.make_async_copy(hg.at[pl.ds(pl.multiple_of(low, 8), size)], hw.at[i], got_h.at[i]))
    others = [pltpu.make_async_copy(a, b, got.at[n]) for n, (a, b) in enumerate(((hid, hv), (slope, sv), (nin, rv), (nrm, nv)))]
    for copy in [others[0], windows[0], others[1]] + sums + windows[1:] + others[2:]:
        copy.start()
    shift[PATCH:, :] = jnp.zeros((WINDOW - PATCH, shift.shape[1]), F32)
    vec[16:32, :] = b_out[...]
    vec[33:40, :] = jnp.zeros((7, 128), F32)
    others[0].wait()
    for i, start in enumerate(starts):
        shift[0:PATCH, :] = hv[i * PATCH : (i + 1) * PATCH, :].astype(F32)
        left = pltpu.roll(shift[...], start - bases[i], 0).astype(BF16)
        windows[i].wait()
        product = contract(left, pw[i], 0, 0)
        acc[...] = product if i == 0 else acc[...] + product
    w_out_part[...] = acc[...].astype(BF16)
    unit = sv.shape[1]
    total = jnp.zeros((1, unit), F32)
    others[1].wait()
    for i, start in enumerate(starts):
        r = slice(i * PATCH, (i + 1) * PATCH)
        sums[i].wait()
        back = jnp.where(start == lows[i], 0, size - (start - lows[i]))
        window = pltpu.roll(hw[i], back, 0)[0:PATCH]
        pg = (window * sv[r, :]).astype(BF16)
        pgs[r, :] = pg
        total = total + jnp.sum(pg.astype(F32), axis=0, keepdims=True)
    vec[32:33, :] = total
    others[2].wait()
    w_in_part[...] = contract(pgs[...], rv[...], 0, 0).T.astype(BF16)
    others[3].wait()
    moment = contract(pgs[...], nv[...], 0, 0)
    column = contract(pgs[...], jnp.ones((pgs.shape[0], 128), BF16), 0, 0)
    for j in range(nv.shape[1] // 128):
        at = slice(j * 128, (j + 1) * 128)
        vec[j : j + 1, :] = jnp.sum(moment[:, at] * turned[:, at], axis=0, keepdims=True)
        vec[8 + j : 9 + j, :] = jnp.sum(column * turned[:, at], axis=0, keepdims=True)


def products(counts, token_pos, grads, hid, slope, nrm, nin, hg, turned, b_out):
    images = token_pos.shape[1] // PATCH
    features, unit, quarter = nrm.shape[1], hg.shape[1], grads.shape[1]
    width = hid.shape[1]
    outs = (
        jax.ShapeDtypeStruct((width, quarter), BF16),
        jax.ShapeDtypeStruct((features, unit), BF16),
        jax.ShapeDtypeStruct((40, 128), F32),
    )
    scratch = [
        pltpu.VMEM((images, WINDOW, quarter), BF16),
        pltpu.VMEM(hid.shape, BF16),
        pltpu.VMEM((images, PATCH + 8, unit), F32),
        pltpu.VMEM(slope.shape, F32),
        pltpu.VMEM(nin.shape, BF16),
        pltpu.VMEM(nrm.shape, BF16),
        pltpu.VMEM((width, quarter), F32),
        pltpu.VMEM((WINDOW, width), F32),
        pltpu.VMEM(slope.shape, BF16),
        DMA((4,)),
        DMA((images,)),
        DMA((images,)),
    ]
    specs = [SMEM] * 2 + [ANY] * 6 + [VMEM] * 2, [VMEM] * 3
    return call(product_kernel, outs, scratch, None, (counts, token_pos, grads, hid, slope, nrm, nin, hg, turned, b_out), 1 << 34, specs)


def last_kernel(
    wo, wi, vec, w_out, w_in, gain, bias, b_out, b_in,
    ry1, s1, rx1, rx2, s2, ry2, ri, v1, t1, v2, t2, v3,
    y1_s, y1_r, x1_s, x1_r, x2_s, x2_r, y2_s, y2_r, i_s, i_r, a_s, a_r, b_s, b_r, d_s, d_r,
):
    layers, ny = v3.shape[0], wi.shape[0]
    z, xl, c = lax.axis_index("seq_0"), lax.axis_index("seq_1"), lax.axis_index("fsdp")
    y, xh = lax.axis_index("img_0"), lax.axis_index("img_1")

    def flip(me, bit):
        return 1 - me if bit else me

    plane = []
    for dy in range(ny):
        for dx in range(2):
            for dc in range(2):
                if (dy, dx, dc) != (0, 0, 0):
                    plane.append((dy, dx, dc))
    plane_ids = [((y + dy) % ny, flip(xh, dx), flip(c, dc)) for dy, dx, dc in plane]
    plane_dev = [{"img_0": a, "img_1": b, "fsdp": d} for a, b, d in plane_ids]
    side_dev = [{"seq_1": 1 - xl}, {"seq_1": 1 - xl, "img_1": 1 - xh}]
    corner = {"seq_1": 1 - xl, "fsdp": 1 - c}
    stack = [{"seq_0": (z + k) % layers} for k in range(1, layers)]
    greet(plane_dev + side_dev + [corner] + stack)
    ys = [{"img_0": (y + k) % ny} for k in range(1, ny)]
    started = []

    def go(copy):
        copy.start()
        started.append(copy)
        return copy

    stage_a = []
    for n, (dy, dx, dc) in enumerate(plane):
        if dc == 0:
            k = len(stage_a)
            stage_a.append(go(remote(vec, v1.at[k], a_s.at[k], a_r.at[k], plane_dev[n])))
    half = ry1.shape[4]
    left, right = pl.ds(0, half), pl.ds(half, half)
    across = [(1 - xl, xh), (1 - xl, 1 - xh), (xl, 1 - xh)]
    across_dev = side_dev + [{"img_1": 1 - xh}]
    x_first, y_first = [], []
    for m, (p, h) in enumerate(across):
        x_first.append(go(remote(wo.at[p, :, h, :, right], rx2.at[m], x2_s.at[m], x2_r.at[m], across_dev[m])))
    for k in range(ny - 1):
        source = wo.at[:, (y + k + 1) % ny, :, :, left]
        y_first.append(go(remote(source, ry1.at[k], y1_s.at[k], y1_r.at[k], ys[k])))
    ins = []
    for n, (dy, dx, dc) in enumerate(plane):
        a, b, d = plane_ids[n]
        ins.append((go(remote(wi.at[a, b, d], ri.at[n], i_s.at[n], i_r.at[n], plane_dev[n])), n, dc))
    total = vec[...]
    for k, copy in enumerate(stage_a):
        copy.wait_recv()
        total = total + v1[k]
    t1[...] = total
    q = xl * 2 + c
    stage_b = []
    for k, (dx, dc) in enumerate(((0, 1), (1, 0), (1, 1))):
        device = {"seq_1": flip(xl, dx), "fsdp": flip(c, dc)}
        stage_b.append(go(remote(t1, v2.at[q], b_s.at[k], b_r.at[k], device)))
    v2[q] = total
    summed = wo[:, y, :, :, 0:half].astype(F32)
    for k, copy in enumerate(y_first):
        copy.wait_recv()
        summed = summed + ry1[k].astype(F32)
    s1[...] = summed.astype(BF16)
    x_second = []
    for m, (p, h) in enumerate(across):
        x_second.append(go(remote(s1.at[p, h], rx1.at[m], x1_s.at[m], x1_r.at[m], across_dev[m])))
    for copy in x_first:
        copy.wait_recv()
    s2[0] = (wo[xl, :, xh, :, half:].astype(F32) + rx2[2].astype(F32)).astype(BF16)
    s2[1] = (rx2[0].astype(F32) + rx2[1].astype(F32)).astype(BF16)
    y_second = []
    for k in range(ny - 1):
        y_second.append(
            go(remote(s2.at[:, (y + k + 1) % ny], ry2.at[k], y2_s.at[k], y2_r.at[k], ys[k]))
        )
    for copy in stage_b:
        copy.wait_recv()
    t2[0:16] = v2[0, 0:16] + v2[1, 0:16] + v2[2, 0:16] + v2[3, 0:16]
    t2[16:32] = v2[0, 16:32] + v2[2, 16:32]
    t2[32:48] = v2[1, 16:32] + v2[3, 16:32]
    for j in range(4):
        t2[48 + j : 49 + j] = v2[j, 32:33]
    t2[52:56] = jnp.zeros((4, 128), F32)
    stage_d = []
    for k in range(1, layers):
        stage_d.append(go(remote(t2, v3.at[z], d_s.at[k - 1], d_r.at[k - 1], stack[k - 1])))
    v3[z] = t2[...]

    same = wi[y, xh, c].astype(F32)
    cross = jnp.zeros_like(same)
    for copy, n, dc in ins:
        copy.wait_recv()
        if dc:
            cross = cross + ri[n].astype(F32)
        else:
            same = same + ri[n].astype(F32)
    width = same.shape[1]
    w_in[:, pl.ds(pl.multiple_of(c * width, 128), width)] = same
    w_in[:, pl.ds(pl.multiple_of((1 - c) * width, 128), width)] = cross
    for copy in x_second:
        copy.wait_recv()
    near = s1[xl, xh].astype(F32) + rx1[2].astype(F32)
    far = rx1[0].astype(F32) + rx1[1].astype(F32)
    near_at = pl.multiple_of(2 * half * xl, 128)
    far_at = pl.multiple_of(2 * half * (1 - xl), 128)
    w_out[:, pl.ds(near_at, half)] = near
    w_out[:, pl.ds(far_at, half)] = far
    near, far = s2[0, y].astype(F32), s2[1, y].astype(F32)
    for k, copy in enumerate(y_second):
        copy.wait_recv()
        near = near + ry2[k, 0].astype(F32)
        far = far + ry2[k, 1].astype(F32)
    w_out[:, pl.ds(near_at + half, half)] = near
    w_out[:, pl.ds(far_at + half, half)] = far

    for copy in stage_d:
        copy.wait_recv()
    total = v3[0]
    for j in range(1, layers):
        total = total + v3[j]
    gain[...] = total[0:8]
    bias[...] = total[8:16]
    b_out[...] = total[16:48]
    for j in range(layers):
        b_in[4 * j : 4 * j + 4, :] = v3[j, 48:52]
    for copy in started:
        copy.wait_send()


def last(wo, wi, vec, layers):
    ny = wi.shape[0]
    members = ny * 4 - 1
    block = wi.shape[3:]
    rows, half = wo.shape[3], wo.shape[4] // 2
    outs = (
        jax.ShapeDtypeStruct((rows, 4 * half), F32),
        jax.ShapeDtypeStruct((block[0], 2 * block[1]), F32),
        jax.ShapeDtypeStruct((8, 128), F32),
        jax.ShapeDtypeStruct((8, 128), F32),
        jax.ShapeDtypeStruct((32, 128), F32),
        jax.ShapeDtypeStruct((4 * layers, 128), F32),
    )
    scratch = [
        pltpu.VMEM((ny - 1, 2, 2, rows, half), BF16),
        pltpu.VMEM((2, 2, rows, half), BF16),
        pltpu.VMEM((3, rows, half), BF16),
        pltpu.VMEM((3, ny, rows, half), BF16),
        pltpu.VMEM((2, ny, rows, half), BF16),
        pltpu.VMEM((ny - 1, 2, rows, half), BF16),
        pltpu.VMEM((members, *block), BF16),
        pltpu.VMEM((2 * ny - 1, 40, 128), F32),
        pltpu.VMEM((40, 128), F32),
        pltpu.VMEM((4, 40, 128), F32),
        pltpu.VMEM((56, 128), F32),
        pltpu.VMEM((layers, 56, 128), F32),
    ]
    for n in (ny - 1, 3, 3, ny - 1, members, 2 * ny - 1, 3, layers - 1):
        scratch += [DMA((n,)), DMA((n,))]
    return call(last_kernel, outs, scratch, 1, (wo, wi, vec), 1 << 32)


def copy_kernel(*refs):
    count = len(refs) // 2
    for source, target in zip(refs[:count], refs[count:]):
        target[...] = source[...]


def result_of(arrays):
    outs = [jax.ShapeDtypeStruct(a.shape, a.dtype) for a in arrays]
    return call(copy_kernel, outs, [], None, arrays, 1 << 20)


def per_device(vision_feats, ln_gain, ln_bias, w_in, b_in, w_out, lm_grad, image_counts, token_pos):
    layers, ny = lax.axis_size("seq_0"), lax.axis_size("img_0")
    pieces = main(
        image_counts,
        token_pos,
        vision_feats[0],
        w_out,
        w_in,
        b_in.reshape(2, -1),
        lm_grad[0],
        ln_gain[None],
        ln_bias[None],
        layers,
    )
    w_out_part, w_in_part, vec = products(image_counts, token_pos, *pieces)
    quarter, unit = w_out_part.shape[1], w_in_part.shape[1]
    sums = last(w_out_part.reshape(2, ny, 2, -1, quarter), w_in_part.reshape(ny, 2, 2, -1, unit), vec, layers)
    w_out_grad, w_in_grad, gain, bias, b_out, b_in_grad = result_of(sums)
    return (w_in_grad, b_in_grad.reshape(-1), w_out_grad, b_out.reshape(-1), gain.reshape(-1), bias.reshape(-1))


def solution(mesh):
    finer = Mesh(
        mesh.devices.reshape(8, 2, 4, 2, mesh.shape["fsdp"]),
        ("seq_0", "seq_1", "img_0", "img_1", "fsdp"),
    )
    placed = (
        P(IMG, SEQ_FSDP, None),
        P(),
        P(),
        P("fsdp", SEQ),
        P(SEQ),
        P(SEQ, "fsdp"),
        P(IMG, SEQ, "fsdp"),
        P(IMG, None),
        P(IMG, None),
    )
    return jax.shard_map(
        per_device,
        mesh=finer,
        in_specs=placed,
        out_specs=(P(IMG_FSDP, SEQ), P(), P(SEQ_IMG, "fsdp"), P(), P(), P()),
        check_vma=False,
    )
```

```python
import jax
import jax.numpy as jnp
from jax import lax
from jax.experimental import pallas as pl
from jax.experimental.pallas import tpu as pltpu
from jax.sharding import Mesh
from jax.sharding import PartitionSpec as P

PATCH = 576
LEN = 2048
SEQ = ("seq_0", "seq_1")
IMG = ("img_0", "img_1")
SEQ_FSDP = ("seq_0", "seq_1", "fsdp")
IMG_FSDP = ("img_0", "img_1", "fsdp")
SEQ_IMG = ("seq_0", "seq_1", "img_0", "img_1")
MESH = pl.DeviceIdType.MESH
BF16 = jnp.bfloat16
F32 = jnp.float32
VMEM = pl.BlockSpec(memory_space=pltpu.VMEM)
SMEM = pl.BlockSpec(memory_space=pltpu.SMEM)
ANY = pl.BlockSpec(memory_space=pl.ANY)
DMA = pltpu.SemaphoreType.DMA
LIMIT = 63 * 1024 * 1024
WINDOW = 640
SUB = 2


def remote(src, dst, send, recv, device):
    return pltpu.make_async_remote_copy(
        src_ref=src, dst_ref=dst, send_sem=send, recv_sem=recv, device_id=device, device_id_type=MESH
    )


def signal(devices):
    barrier = pltpu.get_barrier_semaphore()
    for device in devices:
        pl.semaphore_signal(barrier, inc=1, device_id=device, device_id_type=MESH)


def greet(devices):
    signal(devices)
    pl.semaphore_wait(pltpu.get_barrier_semaphore(), len(devices))


def call(kernel, outs, scratch, number, args, flops, specs=None):
    ins, results = specs or ([VMEM] * len(args), [VMEM] * len(outs))
    return pl.pallas_call(
        kernel,
        out_shape=tuple(outs),
        in_specs=ins,
        out_specs=tuple(results),
        scratch_shapes=scratch,
        compiler_params=pltpu.CompilerParams(
            collective_id=number, has_side_effects=number is not None, vmem_limit_bytes=LIMIT
        ),
        cost_estimate=pl.CostEstimate(flops=flops, bytes_accessed=1 << 20, transcendentals=0),
    )(*args)


def gelu_parts(preact):
    cumul = 0.5 * (1.0 + lax.erf(preact * 0.7071067811865476))
    density = jnp.exp(-0.5 * preact * preact) * 0.3989422804014327
    return (preact * cumul, cumul + preact * density)


def contract(left, right, left_dim, right_dim):
    return lax.dot_general(left, right, (((left_dim,), (right_dim,)), ((), ())), preferred_element_type=F32)


def image_starts(counts, token_pos):
    images = token_pos.shape[1] // PATCH
    return [jnp.where(counts[0, 0] <= i, LEN, 0) + token_pos[0, i * PATCH] for i in range(images)]


def main_kernel(
    counts, token_pos, v, wo, wi, bi, lm, gain, bias,
    grads_out, hid_out, slope_out, nrm_out, nin_out, hg_out, turned, b_out,
    grads, vs, wq, wis, bis, mine, r1, give, r2, hg, nrm, nin, hid, slope, pre, nf, held,
    vu_s, vu_r, vd_s, vd_r, vh_s, vh_r, vx_s, vx_r, vc_s, vc_r,
    pu_s, pu_r, pd_s, pd_r, px_s, px_r, wx_s, wx_r, wc_s, wc_r,
    h1_s, h1_r, h2_s, h2_r, local, put_p, put_v, put_h,
):
    layers = vs.shape[0]
    block_rows = lm.shape[0]
    chunk = block_rows // 2
    quarter = grads.shape[1]
    own_hid = wo.shape[0]
    unit = own_hid // 2
    layer_rows = 4 * v.shape[0]
    z, xl, c = lax.axis_index("seq_0"), lax.axis_index("seq_1"), lax.axis_index("fsdp")
    other, peer = 1 - xl, 1 - c
    up, down = {"seq_0": (z + 1) % layers}, {"seq_0": (z + layers - 1) % layers}
    across, twin = {"seq_1": other}, {"fsdp": peer}
    mine_cols = pl.ds(pl.multiple_of(xl * quarter, 128), quarter)
    their_cols = pl.ds(pl.multiple_of(other * quarter, 128), quarter)

    def below(s):
        return (z + layers - s) % layers

    def above(s):
        return (z + s) % layers

    def rows(zb, xq, k):
        return pl.ds(pl.multiple_of((zb * 2 + xq) * block_rows + k * chunk, 128), chunk)

    def ring_p(s, t, upward, u):
        xq = xl if t == 0 else other
        size = chunk // SUB
        zb, k = (below(s), 0) if upward else (above(s), 1)
        r = pl.ds(pl.multiple_of((zb * 2 + xq) * block_rows + k * chunk + u * size, 16), size)
        if upward:
            return lambda n: remote(grads.at[r], grads.at[r], pu_s.at[n, t, u], pu_r.at[n, t, u], up)
        return lambda n: remote(grads.at[r], grads.at[r], pd_s.at[n, t, u], pd_r.at[n, t, u], down)

    def ring_v(s, upward):
        zb = below(s) if upward else above(s)
        ref = vs.at[zb, xl, c]
        if upward:
            return lambda n: remote(ref, ref, vu_s.at[n], vu_r.at[n], up)
        return lambda n: remote(ref, ref, vd_s.at[n], vd_r.at[n], down)

    def v_across(s, d, xq):
        ref = vs.at[below(s) if d == 0 else above(s), xq, c]
        return remote(ref, ref, vx_s.at[d, s], vx_r.at[d, s], across)

    def v_twin(s, d, xq, t, cq):
        ref = vs.at[below(s) if d == 0 else above(s), xq, cq]
        return remote(ref, ref, vc_s.at[t, d, s], vc_r.at[t, d, s], twin)

    def p_swap(u, k, xq):
        size = chunk // SUB
        r = pl.ds(pl.multiple_of((z * 2 + xq) * block_rows + k * chunk + u * size, 16), size)
        source = lm.at[pl.ds(k * chunk + u * size, size), their_cols]
        return remote(source, grads.at[r], px_s.at[u, k], px_r.at[u, k], across)

    def w_in_at(cq, xq):
        size = wi.shape[0]
        return wis.at[pl.ds(pl.multiple_of(cq * size, 128), size), pl.ds(pl.multiple_of(xq * own_hid, 128), own_hid)]

    def w_out_at(xq):
        return wq.at[pl.ds(pl.multiple_of(xq * own_hid, 128), own_hid)]

    def w_swap(n, xq):
        source = (wo.at[:, their_cols], wi, bi)[n]
        target = (w_out_at(xq), w_in_at(c, xq), bis.at[xq])[n]
        return remote(source, target, wx_s.at[n], wx_r.at[n], across)

    def w_twin(t, cq):
        ref = w_in_at(cq, xl if t == 0 else other)
        return remote(ref, ref, wc_s.at[t], wc_r.at[t], twin)

    def lanes(xq, cq):
        return pl.ds(pl.multiple_of((xq * 2 + cq) * unit, 128), unit)

    def h_twin(s, xq):
        return remote(mine.at[s, :, :, lanes(xq, peer)], r1.at[s, xq], h1_s.at[s, xq], h1_r.at[s, xq], twin)

    def h_across(s):
        return remote(give.at[s], r2.at[s], h2_s.at[s], h2_r.at[s], across)

    signal([up, down, across, twin])
    locals_ = [
        pltpu.make_async_copy(v, vs.at[z, xl, c], local.at[2]),
        pltpu.make_async_copy(lm.at[pl.ds(0, chunk), mine_cols], grads.at[rows(z, xl, 0)], local.at[0]),
        pltpu.make_async_copy(lm.at[pl.ds(chunk, chunk), mine_cols], grads.at[rows(z, xl, 1)], local.at[1]),
        pltpu.make_async_copy(wi, w_in_at(c, xl), local.at[4]),
        pltpu.make_async_copy(wo.at[:, mine_cols], w_out_at(xl), local.at[3]),
        pltpu.make_async_copy(bi, bis.at[xl], local.at[5]),
        pltpu.make_async_copy(lm, held, local.at[6]),
    ]
    for copy in locals_:
        copy.start()
    pl.semaphore_wait(pltpu.get_barrier_semaphore(), 4)
    for u in range(SUB):
        for k in range(2):
            p_swap(u, k, xl).start()
    locals_[0].wait()
    ring_v(0, True)(0).start()
    ring_v(0, False)(0).start()
    for copy in locals_[1:3]:
        copy.wait()
    for u in range(SUB):
        ring_p(0, 0, True, u)(0).start()
        ring_p(0, 0, False, u)(0).start()
    v_across(0, 0, xl).start()
    for n in (1, 2, 0):
        w_swap(n, xl).start()
    v_twin(0, 0, xl, 0, c).start()
    for copy in locals_[3:6]:
        copy.wait()
    w_twin(0, c).start()

    def put_chunk(s, t, upward):
        r = rows(below(s) if upward else above(s), xl if t == 0 else other, 0 if upward else 1)
        return pltpu.make_async_copy(grads.at[r], grads_out.at[r], put_p.at[s, t, 0 if upward else 1])

    def put_layer(s, d, n):
        r = pl.ds(pl.multiple_of((below(s) if d == 0 else above(s)) * layer_rows, 32), layer_rows)
        source = (hid, slope, nrm, nin)[n]
        target = (hid_out, slope_out, nrm_out, nin_out)[n]
        return pltpu.make_async_copy(source.at[r], target.at[r], put_v.at[s, d, n])

    def put_sum(s, xq, k):
        r = rows(below(s) if k == 0 else above(s), xq, k)
        return pltpu.make_async_copy(hg.at[r], hg_out.at[r], put_h.at[s, xq, k])

    for u in range(SUB):
        p_swap(u, 0, other).wait_recv()
        ring_p(0, 1, True, u)(0).start()
        p_swap(u, 1, other).wait_recv()
        ring_p(0, 1, False, u)(0).start()
    for t in range(2):
        put_chunk(0, t, True).start()
        put_chunk(0, t, False).start()
    locals_[6].wait()
    starts = image_starts(counts, token_pos)
    here = (z * 2 + xl) * block_rows + lax.broadcasted_iota(jnp.int32, (block_rows, 1), 0)
    taken = jnp.zeros((block_rows, 1), F32)
    for start in starts:
        taken = taken + jnp.where((here >= start) & (here < start + PATCH), 1.0, 0.0)
    for j in range(lm.shape[1] // 128):
        column = held[:, j * 128 : (j + 1) * 128].astype(F32) * taken
        b_out[j : j + 1, :] = jnp.sum(column, axis=0, keepdims=True)
    def multiply(s):
        for xq in range(2):
            for k in range(2):
                r = rows(below(s) if k == 0 else above(s), xq, k)
                mine[s, xq * 2 + k] = contract(grads[r, :], wq[...], 1, 1)
        for xq in range(2):
            h_twin(s, xq).start()

    def add_twin(s):
        for xq in range(2):
            h_twin(s, xq).wait_recv()
        give[s] = (mine[s, :, :, lanes(other, c)] + r1[s, other]).astype(BF16)
        h_across(s).start()
        for xq in range(2):
            for k in range(2):
                r = rows(below(s) if k == 0 else above(s), xq, k)
                n = xq * 2 + k
                hg[r, :] = mine[s, n, :, lanes(xl, c)] + r1[s, xl, n]

    def add_across(s):
        h_across(s).wait_recv()
        for xq in range(2):
            for k in range(2):
                r = rows(below(s) if k == 0 else above(s), xq, k)
                hg[r, :] = hg[r, :] + r2[s, xq * 2 + k].astype(F32)
                put_sum(s, xq, k).start()

    def span(body, lo, hi):
        def step(s, carry):
            body(s)
            return carry

        lax.fori_loop(lo, hi, step, 0)

    def normalise(zb):
        for n in range(4):
            values = vs[zb, n // 2, n % 2].astype(F32)
            mean = jnp.mean(values, axis=1, keepdims=True)
            centred = values - mean
            var = jnp.mean(centred * centred, axis=1, keepdims=True)
            size = values.shape[0]
            nf[n * size : (n + 1) * size, :] = centred * lax.rsqrt(var + 1e-05)
        r = pl.ds(pl.multiple_of(zb * layer_rows, 32), layer_rows)
        normed = nf[...]
        nrm[r, :] = normed.astype(BF16)
        nin[r, :] = (normed * gain[...] + bias[...]).astype(BF16)
        pre[...] = contract(nin[r, :], wis[...], 1, 0)
        for xq in range(2):
            for half in range(2):
                at = xq * own_hid + half * unit
                pre[:, at : at + unit] = pre[:, at : at + unit] + bis[xq, half : half + 1, :]
        hid[r, :] = gelu_parts(pre[...])[0].astype(BF16)
        slope[r, :] = gelu_parts(pre[:, lanes(xl, c)])[1]

    v_up, v_down = layers // 2, layers // 2 - 1

    def half_v(s, upward):
        size = vs.shape[4] // 2
        if upward:
            ref = vs.at[below(s), xl, c, :, pl.ds(0, size)]
            return remote(ref, ref, vh_s.at[0], vh_r.at[0], up)
        ref = vs.at[above(s), xl, c, :, pl.ds(size, size)]
        return remote(ref, ref, vh_s.at[1], vh_r.at[1], down)

    def serve_v(s):
        for d, upward in enumerate((True, False)):

            @pl.when(s <= v_down)
            def _():
                ring_v(s, upward)(s - 1).wait_recv()

                @pl.when(s < v_down)
                def _():
                    ring_v(s, upward)(s).start()

                @pl.when(s == v_down)
                def _():
                    half_v(s, upward).start()

                v_across(s, d, xl).start()
                v_twin(s, d, xl, 0, c).start()

        @pl.when(s == v_up)
        def _():
            half_v(s, True).wait_recv()
            half_v(s, False).wait_recv()
            v_across(s, 0, xl).start()
            v_twin(s, 0, xl, 0, c).start()

        @pl.when((s >= 2) & (s - 2 <= v_up))
        def _():
            v_across(s - 2, 0, other).wait_recv()
            v_twin(s - 2, 0, other, 1, c).start()

        @pl.when((s >= 3) & (s - 2 <= v_down))
        def _():
            v_across(s - 2, 1, other).wait_recv()
            v_twin(s - 2, 1, other, 1, c).start()

    def serve_p(s, t):
        for u in range(SUB):
            for upward in (True, False):
                ring_p(s, t, upward, u)(s - 1).wait_recv()

                @pl.when(s < layers - 1)
                def _():
                    ring_p(s, t, upward, u)(s).start()

        for upward in (True, False):
            put_chunk(s, t, upward).start()

    def use_v(s):
        @pl.when(s <= v_up)
        def _():
            v_twin(s, 0, xl, 0, peer).wait_recv()
            v_twin(s, 0, other, 1, peer).wait_recv()
            normalise(below(s))
            for n in range(4):
                put_layer(s, 0, n).start()

        @pl.when((s >= 1) & (s <= v_down))
        def _():
            v_twin(s, 1, xl, 0, peer).wait_recv()
            v_twin(s, 1, other, 1, peer).wait_recv()
            normalise(above(s))
            for n in range(4):
                put_layer(s, 1, n).start()

    def count(s):
        return jnp.maximum(jnp.minimum(2 * s - 4, s), 0)

    def step(s, carry):
        serve_v(s)
        serve_p(s, 0)

        @pl.when(s == 2)
        def _():
            w_swap(1, other).wait_recv()
            w_twin(1, c).start()

        @pl.when(s == 3)
        def _():
            w_swap(0, other).wait_recv()
            w_swap(2, other).wait_recv()
            for t in range(2):
                w_twin(t, peer).wait_recv()
            turned[...] = wis[:, lanes(xl, c)].astype(F32).T

        span(add_across, count(s - 3), count(s - 2))
        span(add_twin, count(s - 2), count(s - 1))
        span(multiply, count(s - 1), count(s))
        serve_p(s, 1)

        @pl.when(s >= 3)
        def _():
            use_v(s - 3)

        return carry

    lax.fori_loop(1, layers, step, 0)
    span(multiply, layers - 1, layers)
    span(add_twin, layers - 2, layers)
    span(add_across, layers - 3, layers)

    for u in range(SUB):
        for k in range(2):
            p_swap(u, k, xl).wait_send()
    for n in range(3):
        w_swap(n, xl).wait_send()
    for t in range(2):
        w_twin(t, c).wait_send()

    def sent_p(s, carry):
        for t in range(2):
            for upward in (True, False):
                for u in range(SUB):
                    ring_p(s, t, upward, u)(s).wait_send()
        return carry

    lax.fori_loop(0, layers - 1, sent_p, 0)

    def put_done(s, carry):
        for t in range(2):
            for k in range(2):
                put_chunk(s, t, k == 0).wait()
                put_sum(s, t, k).wait()
        return carry

    lax.fori_loop(0, layers, put_done, 0)
    def sent_h(s):
        for xq in range(2):
            h_twin(s, xq).wait_send()
        h_across(s).wait_send()

    span(sent_h, 0, layers)
    for upward in (True, False):
        for s in range(v_down):
            ring_v(s, upward)(s).wait_send()
        half_v(v_down, upward).wait_send()
    for s in range(v_up + 1):
        for d in range(2):
            if d == 0 or 1 <= s <= v_down:
                for n in range(4):
                    put_layer(s, d, n).wait()
                v_across(s, d, xl).wait_send()
                v_twin(s, d, xl, 0, c).wait_send()
                v_twin(s, d, other, 1, c).wait_send()


def main(counts, token_pos, v, wo, wi, bi, lm, gain, bias, layers):
    rows, width = lm.shape
    quarter = width // 2
    own = wo.shape[0]
    unit = own // 2
    hid = 2 * own
    tokens = token_pos.shape[1]
    features = v.shape[1]
    layer_rows = 4 * v.shape[0]
    chunk = rows // 2
    places = layers * 2 * rows
    shapes = [
        ((places, quarter), BF16),
        ((tokens, hid), BF16),
        ((tokens, unit), F32),
        ((tokens, features), BF16),
        ((tokens, features), BF16),
        ((places, unit), F32),
    ]
    outs = [jax.ShapeDtypeStruct(*shape) for shape in shapes]
    outs += [jax.ShapeDtypeStruct((unit, features), F32), jax.ShapeDtypeStruct((width // 128, 128), F32)]
    scratch = [
        pltpu.VMEM((places, quarter), BF16),
        pltpu.VMEM((layers, 2, 2, *v.shape), BF16),
        pltpu.VMEM((hid, quarter), BF16),
        pltpu.VMEM((features, hid), BF16),
        pltpu.VMEM((2, *bi.shape), F32),
        pltpu.VMEM((layers, 4, chunk, hid), F32),
        pltpu.VMEM((layers, 2, 4, chunk, unit), F32),
        pltpu.VMEM((layers, 4, chunk, unit), BF16),
        pltpu.VMEM((layers, 4, chunk, unit), BF16),
        pltpu.VMEM((places, unit), F32),
        pltpu.VMEM((tokens, features), BF16),
        pltpu.VMEM((tokens, features), BF16),
        pltpu.VMEM((tokens, hid), BF16),
        pltpu.VMEM((tokens, unit), F32),
        pltpu.VMEM((layer_rows, hid), F32),
        pltpu.VMEM((layer_rows, features), F32),
        pltpu.VMEM((rows, width), BF16),
    ]
    half = layers // 2
    sems = [(half - 1,), (half - 1,), (2,), (2, half + 1), (2, 2, half + 1), (layers - 1, 2, SUB), (layers - 1, 2, SUB), (SUB, 2), (3,), (2,)]
    sems += [(layers, 2), (layers,)]
    for shape in sems:
        scratch += [DMA(shape), DMA(shape)]
    scratch += [DMA((7,)), DMA((layers, 2, 2)), DMA((half + 1, 2, 4)), DMA((layers, 2, 2))]
    specs = [SMEM] * 2 + [ANY] * 5 + [VMEM] * 2, [ANY] * 6 + [VMEM] * 2
    return call(main_kernel, outs, scratch, 0, (counts, token_pos, v, wo, wi, bi, lm, gain, bias), 1 << 34, specs)


def product_kernel(
    counts, token_pos, grads, hid, slope, hg,
    w_out_part, pgs, b_in,
    pw, hv, hw, sv, left, shift, got, got_p, got_h,
):
    starts = image_starts(counts, token_pos)
    size = PATCH + 8
    places = grads.shape[0]
    windows, sums, bases, lows = [], [], [], []
    for i, start in enumerate(starts):
        base = jnp.minimum((start // 16) * 16, places - WINDOW)
        low = jnp.minimum((start // 8) * 8, places - size)
        bases.append(base)
        lows.append(low)
        windows.append(
            pltpu.make_async_copy(
                grads.at[pl.ds(pl.multiple_of(base, 16), WINDOW)], pw.at[pl.ds(i * WINDOW, WINDOW)], got_p.at[i]
            )
        )
        sums.append(pltpu.make_async_copy(hg.at[pl.ds(pl.multiple_of(low, 8), size)], hw.at[i], got_h.at[i]))
    others = [pltpu.make_async_copy(a, b, got.at[n]) for n, (a, b) in enumerate(((hid, hv), (slope, sv)))]
    for copy in [others[0]] + windows + [others[1]] + sums:
        copy.start()
    shift[PATCH:, :] = jnp.zeros((WINDOW - PATCH, shift.shape[1]), F32)
    others[0].wait()
    for i, start in enumerate(starts):
        shift[0:PATCH, :] = hv[i * PATCH : (i + 1) * PATCH, :].astype(F32)
        left[i * WINDOW : (i + 1) * WINDOW, :] = pltpu.roll(shift[...], start - bases[i], 0).astype(BF16)
    for copy in windows:
        copy.wait()
    w_out_part[...] = contract(left[...], pw[...], 0, 0).astype(BF16)
    unit = sv.shape[1]
    total = jnp.zeros((1, unit), F32)
    others[1].wait()
    for i, start in enumerate(starts):
        r = slice(i * PATCH, (i + 1) * PATCH)
        sums[i].wait()
        back = jnp.where(start == lows[i], 0, size - (start - lows[i]))
        window = pltpu.roll(hw[i], back, 0)[0:PATCH]
        pg = (window * sv[r, :]).astype(BF16)
        pgs[r, :] = pg
        total = total + jnp.sum(pg.astype(F32), axis=0, keepdims=True)
    b_in[...] = total


def products(counts, token_pos, grads, hid, slope, hg):
    images = token_pos.shape[1] // PATCH
    unit, quarter = hg.shape[1], grads.shape[1]
    width = hid.shape[1]
    outs = (
        jax.ShapeDtypeStruct((width, quarter), BF16),
        jax.ShapeDtypeStruct(slope.shape, BF16),
        jax.ShapeDtypeStruct((1, unit), F32),
    )
    scratch = [
        pltpu.VMEM((images * WINDOW, quarter), BF16),
        pltpu.VMEM(hid.shape, BF16),
        pltpu.VMEM((images, PATCH + 8, unit), F32),
        pltpu.VMEM(slope.shape, F32),
        pltpu.VMEM((images * WINDOW, width), BF16),
        pltpu.VMEM((WINDOW, width), F32),
        DMA((2,)),
        DMA((images,)),
        DMA((images,)),
    ]
    specs = [SMEM] * 2 + [ANY] * 4, [VMEM] * 3
    return call(product_kernel, outs, scratch, None, (counts, token_pos, grads, hid, slope, hg), 1 << 34, specs)


def last_kernel(
    wo_all, pgs_all, turned_all, b_out_part, b_in_part, nrm, nin,
    w_out, w_in, gain, bias, b_out, b_in,
    wo, pgs, turned, nv, rv, wi, vec, got, ry1, s1, rx1, rx2, s2, ry2, ri, v1, t1, v2, t2, v3,
    y1_s, y1_r, x1_s, x1_r, x2_s, x2_r, y2_s, y2_r, i_s, i_r, a_s, a_r, b_s, b_r, d_s, d_r,
):
    layers, ny = v1.shape[0], wo.shape[1]
    z, xl, c = lax.axis_index("seq_0"), lax.axis_index("seq_1"), lax.axis_index("fsdp")
    y, xh = lax.axis_index("img_0"), lax.axis_index("img_1")

    def flip(me, bit):
        return 1 - me if bit else me

    plane = []
    for dy in range(ny):
        for dx in range(2):
            for dc in range(2):
                if (dy, dx, dc) != (0, 0, 0):
                    plane.append((dy, dx, dc))
    plane_ids = [((y + dy) % ny, flip(xh, dx), flip(c, dc)) for dy, dx, dc in plane]
    plane_dev = [{"img_0": a, "img_1": b, "fsdp": d} for a, b, d in plane_ids]
    side_dev = [{"seq_1": 1 - xl}, {"seq_1": 1 - xl, "img_1": 1 - xh}]
    corner = {"seq_1": 1 - xl, "fsdp": 1 - c}
    stack = [{"seq_0": (z + k) % layers} for k in range(1, layers)]
    signal(plane_dev + side_dev + [corner] + stack)
    pairs = ((pgs_all, pgs), (nrm, nv), (turned_all, turned), (wo_all, wo), (nin, rv))
    loads = [pltpu.make_async_copy(source, target, got.at[n]) for n, (source, target) in enumerate(pairs)]
    for copy in loads:
        copy.start()
    ys = [{"img_0": (y + k) % ny} for k in range(1, ny)]
    started = []

    def go(copy):
        copy.start()
        started.append(copy)
        return copy

    vec[16:32, :] = b_out_part[...]
    vec[32:33, :] = b_in_part[...]
    vec[33:40, :] = jnp.zeros((7, 128), F32)
    for copy in loads[:3]:
        copy.wait()
    moment = contract(pgs[...], nv[...], 0, 0)
    column = contract(pgs[...], jnp.ones((pgs.shape[0], 128), BF16), 0, 0)
    for j in range(nv.shape[1] // 128):
        at = slice(j * 128, (j + 1) * 128)
        vec[j : j + 1, :] = jnp.sum(moment[:, at] * turned[:, at], axis=0, keepdims=True)
        vec[8 + j : 9 + j, :] = jnp.sum(column * turned[:, at], axis=0, keepdims=True)
    loads[3].wait()
    pl.semaphore_wait(pltpu.get_barrier_semaphore(), len(plane_dev) + 3 + len(stack))
    stage_a = []
    for k in range(1, layers):
        stage_a.append(go(remote(vec, v1.at[z], a_s.at[k - 1], a_r.at[k - 1], stack[k - 1])))
    v1[z] = vec[...]
    half = ry1.shape[4]
    left, right = pl.ds(0, half), pl.ds(half, half)
    across = [(1 - xl, xh), (1 - xl, 1 - xh), (xl, 1 - xh)]
    across_dev = side_dev + [{"img_1": 1 - xh}]
    x_first, y_first = [], []
    for m, (p, h) in enumerate(across):
        x_first.append(go(remote(wo.at[p, :, h, :, right], rx2.at[m], x2_s.at[m], x2_r.at[m], across_dev[m])))
    for k in range(ny - 1):
        source = wo.at[:, (y + k + 1) % ny, :, :, left]
        y_first.append(go(remote(source, ry1.at[k], y1_s.at[k], y1_r.at[k], ys[k])))
    loads[4].wait()
    wi[...] = contract(pgs[...], rv[...], 0, 0).T.astype(BF16).reshape(wi.shape)
    ins = []
    for n, (dy, dx, dc) in enumerate(plane):
        a, b, d = plane_ids[n]
        ins.append((go(remote(wi.at[a, b, d], ri.at[n], i_s.at[n], i_r.at[n], plane_dev[n])), n, dc))

    for copy in stage_a:
        copy.wait_recv()
    total = v1[0, 0:32]
    for j in range(1, layers):
        total = total + v1[j, 0:32]
    t1[0:32] = total
    for j in range(layers):
        t1[32 + j : 33 + j] = v1[j, 32:33]
    stage_b = []
    for n, (dy, dx, dc) in enumerate(plane):
        if dc == 0:
            k = len(stage_b)
            stage_b.append(go(remote(t1, v2.at[k], b_s.at[k], b_r.at[k], plane_dev[n])))

    summed = wo[:, y, :, :, 0:half].astype(F32)
    for k, copy in enumerate(y_first):
        copy.wait_recv()
        summed = summed + ry1[k].astype(F32)
    s1[...] = summed.astype(BF16)
    x_second = []
    for m, (p, h) in enumerate(across):
        x_second.append(go(remote(s1.at[p, h], rx1.at[m], x1_s.at[m], x1_r.at[m], across_dev[m])))
    for copy in x_first:
        copy.wait_recv()
    s2[0] = (wo[xl, :, xh, :, half:].astype(F32) + rx2[2].astype(F32)).astype(BF16)
    s2[1] = (rx2[0].astype(F32) + rx2[1].astype(F32)).astype(BF16)
    y_second = []
    for k in range(ny - 1):
        y_second.append(
            go(remote(s2.at[:, (y + k + 1) % ny], ry2.at[k], y2_s.at[k], y2_r.at[k], ys[k]))
        )

    total = t1[...]
    for k, copy in enumerate(stage_b):
        copy.wait_recv()
        total = total + v2[k]
    t2[...] = total
    q = xl * 2 + c
    stage_d = []
    for k, (dx, dc) in enumerate(((0, 1), (1, 0), (1, 1))):
        device = {"seq_1": flip(xl, dx), "fsdp": flip(c, dc)}
        stage_d.append(go(remote(t2, v3.at[q], d_s.at[k], d_r.at[k], device)))
    v3[q] = total

    same = wi[y, xh, c].astype(F32)
    cross = jnp.zeros_like(same)
    for copy, n, dc in ins:
        copy.wait_recv()
        if dc:
            cross = cross + ri[n].astype(F32)
        else:
            same = same + ri[n].astype(F32)
    width = same.shape[1]
    w_in[:, pl.ds(pl.multiple_of(c * width, 128), width)] = same
    w_in[:, pl.ds(pl.multiple_of((1 - c) * width, 128), width)] = cross
    for copy in x_second:
        copy.wait_recv()
    near = s1[xl, xh].astype(F32) + rx1[2].astype(F32)
    far = rx1[0].astype(F32) + rx1[1].astype(F32)
    near_at = pl.multiple_of(2 * half * xl, 128)
    far_at = pl.multiple_of(2 * half * (1 - xl), 128)
    w_out[:, pl.ds(near_at, half)] = near
    w_out[:, pl.ds(far_at, half)] = far
    near, far = s2[0, y].astype(F32), s2[1, y].astype(F32)
    for k, copy in enumerate(y_second):
        copy.wait_recv()
        near = near + ry2[k, 0].astype(F32)
        far = far + ry2[k, 1].astype(F32)
    w_out[:, pl.ds(near_at + half, half)] = near
    w_out[:, pl.ds(far_at + half, half)] = far

    for copy in stage_d:
        copy.wait_recv()
    total = v3[0, 0:16] + v3[1, 0:16] + v3[2, 0:16] + v3[3, 0:16]
    gain[...] = total[0:8]
    bias[...] = total[8:16]
    b_out[0:16, :] = v3[0, 16:32] + v3[2, 16:32]
    b_out[16:32, :] = v3[1, 16:32] + v3[3, 16:32]
    for j in range(layers):
        for n in range(4):
            b_in[4 * j + n : 4 * j + n + 1, :] = v3[n, 32 + j : 33 + j]
    for copy in started:
        copy.wait_send()


def last(wo, pgs, turned, b_out, b_in, nrm, nin, layers):
    ny = wo.shape[1]
    members = ny * 4 - 1
    features, unit = nrm.shape[1], pgs.shape[1]
    block = (features // (ny * 4), unit)
    rows, half = wo.shape[3], wo.shape[4] // 2
    outs = (
        jax.ShapeDtypeStruct((rows, 4 * half), F32),
        jax.ShapeDtypeStruct((block[0], 2 * block[1]), F32),
        jax.ShapeDtypeStruct((8, 128), F32),
        jax.ShapeDtypeStruct((8, 128), F32),
        jax.ShapeDtypeStruct((32, 128), F32),
        jax.ShapeDtypeStruct((4 * layers, 128), F32),
    )
    scratch = [
        pltpu.VMEM(wo.shape, BF16),
        pltpu.VMEM(pgs.shape, BF16),
        pltpu.VMEM(turned.shape, F32),
        pltpu.VMEM(nrm.shape, BF16),
        pltpu.VMEM(nin.shape, BF16),
        pltpu.VMEM((ny, 2, 2, *block), BF16),
        pltpu.VMEM((40, 128), F32),
        DMA((5,)),
        pltpu.VMEM((ny - 1, 2, 2, rows, half), BF16),
        pltpu.VMEM((2, 2, rows, half), BF16),
        pltpu.VMEM((3, rows, half), BF16),
        pltpu.VMEM((3, ny, rows, half), BF16),
        pltpu.VMEM((2, ny, rows, half), BF16),
        pltpu.VMEM((ny - 1, 2, rows, half), BF16),
        pltpu.VMEM((members, *block), BF16),
        pltpu.VMEM((layers, 40, 128), F32),
        pltpu.VMEM((40, 128), F32),
        pltpu.VMEM((2 * ny - 1, 40, 128), F32),
        pltpu.VMEM((40, 128), F32),
        pltpu.VMEM((4, 40, 128), F32),
    ]
    for n in (ny - 1, 3, 3, ny - 1, members, layers - 1, 2 * ny - 1, 3):
        scratch += [DMA((n,)), DMA((n,))]
    specs = [ANY] * 3 + [VMEM] * 2 + [ANY] * 2, [VMEM] * 6
    return call(last_kernel, outs, scratch, 1, (wo, pgs, turned, b_out, b_in, nrm, nin), 1 << 32, specs)


def copy_kernel(*refs):
    count = len(refs) // 2
    for source, target in zip(refs[:count], refs[count:]):
        target[...] = source[...]


def result_of(arrays):
    outs = [jax.ShapeDtypeStruct(a.shape, a.dtype) for a in arrays]
    return call(copy_kernel, outs, [], None, arrays, 1 << 20)


def per_device(vision_feats, ln_gain, ln_bias, w_in, b_in, w_out, lm_grad, image_counts, token_pos):
    layers, ny = lax.axis_size("seq_0"), lax.axis_size("img_0")
    grads, hid, slope, nrm, nin, hg, turned, b_out_part = main(
        image_counts,
        token_pos,
        vision_feats[0],
        w_out,
        w_in,
        b_in.reshape(2, -1),
        lm_grad[0],
        ln_gain[None],
        ln_bias[None],
        layers,
    )
    w_out_part, pgs, b_in_part = products(image_counts, token_pos, grads, hid, slope, hg)
    quarter = w_out_part.shape[1]
    w_out_part = w_out_part.reshape(2, ny, 2, -1, quarter)
    sums = last(w_out_part, pgs, turned, b_out_part, b_in_part, nrm, nin, layers)
    w_out_grad, w_in_grad, gain, bias, b_out, b_in_grad = result_of(sums)
    return (w_in_grad, b_in_grad.reshape(-1), w_out_grad, b_out.reshape(-1), gain.reshape(-1), bias.reshape(-1))


def solution(mesh):
    finer = Mesh(
        mesh.devices.reshape(8, 2, 4, 2, mesh.shape["fsdp"]),
        ("seq_0", "seq_1", "img_0", "img_1", "fsdp"),
    )
    placed = (
        P(IMG, SEQ_FSDP, None),
        P(),
        P(),
        P("fsdp", SEQ),
        P(SEQ),
        P(SEQ, "fsdp"),
        P(IMG, SEQ, "fsdp"),
        P(IMG, None),
        P(IMG, None),
    )
    return jax.shard_map(
        per_device,
        mesh=finer,
        in_specs=placed,
        out_specs=(P(IMG_FSDP, SEQ), P(), P(SEQ_IMG, "fsdp"), P(), P(), P()),
        check_vma=False,
    )
```

```python
import jax
import jax.numpy as jnp
from jax import lax
from jax.experimental import pallas as pl
from jax.experimental.pallas import tpu as pltpu
from jax.sharding import Mesh
from jax.sharding import PartitionSpec as P

PATCH = 576
LEN = 2048
SEQ = ("seq_0", "seq_1")
IMG = ("img_0", "img_1")
SEQ_FSDP = ("seq_0", "seq_1", "fsdp")
IMG_FSDP = ("img_0", "img_1", "fsdp")
SEQ_IMG = ("seq_0", "seq_1", "img_0", "img_1")
MESH = pl.DeviceIdType.MESH
BF16 = jnp.bfloat16
F32 = jnp.float32
VMEM = pl.BlockSpec(memory_space=pltpu.VMEM)
SMEM = pl.BlockSpec(memory_space=pltpu.SMEM)
ANY = pl.BlockSpec(memory_space=pl.ANY)
DMA = pltpu.SemaphoreType.DMA
LIMIT = 63 * 1024 * 1024
WINDOW = 640
SUB = 2


def remote(src, dst, send, recv, device):
    return pltpu.make_async_remote_copy(
        src_ref=src, dst_ref=dst, send_sem=send, recv_sem=recv, device_id=device, device_id_type=MESH
    )


def signal(devices):
    barrier = pltpu.get_barrier_semaphore()
    for device in devices:
        pl.semaphore_signal(barrier, inc=1, device_id=device, device_id_type=MESH)


def greet(devices):
    signal(devices)
    pl.semaphore_wait(pltpu.get_barrier_semaphore(), len(devices))


def call(kernel, outs, scratch, number, args, flops, specs=None):
    ins, results = specs or ([VMEM] * len(args), [VMEM] * len(outs))
    return pl.pallas_call(
        kernel,
        out_shape=tuple(outs),
        in_specs=ins,
        out_specs=tuple(results),
        scratch_shapes=scratch,
        compiler_params=pltpu.CompilerParams(
            collective_id=number, has_side_effects=number is not None, vmem_limit_bytes=LIMIT
        ),
        cost_estimate=pl.CostEstimate(flops=flops, bytes_accessed=1 << 20, transcendentals=0),
    )(*args)


def gelu_parts(preact):
    cumul = 0.5 * (1.0 + lax.erf(preact * 0.7071067811865476))
    density = jnp.exp(-0.5 * preact * preact) * 0.3989422804014327
    return (preact * cumul, cumul + preact * density)


def contract(left, right, left_dim, right_dim):
    return lax.dot_general(left, right, (((left_dim,), (right_dim,)), ((), ())), preferred_element_type=F32)


def image_starts(counts, token_pos):
    images = token_pos.shape[1] // PATCH
    return [jnp.where(counts[0, 0] <= i, LEN, 0) + token_pos[0, i * PATCH] for i in range(images)]


def main_kernel(
    counts, token_pos, v, wo, wi, bi, lm, gain, bias,
    grads_out, hid_out, slope_out, nrm_out, nin_out, hg_out, turned, b_out,
    grads, vs, wq, wis, bis, mine, r1, give, r2, hg, nrm, nin, hid, slope, pre, nf, held,
    vu_s, vu_r, vd_s, vd_r, vh_s, vh_r, vx_s, vx_r, vc_s, vc_r,
    pu_s, pu_r, pd_s, pd_r, px_s, px_r, wx_s, wx_r, wc_s, wc_r,
    h1_s, h1_r, h2_s, h2_r, local, put_p, put_v, put_h,
):
    layers = vs.shape[0]
    block_rows = lm.shape[0]
    chunk = block_rows // 2
    quarter = grads.shape[1]
    own_hid = wo.shape[0]
    unit = own_hid // 2
    layer_rows = 4 * v.shape[0]
    z, xl, c = lax.axis_index("seq_0"), lax.axis_index("seq_1"), lax.axis_index("fsdp")
    other, peer = 1 - xl, 1 - c
    up, down = {"seq_0": (z + 1) % layers}, {"seq_0": (z + layers - 1) % layers}
    across, twin = {"seq_1": other}, {"fsdp": peer}
    mine_cols = pl.ds(pl.multiple_of(xl * quarter, 128), quarter)
    their_cols = pl.ds(pl.multiple_of(other * quarter, 128), quarter)

    def below(s):
        return (z + layers - s) % layers

    def above(s):
        return (z + s) % layers

    def rows(zb, xq, k):
        return pl.ds(pl.multiple_of((zb * 2 + xq) * block_rows + k * chunk, 128), chunk)

    def ring_p(s, t, upward, u):
        xq = xl if t == 0 else other
        size = chunk // SUB
        zb, k = (below(s), 0) if upward else (above(s), 1)
        r = pl.ds(pl.multiple_of((zb * 2 + xq) * block_rows + k * chunk + u * size, 16), size)
        if upward:
            return lambda n: remote(grads.at[r], grads.at[r], pu_s.at[n, t, u], pu_r.at[n, t, u], up)
        return lambda n: remote(grads.at[r], grads.at[r], pd_s.at[n, t, u], pd_r.at[n, t, u], down)

    def ring_v(s, upward):
        zb = below(s) if upward else above(s)
        ref = vs.at[zb, xl, c]
        if upward:
            return lambda n: remote(ref, ref, vu_s.at[n], vu_r.at[n], up)
        return lambda n: remote(ref, ref, vd_s.at[n], vd_r.at[n], down)

    def v_across(s, d, xq):
        ref = vs.at[below(s) if d == 0 else above(s), xq, c]
        return remote(ref, ref, vx_s.at[d, s], vx_r.at[d, s], across)

    def v_twin(s, d, xq, t, cq):
        ref = vs.at[below(s) if d == 0 else above(s), xq, cq]
        return remote(ref, ref, vc_s.at[t, d, s], vc_r.at[t, d, s], twin)

    def p_swap(u, k, xq):
        size = chunk // SUB
        r = pl.ds(pl.multiple_of((z * 2 + xq) * block_rows + k * chunk + u * size, 16), size)
        source = lm.at[pl.ds(k * chunk + u * size, size), their_cols]
        return remote(source, grads.at[r], px_s.at[u, k], px_r.at[u, k], across)

    def w_in_at(cq, xq):
        size = wi.shape[0]
        return wis.at[pl.ds(pl.multiple_of(cq * size, 128), size), pl.ds(pl.multiple_of(xq * own_hid, 128), own_hid)]

    def w_out_at(xq):
        return wq.at[pl.ds(pl.multiple_of(xq * own_hid, 128), own_hid)]

    def w_swap(n, xq):
        source = (wo.at[:, their_cols], wi, bi)[n]
        target = (w_out_at(xq), w_in_at(c, xq), bis.at[xq])[n]
        return remote(source, target, wx_s.at[n], wx_r.at[n], across)

    def w_twin(t, cq):
        ref = w_in_at(cq, xl if t == 0 else other)
        return remote(ref, ref, wc_s.at[t], wc_r.at[t], twin)

    def lanes(xq, cq):
        return pl.ds(pl.multiple_of((xq * 2 + cq) * unit, 128), unit)

    def pair(xq):
        return pl.ds(2 * xq, 2)

    def h_twin(s, xq, side):
        source = mine.at[s, pair(xq), :, lanes(side, peer)]
        return remote(source, r1.at[s, side, pair(xq)], h1_s.at[s, xq, side], h1_r.at[s, xq, side], twin)

    def h_across(s, xq):
        return remote(give.at[s, pair(xq)], r2.at[s, pair(xq)], h2_s.at[s, xq], h2_r.at[s, xq], across)

    signal([up, down, across, twin])
    locals_ = [
        pltpu.make_async_copy(v, vs.at[z, xl, c], local.at[2]),
        pltpu.make_async_copy(lm.at[pl.ds(0, chunk), mine_cols], grads.at[rows(z, xl, 0)], local.at[0]),
        pltpu.make_async_copy(lm.at[pl.ds(chunk, chunk), mine_cols], grads.at[rows(z, xl, 1)], local.at[1]),
        pltpu.make_async_copy(wi, w_in_at(c, xl), local.at[4]),
        pltpu.make_async_copy(wo.at[:, mine_cols], w_out_at(xl), local.at[3]),
        pltpu.make_async_copy(bi, bis.at[xl], local.at[5]),
        pltpu.make_async_copy(lm, held, local.at[6]),
    ]
    for copy in locals_:
        copy.start()
    pl.semaphore_wait(pltpu.get_barrier_semaphore(), 4)
    for u in range(SUB):
        for k in range(2):
            p_swap(u, k, xl).start()
    locals_[0].wait()
    ring_v(0, True)(0).start()
    ring_v(0, False)(0).start()
    for copy in locals_[1:3]:
        copy.wait()
    for u in range(SUB):
        ring_p(0, 0, True, u)(0).start()
        ring_p(0, 0, False, u)(0).start()
    v_across(0, 0, xl).start()
    for n in (1, 2, 0):
        w_swap(n, xl).start()
    v_twin(0, 0, xl, 0, c).start()
    for copy in locals_[3:6]:
        copy.wait()
    w_twin(0, c).start()

    def put_chunk(s, t, upward):
        r = rows(below(s) if upward else above(s), xl if t == 0 else other, 0 if upward else 1)
        return pltpu.make_async_copy(grads.at[r], grads_out.at[r], put_p.at[s, t, 0 if upward else 1])

    def put_layer(s, d, n):
        r = pl.ds(pl.multiple_of((below(s) if d == 0 else above(s)) * layer_rows, 32), layer_rows)
        source = (hid, slope, nrm, nin)[n]
        target = (hid_out, slope_out, nrm_out, nin_out)[n]
        return pltpu.make_async_copy(source.at[r], target.at[r], put_v.at[s, d, n])

    def put_sum(s, xq, k):
        r = rows(below(s) if k == 0 else above(s), xq, k)
        return pltpu.make_async_copy(hg.at[r], hg_out.at[r], put_h.at[s, xq, k])

    for u in range(SUB):
        p_swap(u, 0, other).wait_recv()
        ring_p(0, 1, True, u)(0).start()
        p_swap(u, 1, other).wait_recv()
        ring_p(0, 1, False, u)(0).start()
    for t in range(2):
        put_chunk(0, t, True).start()
        put_chunk(0, t, False).start()
    locals_[6].wait()
    starts = image_starts(counts, token_pos)
    here = (z * 2 + xl) * block_rows + lax.broadcasted_iota(jnp.int32, (block_rows, 1), 0)
    taken = jnp.zeros((block_rows, 1), F32)
    for start in starts:
        taken = taken + jnp.where((here >= start) & (here < start + PATCH), 1.0, 0.0)
    for j in range(lm.shape[1] // 128):
        column = held[:, j * 128 : (j + 1) * 128].astype(F32) * taken
        b_out[j : j + 1, :] = jnp.sum(column, axis=0, keepdims=True)
    def part_of(g):
        s, t = g // 2, g % 2
        return s, xl * (1 - t) + other * t

    def multiply(g):
        s, xq = part_of(g)
        for k in range(2):
            r = rows(below(s) if k == 0 else above(s), xq, k)
            mine[s, xq * 2 + k] = contract(grads[r, :], wq[...], 1, 1)
        for side in range(2):
            h_twin(s, xq, side).start()

    def add_twin(g):
        s, xq = part_of(g)
        for side in range(2):
            h_twin(s, xq, side).wait_recv()
        give[s, pair(xq)] = (mine[s, pair(xq), :, lanes(other, c)] + r1[s, other, pair(xq)]).astype(BF16)
        h_across(s, xq).start()
        for k in range(2):
            r = rows(below(s) if k == 0 else above(s), xq, k)
            n = xq * 2 + k
            hg[r, :] = mine[s, n, :, lanes(xl, c)] + r1[s, xl, n]

    def add_across(g):
        s, xq = part_of(g)
        h_across(s, xq).wait_recv()
        for k in range(2):
            r = rows(below(s) if k == 0 else above(s), xq, k)
            hg[r, :] = hg[r, :] + r2[s, xq * 2 + k].astype(F32)
            put_sum(s, xq, k).start()

    def span(body, lo, hi):
        def step(s, carry):
            body(s)
            return carry

        lax.fori_loop(lo, hi, step, 0)

    def normalise(zb):
        for n in range(4):
            values = vs[zb, n // 2, n % 2].astype(F32)
            mean = jnp.mean(values, axis=1, keepdims=True)
            centred = values - mean
            var = jnp.mean(centred * centred, axis=1, keepdims=True)
            size = values.shape[0]
            nf[n * size : (n + 1) * size, :] = centred * lax.rsqrt(var + 1e-05)
        r = pl.ds(pl.multiple_of(zb * layer_rows, 32), layer_rows)
        normed = nf[...]
        nrm[r, :] = normed.astype(BF16)
        nin[r, :] = (normed * gain[...] + bias[...]).astype(BF16)
        pre[...] = contract(nin[r, :], wis[...], 1, 0)
        for xq in range(2):
            for half in range(2):
                at = xq * own_hid + half * unit
                pre[:, at : at + unit] = pre[:, at : at + unit] + bis[xq, half : half + 1, :]
        hid[r, :] = gelu_parts(pre[...])[0].astype(BF16)
        slope[r, :] = gelu_parts(pre[:, lanes(xl, c)])[1]

    v_up, v_down = layers // 2, layers // 2 - 1

    def half_v(s, upward):
        size = vs.shape[4] // 2
        if upward:
            ref = vs.at[below(s), xl, c, :, pl.ds(0, size)]
            return remote(ref, ref, vh_s.at[0], vh_r.at[0], up)
        ref = vs.at[above(s), xl, c, :, pl.ds(size, size)]
        return remote(ref, ref, vh_s.at[1], vh_r.at[1], down)

    def serve_v(s):
        for d, upward in enumerate((True, False)):

            @pl.when(s <= v_down)
            def _():
                ring_v(s, upward)(s - 1).wait_recv()

                @pl.when(s < v_down)
                def _():
                    ring_v(s, upward)(s).start()

                @pl.when(s == v_down)
                def _():
                    half_v(s, upward).start()

                v_across(s, d, xl).start()
                v_twin(s, d, xl, 0, c).start()

        @pl.when(s == v_up)
        def _():
            half_v(s, True).wait_recv()
            half_v(s, False).wait_recv()
            v_across(s, 0, xl).start()
            v_twin(s, 0, xl, 0, c).start()

        @pl.when((s >= 2) & (s - 2 <= v_up))
        def _():
            v_across(s - 2, 0, other).wait_recv()
            v_twin(s - 2, 0, other, 1, c).start()

        @pl.when((s >= 3) & (s - 2 <= v_down))
        def _():
            v_across(s - 2, 1, other).wait_recv()
            v_twin(s - 2, 1, other, 1, c).start()

    def serve_p(s, t):
        for u in range(SUB):
            for upward in (True, False):
                ring_p(s, t, upward, u)(s - 1).wait_recv()

                @pl.when(s < layers - 1)
                def _():
                    ring_p(s, t, upward, u)(s).start()

        for upward in (True, False):
            put_chunk(s, t, upward).start()

    def use_v(s):
        @pl.when(s <= v_up)
        def _():
            v_twin(s, 0, xl, 0, peer).wait_recv()
            v_twin(s, 0, other, 1, peer).wait_recv()
            normalise(below(s))
            for n in range(4):
                put_layer(s, 0, n).start()

        @pl.when((s >= 1) & (s <= v_down))
        def _():
            v_twin(s, 1, xl, 0, peer).wait_recv()
            v_twin(s, 1, other, 1, peer).wait_recv()
            normalise(above(s))
            for n in range(4):
                put_layer(s, 1, n).start()

    def count(s):
        return jnp.maximum(jnp.minimum(4 * s - 8, 2 * s + 1), 0)

    def step(s, carry):
        serve_v(s)
        serve_p(s, 0)

        @pl.when(s == 2)
        def _():
            w_swap(1, other).wait_recv()
            w_twin(1, c).start()

        @pl.when(s == 3)
        def _():
            w_swap(0, other).wait_recv()
            w_swap(2, other).wait_recv()
            for t in range(2):
                w_twin(t, peer).wait_recv()
            turned[...] = wis[:, lanes(xl, c)].astype(F32).T

        span(add_across, count(s - 4), count(s - 3))
        span(add_twin, count(s - 2), count(s - 1))
        span(multiply, count(s - 1), count(s))
        serve_p(s, 1)

        @pl.when(s >= 3)
        def _():
            use_v(s - 3)

        return carry

    lax.fori_loop(1, layers, step, 0)
    last_g = 2 * layers
    served = min(4 * (layers - 4) - 8, 2 * (layers - 4) + 1)
    begun = min(4 * (layers - 2) - 8, 2 * (layers - 2) + 1)
    span(multiply, last_g - 1, last_g)
    span(add_twin, begun, last_g - 1)
    span(add_across, served, last_g - 4)
    span(add_twin, last_g - 1, last_g)
    span(add_across, last_g - 4, last_g)

    for u in range(SUB):
        for k in range(2):
            p_swap(u, k, xl).wait_send()
    for n in range(3):
        w_swap(n, xl).wait_send()
    for t in range(2):
        w_twin(t, c).wait_send()

    def sent_p(s, carry):
        for t in range(2):
            for upward in (True, False):
                for u in range(SUB):
                    ring_p(s, t, upward, u)(s).wait_send()
        return carry

    lax.fori_loop(0, layers - 1, sent_p, 0)

    def put_done(s, carry):
        for t in range(2):
            for k in range(2):
                put_chunk(s, t, k == 0).wait()
                put_sum(s, t, k).wait()
        return carry

    lax.fori_loop(0, layers, put_done, 0)
    def sent_h(s):
        for xq in range(2):
            for side in range(2):
                h_twin(s, xq, side).wait_send()
            h_across(s, xq).wait_send()

    span(sent_h, 0, layers)
    for upward in (True, False):
        for s in range(v_down):
            ring_v(s, upward)(s).wait_send()
        half_v(v_down, upward).wait_send()
    for s in range(v_up + 1):
        for d in range(2):
            if d == 0 or 1 <= s <= v_down:
                for n in range(4):
                    put_layer(s, d, n).wait()
                v_across(s, d, xl).wait_send()
                v_twin(s, d, xl, 0, c).wait_send()
                v_twin(s, d, other, 1, c).wait_send()


def main(counts, token_pos, v, wo, wi, bi, lm, gain, bias, layers):
    rows, width = lm.shape
    quarter = width // 2
    own = wo.shape[0]
    unit = own // 2
    hid = 2 * own
    tokens = token_pos.shape[1]
    features = v.shape[1]
    layer_rows = 4 * v.shape[0]
    chunk = rows // 2
    places = layers * 2 * rows
    shapes = [
        ((places, quarter), BF16),
        ((tokens, hid), BF16),
        ((tokens, unit), F32),
        ((tokens, features), BF16),
        ((tokens, features), BF16),
        ((places, unit), F32),
    ]
    outs = [jax.ShapeDtypeStruct(*shape) for shape in shapes]
    outs += [jax.ShapeDtypeStruct((unit, features), F32), jax.ShapeDtypeStruct((width // 128, 128), F32)]
    scratch = [
        pltpu.VMEM((places, quarter), BF16),
        pltpu.VMEM((layers, 2, 2, *v.shape), BF16),
        pltpu.VMEM((hid, quarter), BF16),
        pltpu.VMEM((features, hid), BF16),
        pltpu.VMEM((2, *bi.shape), F32),
        pltpu.VMEM((layers, 4, chunk, hid), F32),
        pltpu.VMEM((layers, 2, 4, chunk, unit), F32),
        pltpu.VMEM((layers, 4, chunk, unit), BF16),
        pltpu.VMEM((layers, 4, chunk, unit), BF16),
        pltpu.VMEM((places, unit), F32),
        pltpu.VMEM((tokens, features), BF16),
        pltpu.VMEM((tokens, features), BF16),
        pltpu.VMEM((tokens, hid), BF16),
        pltpu.VMEM((tokens, unit), F32),
        pltpu.VMEM((layer_rows, hid), F32),
        pltpu.VMEM((layer_rows, features), F32),
        pltpu.VMEM((rows, width), BF16),
    ]
    half = layers // 2
    sems = [(half - 1,), (half - 1,), (2,), (2, half + 1), (2, 2, half + 1), (layers - 1, 2, SUB), (layers - 1, 2, SUB), (SUB, 2), (3,), (2,)]
    sems += [(layers, 2, 2), (layers, 2)]
    for shape in sems:
        scratch += [DMA(shape), DMA(shape)]
    scratch += [DMA((7,)), DMA((layers, 2, 2)), DMA((half + 1, 2, 4)), DMA((layers, 2, 2))]
    specs = [SMEM] * 2 + [ANY] * 5 + [VMEM] * 2, [ANY] * 6 + [VMEM] * 2
    return call(main_kernel, outs, scratch, 0, (counts, token_pos, v, wo, wi, bi, lm, gain, bias), 1 << 34, specs)


def product_kernel(
    counts, token_pos, grads, hid, slope, hg,
    w_out_part, pgs, b_in,
    pw, hv, hw, sv, left, got, got_p, got_h,
):
    starts = image_starts(counts, token_pos)
    size = PATCH + 8
    places = grads.shape[0]
    windows, sums, bases, lows = [], [], [], []
    for i, start in enumerate(starts):
        base = jnp.minimum((start // 16) * 16, places - WINDOW)
        low = jnp.minimum((start // 8) * 8, places - size)
        bases.append(base)
        lows.append(low)
        windows.append(
            pltpu.make_async_copy(
                grads.at[pl.ds(pl.multiple_of(base, 16), WINDOW)], pw.at[pl.ds(i * WINDOW, WINDOW)], got_p.at[i]
            )
        )
        sums.append(pltpu.make_async_copy(hg.at[pl.ds(pl.multiple_of(low, 8), size)], hw.at[i], got_h.at[i]))
    hidden = []
    for i in range(len(starts)):
        r = pl.ds(i * PATCH, PATCH)
        hidden.append(pltpu.make_async_copy(hid.at[r], hv.at[r], got.at[i]))
    slopes = pltpu.make_async_copy(slope, sv, got.at[len(starts)])
    for copy in hidden + windows + [slopes] + sums:
        copy.start()
    shape = (WINDOW, PATCH)
    offset = lax.broadcasted_iota(jnp.int32, shape, 0) - lax.broadcasted_iota(jnp.int32, shape, 1)
    for i, start in enumerate(starts):
        place = jnp.where(offset == start - bases[i], 1.0, 0.0).astype(BF16)
        hidden[i].wait()
        moved = contract(place, hv[i * PATCH : (i + 1) * PATCH, :], 1, 0)
        left[i * WINDOW : (i + 1) * WINDOW, :] = moved.astype(BF16)
    for copy in windows:
        copy.wait()
    w_out_part[...] = contract(left[...], pw[...], 0, 0).astype(BF16)
    unit = sv.shape[1]
    total = jnp.zeros((1, unit), F32)
    slopes.wait()
    for i, start in enumerate(starts):
        r = slice(i * PATCH, (i + 1) * PATCH)
        sums[i].wait()
        back = jnp.where(start == lows[i], 0, size - (start - lows[i]))
        window = pltpu.roll(hw[i], back, 0)[0:PATCH]
        pg = (window * sv[r, :]).astype(BF16)
        pgs[r, :] = pg
        total = total + jnp.sum(pg.astype(F32), axis=0, keepdims=True)
    b_in[...] = total


def products(counts, token_pos, grads, hid, slope, hg):
    images = token_pos.shape[1] // PATCH
    unit, quarter = hg.shape[1], grads.shape[1]
    width = hid.shape[1]
    outs = (
        jax.ShapeDtypeStruct((width, quarter), BF16),
        jax.ShapeDtypeStruct(slope.shape, BF16),
        jax.ShapeDtypeStruct((1, unit), F32),
    )
    scratch = [
        pltpu.VMEM((images * WINDOW, quarter), BF16),
        pltpu.VMEM(hid.shape, BF16),
        pltpu.VMEM((images, PATCH + 8, unit), F32),
        pltpu.VMEM(slope.shape, F32),
        pltpu.VMEM((images * WINDOW, width), BF16),
        DMA((images + 1,)),
        DMA((images,)),
        DMA((images,)),
    ]
    specs = [SMEM] * 2 + [ANY] * 4, [VMEM] * 3
    return call(product_kernel, outs, scratch, None, (counts, token_pos, grads, hid, slope, hg), 1 << 34, specs)


def last_kernel(
    wo_all, pgs_all, turned_all, b_out_part, b_in_part, nrm, nin,
    w_out, w_in, gain, bias, b_out, b_in,
    wo, pgs, turned, nv, rv, wi, vec, got, ry1, s1, rx1, rx2, s2, ry2, ri, v1, vo, t1, v2, t2, v3,
    y1_s, y1_r, x1_s, x1_r, x2_s, x2_r, y2_s, y2_r, i_s, i_r, a_s, a_r, o_s, o_r, b_s, b_r, d_s, d_r,
):
    layers, ny = v1.shape[0], wo.shape[1]
    z, xl, c = lax.axis_index("seq_0"), lax.axis_index("seq_1"), lax.axis_index("fsdp")
    y, xh = lax.axis_index("img_0"), lax.axis_index("img_1")

    def flip(me, bit):
        return 1 - me if bit else me

    plane = []
    for dy in range(ny):
        for dx in range(2):
            for dc in range(2):
                if (dy, dx, dc) != (0, 0, 0):
                    plane.append((dy, dx, dc))
    plane_ids = [((y + dy) % ny, flip(xh, dx), flip(c, dc)) for dy, dx, dc in plane]
    plane_dev = [{"img_0": a, "img_1": b, "fsdp": d} for a, b, d in plane_ids]
    side_dev = [{"seq_1": 1 - xl}, {"seq_1": 1 - xl, "img_1": 1 - xh}]
    corner = {"seq_1": 1 - xl, "fsdp": 1 - c}
    stack = [{"seq_0": (z + k) % layers} for k in range(1, layers)]
    signal(plane_dev + side_dev + [corner] + stack)
    pairs = ((wo_all, wo), (pgs_all, pgs), (nrm, nv), (turned_all, turned), (nin, rv))
    loads = [pltpu.make_async_copy(source, target, got.at[n]) for n, (source, target) in enumerate(pairs)]
    for copy in loads:
        copy.start()
    ys = [{"img_0": (y + k) % ny} for k in range(1, ny)]
    started = []

    def go(copy):
        copy.start()
        started.append(copy)
        return copy

    vec[16:17, :] = b_in_part[...]
    vec[17:24, :] = jnp.zeros((7, 128), F32)
    loads[0].wait()
    pl.semaphore_wait(pltpu.get_barrier_semaphore(), len(plane_dev) + 3 + len(stack))
    stage_o = []
    for k in range(1, layers):
        stage_o.append(go(remote(b_out_part, vo.at[z], o_s.at[k - 1], o_r.at[k - 1], stack[k - 1])))
    vo[z] = b_out_part[...]
    half = ry1.shape[4]
    left, right = pl.ds(0, half), pl.ds(half, half)
    across = [(1 - xl, xh), (1 - xl, 1 - xh), (xl, 1 - xh)]
    across_dev = side_dev + [{"img_1": 1 - xh}]
    x_first, y_first = [], []
    for m, (p, h) in enumerate(across):
        x_first.append(go(remote(wo.at[p, :, h, :, right], rx2.at[m], x2_s.at[m], x2_r.at[m], across_dev[m])))
    for k in range(ny - 1):
        source = wo.at[:, (y + k + 1) % ny, :, :, left]
        y_first.append(go(remote(source, ry1.at[k], y1_s.at[k], y1_r.at[k], ys[k])))
    for copy in loads[1:4]:
        copy.wait()
    moment = contract(pgs[...], nv[...], 0, 0)
    column = contract(pgs[...], jnp.ones((pgs.shape[0], 128), BF16), 0, 0)
    for j in range(nv.shape[1] // 128):
        at = slice(j * 128, (j + 1) * 128)
        vec[j : j + 1, :] = jnp.sum(moment[:, at] * turned[:, at], axis=0, keepdims=True)
        vec[8 + j : 9 + j, :] = jnp.sum(column * turned[:, at], axis=0, keepdims=True)
    stage_a = []
    for k in range(1, layers):
        stage_a.append(go(remote(vec, v1.at[z], a_s.at[k - 1], a_r.at[k - 1], stack[k - 1])))
    v1[z] = vec[...]
    loads[4].wait()
    wi[...] = contract(pgs[...], rv[...], 0, 0).T.astype(BF16).reshape(wi.shape)
    ins = []
    for n, (dy, dx, dc) in enumerate(plane):
        a, b, d = plane_ids[n]
        ins.append((go(remote(wi.at[a, b, d], ri.at[n], i_s.at[n], i_r.at[n], plane_dev[n])), n, dc))

    for copy in stage_a:
        copy.wait_recv()
    for copy in stage_o:
        copy.wait_recv()
    total, spread = v1[0, 0:16], vo[0]
    for j in range(1, layers):
        total, spread = total + v1[j, 0:16], spread + vo[j]
    t1[0:16] = total
    t1[16:32] = spread
    for j in range(layers):
        t1[32 + j : 33 + j] = v1[j, 16:17]
    stage_b = []
    for n, (dy, dx, dc) in enumerate(plane):
        if dc == 0:
            k = len(stage_b)
            stage_b.append(go(remote(t1, v2.at[k], b_s.at[k], b_r.at[k], plane_dev[n])))

    summed = wo[:, y, :, :, 0:half].astype(F32)
    for k, copy in enumerate(y_first):
        copy.wait_recv()
        summed = summed + ry1[k].astype(F32)
    s1[...] = summed.astype(BF16)
    x_second = []
    for m, (p, h) in enumerate(across):
        x_second.append(go(remote(s1.at[p, h], rx1.at[m], x1_s.at[m], x1_r.at[m], across_dev[m])))
    for copy in x_first:
        copy.wait_recv()
    s2[0] = (wo[xl, :, xh, :, half:].astype(F32) + rx2[2].astype(F32)).astype(BF16)
    s2[1] = (rx2[0].astype(F32) + rx2[1].astype(F32)).astype(BF16)
    y_second = []
    for k in range(ny - 1):
        y_second.append(
            go(remote(s2.at[:, (y + k + 1) % ny], ry2.at[k], y2_s.at[k], y2_r.at[k], ys[k]))
        )

    total = t1[...]
    for k, copy in enumerate(stage_b):
        copy.wait_recv()
        total = total + v2[k]
    t2[...] = total
    q = xl * 2 + c
    stage_d = []
    for k, (dx, dc) in enumerate(((0, 1), (1, 0), (1, 1))):
        device = {"seq_1": flip(xl, dx), "fsdp": flip(c, dc)}
        stage_d.append(go(remote(t2, v3.at[q], d_s.at[k], d_r.at[k], device)))
    v3[q] = total

    same = wi[y, xh, c].astype(F32)
    cross = jnp.zeros_like(same)
    for copy, n, dc in ins:
        copy.wait_recv()
        if dc:
            cross = cross + ri[n].astype(F32)
        else:
            same = same + ri[n].astype(F32)
    width = same.shape[1]
    w_in[:, pl.ds(pl.multiple_of(c * width, 128), width)] = same
    w_in[:, pl.ds(pl.multiple_of((1 - c) * width, 128), width)] = cross
    for copy in x_second:
        copy.wait_recv()
    near = s1[xl, xh].astype(F32) + rx1[2].astype(F32)
    far = rx1[0].astype(F32) + rx1[1].astype(F32)
    near_at = pl.multiple_of(2 * half * xl, 128)
    far_at = pl.multiple_of(2 * half * (1 - xl), 128)
    w_out[:, pl.ds(near_at, half)] = near
    w_out[:, pl.ds(far_at, half)] = far
    near, far = s2[0, y].astype(F32), s2[1, y].astype(F32)
    for k, copy in enumerate(y_second):
        copy.wait_recv()
        near = near + ry2[k, 0].astype(F32)
        far = far + ry2[k, 1].astype(F32)
    w_out[:, pl.ds(near_at + half, half)] = near
    w_out[:, pl.ds(far_at + half, half)] = far

    for copy in stage_d:
        copy.wait_recv()
    total = v3[0, 0:16] + v3[1, 0:16] + v3[2, 0:16] + v3[3, 0:16]
    gain[...] = total[0:8]
    bias[...] = total[8:16]
    b_out[0:16, :] = v3[0, 16:32] + v3[2, 16:32]
    b_out[16:32, :] = v3[1, 16:32] + v3[3, 16:32]
    for j in range(layers):
        for n in range(4):
            b_in[4 * j + n : 4 * j + n + 1, :] = v3[n, 32 + j : 33 + j]
    for copy in started:
        copy.wait_send()


def last(wo, pgs, turned, b_out, b_in, nrm, nin, layers):
    ny = wo.shape[1]
    members = ny * 4 - 1
    features, unit = nrm.shape[1], pgs.shape[1]
    block = (features // (ny * 4), unit)
    rows, half = wo.shape[3], wo.shape[4] // 2
    outs = (
        jax.ShapeDtypeStruct((rows, 4 * half), F32),
        jax.ShapeDtypeStruct((block[0], 2 * block[1]), F32),
        jax.ShapeDtypeStruct((8, 128), F32),
        jax.ShapeDtypeStruct((8, 128), F32),
        jax.ShapeDtypeStruct((32, 128), F32),
        jax.ShapeDtypeStruct((4 * layers, 128), F32),
    )
    scratch = [
        pltpu.VMEM(wo.shape, BF16),
        pltpu.VMEM(pgs.shape, BF16),
        pltpu.VMEM(turned.shape, F32),
        pltpu.VMEM(nrm.shape, BF16),
        pltpu.VMEM(nin.shape, BF16),
        pltpu.VMEM((ny, 2, 2, *block), BF16),
        pltpu.VMEM((24, 128), F32),
        DMA((5,)),
        pltpu.VMEM((ny - 1, 2, 2, rows, half), BF16),
        pltpu.VMEM((2, 2, rows, half), BF16),
        pltpu.VMEM((3, rows, half), BF16),
        pltpu.VMEM((3, ny, rows, half), BF16),
        pltpu.VMEM((2, ny, rows, half), BF16),
        pltpu.VMEM((ny - 1, 2, rows, half), BF16),
        pltpu.VMEM((members, *block), BF16),
        pltpu.VMEM((layers, 24, 128), F32),
        pltpu.VMEM((layers, 16, 128), F32),
        pltpu.VMEM((40, 128), F32),
        pltpu.VMEM((2 * ny - 1, 40, 128), F32),
        pltpu.VMEM((40, 128), F32),
        pltpu.VMEM((4, 40, 128), F32),
    ]
    for n in (ny - 1, 3, 3, ny - 1, members, layers - 1, layers - 1, 2 * ny - 1, 3):
        scratch += [DMA((n,)), DMA((n,))]
    specs = [ANY] * 3 + [VMEM] * 2 + [ANY] * 2, [VMEM] * 6
    return call(last_kernel, outs, scratch, 1, (wo, pgs, turned, b_out, b_in, nrm, nin), 1 << 32, specs)


def copy_kernel(*refs):
    count = len(refs) // 2
    for source, target in zip(refs[:count], refs[count:]):
        target[...] = source[...]


def result_of(arrays):
    outs = [jax.ShapeDtypeStruct(a.shape, a.dtype) for a in arrays]
    return call(copy_kernel, outs, [], None, arrays, 1 << 20)


def per_device(vision_feats, ln_gain, ln_bias, w_in, b_in, w_out, lm_grad, image_counts, token_pos):
    layers, ny = lax.axis_size("seq_0"), lax.axis_size("img_0")
    grads, hid, slope, nrm, nin, hg, turned, b_out_part = main(
        image_counts,
        token_pos,
        vision_feats[0],
        w_out,
        w_in,
        b_in.reshape(2, -1),
        lm_grad[0],
        ln_gain[None],
        ln_bias[None],
        layers,
    )
    w_out_part, pgs, b_in_part = products(image_counts, token_pos, grads, hid, slope, hg)
    quarter = w_out_part.shape[1]
    w_out_part = w_out_part.reshape(2, ny, 2, -1, quarter)
    sums = last(w_out_part, pgs, turned, b_out_part, b_in_part, nrm, nin, layers)
    w_out_grad, w_in_grad, gain, bias, b_out, b_in_grad = result_of(sums)
    return (w_in_grad, b_in_grad.reshape(-1), w_out_grad, b_out.reshape(-1), gain.reshape(-1), bias.reshape(-1))


def solution(mesh):
    finer = Mesh(
        mesh.devices.reshape(8, 2, 4, 2, mesh.shape["fsdp"]),
        ("seq_0", "seq_1", "img_0", "img_1", "fsdp"),
    )
    placed = (
        P(IMG, SEQ_FSDP, None),
        P(),
        P(),
        P("fsdp", SEQ),
        P(SEQ),
        P(SEQ, "fsdp"),
        P(IMG, SEQ, "fsdp"),
        P(IMG, None),
        P(IMG, None),
    )
    return jax.shard_map(
        per_device,
        mesh=finer,
        in_specs=placed,
        out_specs=(P(IMG_FSDP, SEQ), P(), P(SEQ_IMG, "fsdp"), P(), P(), P()),
        check_vma=False,
    )
```

```python
import jax
import jax.numpy as jnp
from jax import lax
from jax.experimental import pallas as pl
from jax.experimental.pallas import tpu as pltpu
from jax.sharding import Mesh
from jax.sharding import PartitionSpec as P

PATCH = 576
LEN = 2048
SEQ = ("seq_0", "seq_1")
IMG = ("img_0", "img_1")
SEQ_FSDP = ("seq_0", "seq_1", "fsdp")
IMG_FSDP = ("img_0", "img_1", "fsdp")
SEQ_IMG = ("seq_0", "seq_1", "img_0", "img_1")
MESH = pl.DeviceIdType.MESH
BF16 = jnp.bfloat16
F32 = jnp.float32
VMEM = pl.BlockSpec(memory_space=pltpu.VMEM)
SMEM = pl.BlockSpec(memory_space=pltpu.SMEM)
ANY = pl.BlockSpec(memory_space=pl.ANY)
DMA = pltpu.SemaphoreType.DMA
LIMIT = 63 * 1024 * 1024
WINDOW = 640
SUB = 2


def remote(src, dst, send, recv, device):
    return pltpu.make_async_remote_copy(
        src_ref=src, dst_ref=dst, send_sem=send, recv_sem=recv, device_id=device, device_id_type=MESH
    )


def signal(devices):
    barrier = pltpu.get_barrier_semaphore()
    for device in devices:
        pl.semaphore_signal(barrier, inc=1, device_id=device, device_id_type=MESH)


def greet(devices):
    signal(devices)
    pl.semaphore_wait(pltpu.get_barrier_semaphore(), len(devices))


def call(kernel, outs, scratch, number, args, flops, specs=None):
    ins, results = specs or ([VMEM] * len(args), [VMEM] * len(outs))
    return pl.pallas_call(
        kernel,
        out_shape=tuple(outs),
        in_specs=ins,
        out_specs=tuple(results),
        scratch_shapes=scratch,
        compiler_params=pltpu.CompilerParams(
            collective_id=number, has_side_effects=number is not None, vmem_limit_bytes=LIMIT
        ),
        cost_estimate=pl.CostEstimate(flops=flops, bytes_accessed=1 << 20, transcendentals=0),
    )(*args)


def gelu_parts(preact):
    cumul = 0.5 * (1.0 + lax.erf(preact * 0.7071067811865476))
    density = jnp.exp(-0.5 * preact * preact) * 0.3989422804014327
    return (preact * cumul, cumul + preact * density)


def contract(left, right, left_dim, right_dim):
    return lax.dot_general(left, right, (((left_dim,), (right_dim,)), ((), ())), preferred_element_type=F32)


def image_starts(counts, token_pos):
    images = token_pos.shape[1] // PATCH
    return [jnp.where(counts[0, 0] <= i, LEN, 0) + token_pos[0, i * PATCH] for i in range(images)]


def main_kernel(
    counts, token_pos, v, wo, wi, bi, lm, gain, bias,
    grads_out, hid_out, slope_out, nrm_out, nin_out, hg_out, turned, b_out,
    grads, vs, wq, wis, bis, mine, r1, give, r2, hg, nrm, nin, hid, slope, pre, nf, held,
    vu_s, vu_r, vd_s, vd_r, vh_s, vh_r, vx_s, vx_r, vc_s, vc_r,
    pu_s, pu_r, pd_s, pd_r, px_s, px_r, wx_s, wx_r, wc_s, wc_r,
    h1_s, h1_r, h2_s, h2_r, local, put_p, put_v, put_h,
):
    layers = vs.shape[0]
    block_rows = lm.shape[0]
    chunk = block_rows // 2
    quarter = grads.shape[1]
    own_hid = wo.shape[0]
    unit = own_hid // 2
    layer_rows = 4 * v.shape[0]
    z, xl, c = lax.axis_index("seq_0"), lax.axis_index("seq_1"), lax.axis_index("fsdp")
    other, peer = 1 - xl, 1 - c
    up, down = {"seq_0": (z + 1) % layers}, {"seq_0": (z + layers - 1) % layers}
    across, twin = {"seq_1": other}, {"fsdp": peer}
    mine_cols = pl.ds(pl.multiple_of(xl * quarter, 128), quarter)
    their_cols = pl.ds(pl.multiple_of(other * quarter, 128), quarter)

    def below(s):
        return (z + layers - s) % layers

    def above(s):
        return (z + s) % layers

    def rows(zb, xq, k):
        return pl.ds(pl.multiple_of((zb * 2 + xq) * block_rows + k * chunk, 128), chunk)

    def ring_p(s, t, upward, u):
        xq = xl if t == 0 else other
        size = chunk // SUB
        zb, k = (below(s), 0) if upward else (above(s), 1)
        r = pl.ds(pl.multiple_of((zb * 2 + xq) * block_rows + k * chunk + u * size, 16), size)
        if upward:
            return lambda n: remote(grads.at[r], grads.at[r], pu_s.at[n, t, u], pu_r.at[n, t, u], up)
        return lambda n: remote(grads.at[r], grads.at[r], pd_s.at[n, t, u], pd_r.at[n, t, u], down)

    def ring_v(s, upward):
        zb = below(s) if upward else above(s)
        ref = vs.at[zb, xl, c]
        if upward:
            return lambda n: remote(ref, ref, vu_s.at[n], vu_r.at[n], up)
        return lambda n: remote(ref, ref, vd_s.at[n], vd_r.at[n], down)

    def v_across(s, d, xq):
        ref = vs.at[below(s) if d == 0 else above(s), xq, c]
        return remote(ref, ref, vx_s.at[d, s], vx_r.at[d, s], across)

    def v_twin(s, d, xq, t, cq):
        ref = vs.at[below(s) if d == 0 else above(s), xq, cq]
        return remote(ref, ref, vc_s.at[t, d, s], vc_r.at[t, d, s], twin)

    def p_swap(u, k, xq):
        size = chunk // SUB
        r = pl.ds(pl.multiple_of((z * 2 + xq) * block_rows + k * chunk + u * size, 16), size)
        source = lm.at[pl.ds(k * chunk + u * size, size), their_cols]
        return remote(source, grads.at[r], px_s.at[u, k], px_r.at[u, k], across)

    def w_in_at(cq, xq):
        size = wi.shape[0]
        return wis.at[pl.ds(pl.multiple_of(cq * size, 128), size), pl.ds(pl.multiple_of(xq * own_hid, 128), own_hid)]

    def w_out_at(xq):
        return wq.at[pl.ds(pl.multiple_of(xq * own_hid, 128), own_hid)]

    def w_swap(n, xq):
        source = (wo.at[:, their_cols], wi, bi)[n]
        target = (w_out_at(xq), w_in_at(c, xq), bis.at[xq])[n]
        return remote(source, target, wx_s.at[n], wx_r.at[n], across)

    def w_twin(t, cq):
        ref = w_in_at(cq, xl if t == 0 else other)
        return remote(ref, ref, wc_s.at[t], wc_r.at[t], twin)

    def lanes(xq, cq):
        return pl.ds(pl.multiple_of((xq * 2 + cq) * unit, 128), unit)

    def pair(xq):
        return pl.ds(2 * xq, 2)

    def h_twin(s, xq, side):
        source = mine.at[s, pair(xq), :, lanes(side, peer)]
        return remote(source, r1.at[s, side, pair(xq)], h1_s.at[s, xq, side], h1_r.at[s, xq, side], twin)

    def h_across(s, xq):
        return remote(give.at[s, pair(xq)], r2.at[s, pair(xq)], h2_s.at[s, xq], h2_r.at[s, xq], across)

    signal([up, down, across, twin])
    locals_ = [
        pltpu.make_async_copy(v, vs.at[z, xl, c], local.at[2]),
        pltpu.make_async_copy(lm.at[pl.ds(0, chunk), mine_cols], grads.at[rows(z, xl, 0)], local.at[0]),
        pltpu.make_async_copy(lm.at[pl.ds(chunk, chunk), mine_cols], grads.at[rows(z, xl, 1)], local.at[1]),
        pltpu.make_async_copy(wi, w_in_at(c, xl), local.at[4]),
        pltpu.make_async_copy(wo.at[:, mine_cols], w_out_at(xl), local.at[3]),
        pltpu.make_async_copy(bi, bis.at[xl], local.at[5]),
        pltpu.make_async_copy(lm, held, local.at[6]),
    ]
    for copy in locals_:
        copy.start()
    pl.semaphore_wait(pltpu.get_barrier_semaphore(), 4)
    for u in range(SUB):
        for k in range(2):
            p_swap(u, k, xl).start()
    locals_[0].wait()
    ring_v(0, True)(0).start()
    ring_v(0, False)(0).start()
    for copy in locals_[1:3]:
        copy.wait()
    for u in range(SUB):
        ring_p(0, 0, True, u)(0).start()
        ring_p(0, 0, False, u)(0).start()
    v_across(0, 0, xl).start()
    for n in (1, 2, 0):
        w_swap(n, xl).start()
    v_twin(0, 0, xl, 0, c).start()
    for copy in locals_[3:6]:
        copy.wait()
    w_twin(0, c).start()

    def put_chunk(s, t, upward):
        r = rows(below(s) if upward else above(s), xl if t == 0 else other, 0 if upward else 1)
        return pltpu.make_async_copy(grads.at[r], grads_out.at[r], put_p.at[s, t, 0 if upward else 1])

    def put_layer(s, d, n):
        r = pl.ds(pl.multiple_of((below(s) if d == 0 else above(s)) * layer_rows, 32), layer_rows)
        source = (hid, slope, nrm, nin)[n]
        target = (hid_out, slope_out, nrm_out, nin_out)[n]
        return pltpu.make_async_copy(source.at[r], target.at[r], put_v.at[s, d, n])

    def put_sum(s, xq, k):
        r = rows(below(s) if k == 0 else above(s), xq, k)
        return pltpu.make_async_copy(hg.at[r], hg_out.at[r], put_h.at[s, xq, k])

    for u in range(SUB):
        p_swap(u, 0, other).wait_recv()
        ring_p(0, 1, True, u)(0).start()
        p_swap(u, 1, other).wait_recv()
        ring_p(0, 1, False, u)(0).start()
    for t in range(2):
        put_chunk(0, t, True).start()
        put_chunk(0, t, False).start()
    locals_[6].wait()
    starts = image_starts(counts, token_pos)
    here = (z * 2 + xl) * block_rows + lax.broadcasted_iota(jnp.int32, (block_rows, 1), 0)
    taken = jnp.zeros((block_rows, 1), F32)
    for start in starts:
        taken = taken + jnp.where((here >= start) & (here < start + PATCH), 1.0, 0.0)
    for j in range(lm.shape[1] // 128):
        column = held[:, j * 128 : (j + 1) * 128].astype(F32) * taken
        b_out[j : j + 1, :] = jnp.sum(column, axis=0, keepdims=True)
    def part_of(g):
        s, t = g // 2, g % 2
        return s, xl * (1 - t) + other * t

    def multiply(g):
        s, xq = part_of(g)
        for k in range(2):
            r = rows(below(s) if k == 0 else above(s), xq, k)
            mine[s, xq * 2 + k] = contract(grads[r, :], wq[...], 1, 1)
        for side in range(2):
            h_twin(s, xq, side).start()

    def add_twin(g):
        s, xq = part_of(g)
        for side in range(2):
            h_twin(s, xq, side).wait_recv()
        give[s, pair(xq)] = (mine[s, pair(xq), :, lanes(other, c)] + r1[s, other, pair(xq)]).astype(BF16)
        h_across(s, xq).start()
        for k in range(2):
            r = rows(below(s) if k == 0 else above(s), xq, k)
            n = xq * 2 + k
            hg[r, :] = mine[s, n, :, lanes(xl, c)] + r1[s, xl, n]

    def add_across(g):
        s, xq = part_of(g)
        h_across(s, xq).wait_recv()
        for k in range(2):
            r = rows(below(s) if k == 0 else above(s), xq, k)
            hg[r, :] = hg[r, :] + r2[s, xq * 2 + k].astype(F32)
            put_sum(s, xq, k).start()

    def span(body, lo, hi):
        def step(s, carry):
            body(s)
            return carry

        lax.fori_loop(lo, hi, step, 0)

    def normalise(zb):
        for n in range(4):
            values = vs[zb, n // 2, n % 2].astype(F32)
            mean = jnp.mean(values, axis=1, keepdims=True)
            centred = values - mean
            var = jnp.mean(centred * centred, axis=1, keepdims=True)
            size = values.shape[0]
            nf[n * size : (n + 1) * size, :] = centred * lax.rsqrt(var + 1e-05)
        r = pl.ds(pl.multiple_of(zb * layer_rows, 32), layer_rows)
        normed = nf[...]
        nrm[r, :] = normed.astype(BF16)
        nin[r, :] = (normed * gain[...] + bias[...]).astype(BF16)
        pre[...] = contract(nin[r, :], wis[...], 1, 0)
        for xq in range(2):
            for half in range(2):
                at = xq * own_hid + half * unit
                pre[:, at : at + unit] = pre[:, at : at + unit] + bis[xq, half : half + 1, :]
        hid[r, :] = gelu_parts(pre[...])[0].astype(BF16)
        slope[r, :] = gelu_parts(pre[:, lanes(xl, c)])[1]

    v_up, v_down = layers // 2, layers // 2 - 1

    def half_v(s, upward):
        size = vs.shape[4] // 2
        if upward:
            ref = vs.at[below(s), xl, c, :, pl.ds(0, size)]
            return remote(ref, ref, vh_s.at[0], vh_r.at[0], up)
        ref = vs.at[above(s), xl, c, :, pl.ds(size, size)]
        return remote(ref, ref, vh_s.at[1], vh_r.at[1], down)

    def serve_v(s):
        for d, upward in enumerate((True, False)):

            @pl.when(s <= v_down)
            def _():
                ring_v(s, upward)(s - 1).wait_recv()

                @pl.when(s < v_down)
                def _():
                    ring_v(s, upward)(s).start()

                @pl.when(s == v_down)
                def _():
                    half_v(s, upward).start()

                v_across(s, d, xl).start()
                v_twin(s, d, xl, 0, c).start()

        @pl.when(s == v_up)
        def _():
            half_v(s, True).wait_recv()
            half_v(s, False).wait_recv()
            v_across(s, 0, xl).start()
            v_twin(s, 0, xl, 0, c).start()

        @pl.when((s >= 2) & (s - 2 <= v_up))
        def _():
            v_across(s - 2, 0, other).wait_recv()
            v_twin(s - 2, 0, other, 1, c).start()

        @pl.when((s >= 3) & (s - 2 <= v_down))
        def _():
            v_across(s - 2, 1, other).wait_recv()
            v_twin(s - 2, 1, other, 1, c).start()

    def serve_p(s, t):
        for u in range(SUB):
            for upward in (True, False):
                ring_p(s, t, upward, u)(s - 1).wait_recv()

                @pl.when(s < layers - 1)
                def _():
                    ring_p(s, t, upward, u)(s).start()

        for upward in (True, False):
            put_chunk(s, t, upward).start()

    def use_v(s, d):
        layer = below(s) if d == 0 else above(s)
        wanted = s <= v_up if d == 0 else (s >= 1) & (s <= v_down)

        @pl.when(wanted)
        def _():
            v_twin(s, d, xl, 0, peer).wait_recv()
            v_twin(s, d, other, 1, peer).wait_recv()
            normalise(layer)
            for n in range(4):
                put_layer(s, d, n).start()

    def count(s):
        return jnp.maximum(jnp.minimum(4 * s - 8, 2 * s + 1), 0)

    def step(s, carry):
        serve_v(s)
        serve_p(s, 0)

        @pl.when(s == 2)
        def _():
            w_swap(1, other).wait_recv()
            w_twin(1, c).start()

        @pl.when(s == 3)
        def _():
            w_swap(0, other).wait_recv()
            w_swap(2, other).wait_recv()
            for t in range(2):
                w_twin(t, peer).wait_recv()
            turned[...] = wis[:, lanes(xl, c)].astype(F32).T

        span(add_across, count(s - 4), count(s - 3))
        span(add_twin, count(s - 2), count(s - 1))
        span(multiply, count(s - 1), count(s))

        @pl.when(s >= 3)
        def _():
            use_v(s - 3, 0)

        serve_p(s, 1)

        @pl.when(s >= 3)
        def _():
            use_v(s - 3, 1)

        return carry

    lax.fori_loop(1, layers, step, 0)
    last_g = 2 * layers
    served = min(4 * (layers - 4) - 8, 2 * (layers - 4) + 1)
    begun = min(4 * (layers - 2) - 8, 2 * (layers - 2) + 1)
    span(multiply, last_g - 1, last_g)
    span(add_twin, begun, last_g - 1)
    span(add_across, served, last_g - 4)
    span(add_twin, last_g - 1, last_g)
    span(add_across, last_g - 4, last_g)

    for u in range(SUB):
        for k in range(2):
            p_swap(u, k, xl).wait_send()
    for n in range(3):
        w_swap(n, xl).wait_send()
    for t in range(2):
        w_twin(t, c).wait_send()

    def sent_p(s, carry):
        for t in range(2):
            for upward in (True, False):
                for u in range(SUB):
                    ring_p(s, t, upward, u)(s).wait_send()
        return carry

    lax.fori_loop(0, layers - 1, sent_p, 0)

    def put_done(s, carry):
        for t in range(2):
            for k in range(2):
                put_chunk(s, t, k == 0).wait()
                put_sum(s, t, k).wait()
        return carry

    lax.fori_loop(0, layers, put_done, 0)
    def sent_h(s):
        for xq in range(2):
            for side in range(2):
                h_twin(s, xq, side).wait_send()
            h_across(s, xq).wait_send()

    span(sent_h, 0, layers)
    for upward in (True, False):
        for s in range(v_down):
            ring_v(s, upward)(s).wait_send()
        half_v(v_down, upward).wait_send()
    for s in range(v_up + 1):
        for d in range(2):
            if d == 0 or 1 <= s <= v_down:
                for n in range(4):
                    put_layer(s, d, n).wait()
                v_across(s, d, xl).wait_send()
                v_twin(s, d, xl, 0, c).wait_send()
                v_twin(s, d, other, 1, c).wait_send()


def main(counts, token_pos, v, wo, wi, bi, lm, gain, bias, layers):
    rows, width = lm.shape
    quarter = width // 2
    own = wo.shape[0]
    unit = own // 2
    hid = 2 * own
    tokens = token_pos.shape[1]
    features = v.shape[1]
    layer_rows = 4 * v.shape[0]
    chunk = rows // 2
    places = layers * 2 * rows
    shapes = [
        ((places, quarter), BF16),
        ((tokens, hid), BF16),
        ((tokens, unit), F32),
        ((tokens, features), BF16),
        ((tokens, features), BF16),
        ((places, unit), F32),
    ]
    outs = [jax.ShapeDtypeStruct(*shape) for shape in shapes]
    outs += [jax.ShapeDtypeStruct((unit, features), F32), jax.ShapeDtypeStruct((width // 128, 128), F32)]
    scratch = [
        pltpu.VMEM((places, quarter), BF16),
        pltpu.VMEM((layers, 2, 2, *v.shape), BF16),
        pltpu.VMEM((hid, quarter), BF16),
        pltpu.VMEM((features, hid), BF16),
        pltpu.VMEM((2, *bi.shape), F32),
        pltpu.VMEM((layers, 4, chunk, hid), F32),
        pltpu.VMEM((layers, 2, 4, chunk, unit), F32),
        pltpu.VMEM((layers, 4, chunk, unit), BF16),
        pltpu.VMEM((layers, 4, chunk, unit), BF16),
        pltpu.VMEM((places, unit), F32),
        pltpu.VMEM((tokens, features), BF16),
        pltpu.VMEM((tokens, features), BF16),
        pltpu.VMEM((tokens, hid), BF16),
        pltpu.VMEM((tokens, unit), F32),
        pltpu.VMEM((layer_rows, hid), F32),
        pltpu.VMEM((layer_rows, features), F32),
        pltpu.VMEM((rows, width), BF16),
    ]
    half = layers // 2
    sems = [(half - 1,), (half - 1,), (2,), (2, half + 1), (2, 2, half + 1), (layers - 1, 2, SUB), (layers - 1, 2, SUB), (SUB, 2), (3,), (2,)]
    sems += [(layers, 2, 2), (layers, 2)]
    for shape in sems:
        scratch += [DMA(shape), DMA(shape)]
    scratch += [DMA((7,)), DMA((layers, 2, 2)), DMA((half + 1, 2, 4)), DMA((layers, 2, 2))]
    specs = [SMEM] * 2 + [ANY] * 5 + [VMEM] * 2, [ANY] * 6 + [VMEM] * 2
    return call(main_kernel, outs, scratch, 0, (counts, token_pos, v, wo, wi, bi, lm, gain, bias), 1 << 34, specs)


def product_kernel(
    counts, token_pos, grads, hid, slope, hg,
    w_out_part, pgs, b_in,
    pw, hv, hw, sv, left, result, got, got_p, got_h,
):
    starts = image_starts(counts, token_pos)
    size = PATCH + 8
    places = grads.shape[0]
    windows, sums, bases, lows = [], [], [], []
    for i, start in enumerate(starts):
        base = jnp.minimum((start // 16) * 16, places - WINDOW)
        low = jnp.minimum((start // 8) * 8, places - size)
        bases.append(base)
        lows.append(low)
        windows.append(
            pltpu.make_async_copy(
                grads.at[pl.ds(pl.multiple_of(base, 16), WINDOW)], pw.at[pl.ds(i * WINDOW, WINDOW)], got_p.at[i]
            )
        )
        sums.append(pltpu.make_async_copy(hg.at[pl.ds(pl.multiple_of(low, 8), size)], hw.at[i], got_h.at[i]))
    hidden = []
    for i in range(len(starts)):
        r = pl.ds(i * PATCH, PATCH)
        hidden.append(pltpu.make_async_copy(hid.at[r], hv.at[r], got.at[i]))
    slopes = pltpu.make_async_copy(slope, sv, got.at[len(starts)])
    for copy in hidden + windows + [slopes] + sums:
        copy.start()
    shape = (WINDOW, PATCH)
    offset = lax.broadcasted_iota(jnp.int32, shape, 0) - lax.broadcasted_iota(jnp.int32, shape, 1)
    for i, start in enumerate(starts):
        place = jnp.where(offset == start - bases[i], 1.0, 0.0).astype(BF16)
        hidden[i].wait()
        moved = contract(place, hv[i * PATCH : (i + 1) * PATCH, :], 1, 0)
        left[i * WINDOW : (i + 1) * WINDOW, :] = moved.astype(BF16)
    for copy in windows:
        copy.wait()
    result[...] = contract(left[...], pw[...], 0, 0).astype(BF16)
    put = pltpu.make_async_copy(result, w_out_part, got.at[len(starts) + 1])
    put.start()
    unit = sv.shape[1]
    total = jnp.zeros((1, unit), F32)
    slopes.wait()
    for i, start in enumerate(starts):
        r = slice(i * PATCH, (i + 1) * PATCH)
        sums[i].wait()
        back = jnp.where(start == lows[i], 0, size - (start - lows[i]))
        window = pltpu.roll(hw[i], back, 0)[0:PATCH]
        pg = (window * sv[r, :]).astype(BF16)
        pgs[r, :] = pg
        total = total + jnp.sum(pg.astype(F32), axis=0, keepdims=True)
    b_in[...] = total
    put.wait()


def products(counts, token_pos, grads, hid, slope, hg):
    images = token_pos.shape[1] // PATCH
    unit, quarter = hg.shape[1], grads.shape[1]
    width = hid.shape[1]
    outs = (
        jax.ShapeDtypeStruct((width, quarter), BF16),
        jax.ShapeDtypeStruct(slope.shape, BF16),
        jax.ShapeDtypeStruct((1, unit), F32),
    )
    scratch = [
        pltpu.VMEM((images * WINDOW, quarter), BF16),
        pltpu.VMEM(hid.shape, BF16),
        pltpu.VMEM((images, PATCH + 8, unit), F32),
        pltpu.VMEM(slope.shape, F32),
        pltpu.VMEM((images * WINDOW, width), BF16),
        pltpu.VMEM((width, quarter), BF16),
        DMA((images + 2,)),
        DMA((images,)),
        DMA((images,)),
    ]
    specs = [SMEM] * 2 + [ANY] * 4, [ANY] + [VMEM] * 2
    return call(product_kernel, outs, scratch, None, (counts, token_pos, grads, hid, slope, hg), 1 << 34, specs)


def last_kernel(
    wo_all, pgs_all, turned_all, b_out_part, b_in_part, nrm, nin,
    w_out, w_in, gain, bias, b_out, b_in,
    wo, pgs, turned, nv, rv, wi, vec, got, ry1, s1, rx1, rx2, s2, ry2, ri, v1, vo, t1, v2, t2, v3,
    y1_s, y1_r, x1_s, x1_r, x2_s, x2_r, y2_s, y2_r, i_s, i_r, a_s, a_r, o_s, o_r, b_s, b_r, d_s, d_r,
):
    layers, ny = v1.shape[0], wo.shape[1]
    z, xl, c = lax.axis_index("seq_0"), lax.axis_index("seq_1"), lax.axis_index("fsdp")
    y, xh = lax.axis_index("img_0"), lax.axis_index("img_1")

    def flip(me, bit):
        return 1 - me if bit else me

    plane = []
    for dy in range(ny):
        for dx in range(2):
            for dc in range(2):
                if (dy, dx, dc) != (0, 0, 0):
                    plane.append((dy, dx, dc))
    plane_ids = [((y + dy) % ny, flip(xh, dx), flip(c, dc)) for dy, dx, dc in plane]
    plane_dev = [{"img_0": a, "img_1": b, "fsdp": d} for a, b, d in plane_ids]
    side_dev = [{"seq_1": 1 - xl}, {"seq_1": 1 - xl, "img_1": 1 - xh}]
    corner = {"seq_1": 1 - xl, "fsdp": 1 - c}
    stack = [{"seq_0": (z + k) % layers} for k in range(1, layers)]
    signal(plane_dev + side_dev + [corner] + stack)
    pairs = ((wo_all, wo), (pgs_all, pgs), (nrm, nv), (turned_all, turned), (nin, rv))
    loads = [pltpu.make_async_copy(source, target, got.at[n]) for n, (source, target) in enumerate(pairs)]
    for copy in loads:
        copy.start()
    ys = [{"img_0": (y + k) % ny} for k in range(1, ny)]
    started = []

    def go(copy):
        copy.start()
        started.append(copy)
        return copy

    vec[16:17, :] = b_in_part[...]
    vec[17:24, :] = jnp.zeros((7, 128), F32)
    loads[0].wait()
    pl.semaphore_wait(pltpu.get_barrier_semaphore(), len(plane_dev) + 3 + len(stack))
    stage_o = []
    for k in range(1, layers):
        stage_o.append(go(remote(b_out_part, vo.at[z], o_s.at[k - 1], o_r.at[k - 1], stack[k - 1])))
    vo[z] = b_out_part[...]
    half = ry1.shape[4]
    left, right = pl.ds(0, half), pl.ds(half, half)
    across = [(1 - xl, xh), (1 - xl, 1 - xh), (xl, 1 - xh)]
    across_dev = side_dev + [{"img_1": 1 - xh}]
    x_first, y_first = [], []
    for m, (p, h) in enumerate(across):
        x_first.append(go(remote(wo.at[p, :, h, :, right], rx2.at[m], x2_s.at[m], x2_r.at[m], across_dev[m])))
    for k in range(ny - 1):
        source = wo.at[:, (y + k + 1) % ny, :, :, left]
        y_first.append(go(remote(source, ry1.at[k], y1_s.at[k], y1_r.at[k], ys[k])))
    for copy in loads[1:4]:
        copy.wait()
    moment = contract(pgs[...], nv[...], 0, 0)
    column = contract(pgs[...], jnp.ones((pgs.shape[0], 128), BF16), 0, 0)
    for j in range(nv.shape[1] // 128):
        at = slice(j * 128, (j + 1) * 128)
        vec[j : j + 1, :] = jnp.sum(moment[:, at] * turned[:, at], axis=0, keepdims=True)
        vec[8 + j : 9 + j, :] = jnp.sum(column * turned[:, at], axis=0, keepdims=True)
    stage_a = []
    for k in range(1, layers):
        stage_a.append(go(remote(vec, v1.at[z], a_s.at[k - 1], a_r.at[k - 1], stack[k - 1])))
    v1[z] = vec[...]
    loads[4].wait()
    wi[...] = contract(pgs[...], rv[...], 0, 0).T.astype(BF16).reshape(wi.shape)
    ins = []
    for n, (dy, dx, dc) in enumerate(plane):
        a, b, d = plane_ids[n]
        ins.append((go(remote(wi.at[a, b, d], ri.at[n], i_s.at[n], i_r.at[n], plane_dev[n])), n, dc))

    for copy in stage_a:
        copy.wait_recv()
    for copy in stage_o:
        copy.wait_recv()
    total, spread = v1[0, 0:16], vo[0]
    for j in range(1, layers):
        total, spread = total + v1[j, 0:16], spread + vo[j]
    t1[0:16] = total
    t1[16:32] = spread
    for j in range(layers):
        t1[32 + j : 33 + j] = v1[j, 16:17]
    stage_b = []
    for n, (dy, dx, dc) in enumerate(plane):
        if dc == 0:
            k = len(stage_b)
            stage_b.append(go(remote(t1, v2.at[k], b_s.at[k], b_r.at[k], plane_dev[n])))

    summed = wo[:, y, :, :, 0:half].astype(F32)
    for k, copy in enumerate(y_first):
        copy.wait_recv()
        summed = summed + ry1[k].astype(F32)
    s1[...] = summed.astype(BF16)
    x_second = []
    for m, (p, h) in enumerate(across):
        x_second.append(go(remote(s1.at[p, h], rx1.at[m], x1_s.at[m], x1_r.at[m], across_dev[m])))
    for copy in x_first:
        copy.wait_recv()
    s2[0] = (wo[xl, :, xh, :, half:].astype(F32) + rx2[2].astype(F32)).astype(BF16)
    s2[1] = (rx2[0].astype(F32) + rx2[1].astype(F32)).astype(BF16)
    y_second = []
    for k in range(ny - 1):
        y_second.append(
            go(remote(s2.at[:, (y + k + 1) % ny], ry2.at[k], y2_s.at[k], y2_r.at[k], ys[k]))
        )

    total = t1[...]
    for k, copy in enumerate(stage_b):
        copy.wait_recv()
        total = total + v2[k]
    t2[...] = total
    q = xl * 2 + c
    stage_d = []
    for k, (dx, dc) in enumerate(((0, 1), (1, 0), (1, 1))):
        device = {"seq_1": flip(xl, dx), "fsdp": flip(c, dc)}
        stage_d.append(go(remote(t2, v3.at[q], d_s.at[k], d_r.at[k], device)))
    v3[q] = total

    same = wi[y, xh, c].astype(F32)
    cross = jnp.zeros_like(same)
    for copy, n, dc in ins:
        copy.wait_recv()
        if dc:
            cross = cross + ri[n].astype(F32)
        else:
            same = same + ri[n].astype(F32)
    width = same.shape[1]
    w_in[:, pl.ds(pl.multiple_of(c * width, 128), width)] = same
    w_in[:, pl.ds(pl.multiple_of((1 - c) * width, 128), width)] = cross
    for copy in x_second:
        copy.wait_recv()
    near = s1[xl, xh].astype(F32) + rx1[2].astype(F32)
    far = rx1[0].astype(F32) + rx1[1].astype(F32)
    near_at = pl.multiple_of(2 * half * xl, 128)
    far_at = pl.multiple_of(2 * half * (1 - xl), 128)
    w_out[:, pl.ds(near_at, half)] = near
    w_out[:, pl.ds(far_at, half)] = far
    near, far = s2[0, y].astype(F32), s2[1, y].astype(F32)
    for k, copy in enumerate(y_second):
        copy.wait_recv()
        near = near + ry2[k, 0].astype(F32)
        far = far + ry2[k, 1].astype(F32)
    w_out[:, pl.ds(near_at + half, half)] = near
    w_out[:, pl.ds(far_at + half, half)] = far

    for copy in stage_d:
        copy.wait_recv()
    total = v3[0, 0:16] + v3[1, 0:16] + v3[2, 0:16] + v3[3, 0:16]
    gain[...] = total[0:8]
    bias[...] = total[8:16]
    b_out[0:16, :] = v3[0, 16:32] + v3[2, 16:32]
    b_out[16:32, :] = v3[1, 16:32] + v3[3, 16:32]
    for j in range(layers):
        for n in range(4):
            b_in[4 * j + n : 4 * j + n + 1, :] = v3[n, 32 + j : 33 + j]
    for copy in started:
        copy.wait_send()


def last(wo, pgs, turned, b_out, b_in, nrm, nin, layers):
    ny = wo.shape[1]
    members = ny * 4 - 1
    features, unit = nrm.shape[1], pgs.shape[1]
    block = (features // (ny * 4), unit)
    rows, half = wo.shape[3], wo.shape[4] // 2
    outs = (
        jax.ShapeDtypeStruct((rows, 4 * half), F32),
        jax.ShapeDtypeStruct((block[0], 2 * block[1]), F32),
        jax.ShapeDtypeStruct((8, 128), F32),
        jax.ShapeDtypeStruct((8, 128), F32),
        jax.ShapeDtypeStruct((32, 128), F32),
        jax.ShapeDtypeStruct((4 * layers, 128), F32),
    )
    scratch = [
        pltpu.VMEM(wo.shape, BF16),
        pltpu.VMEM(pgs.shape, BF16),
        pltpu.VMEM(turned.shape, F32),
        pltpu.VMEM(nrm.shape, BF16),
        pltpu.VMEM(nin.shape, BF16),
        pltpu.VMEM((ny, 2, 2, *block), BF16),
        pltpu.VMEM((24, 128), F32),
        DMA((5,)),
        pltpu.VMEM((ny - 1, 2, 2, rows, half), BF16),
        pltpu.VMEM((2, 2, rows, half), BF16),
        pltpu.VMEM((3, rows, half), BF16),
        pltpu.VMEM((3, ny, rows, half), BF16),
        pltpu.VMEM((2, ny, rows, half), BF16),
        pltpu.VMEM((ny - 1, 2, rows, half), BF16),
        pltpu.VMEM((members, *block), BF16),
        pltpu.VMEM((layers, 24, 128), F32),
        pltpu.VMEM((layers, 16, 128), F32),
        pltpu.VMEM((40, 128), F32),
        pltpu.VMEM((2 * ny - 1, 40, 128), F32),
        pltpu.VMEM((40, 128), F32),
        pltpu.VMEM((4, 40, 128), F32),
    ]
    for n in (ny - 1, 3, 3, ny - 1, members, layers - 1, layers - 1, 2 * ny - 1, 3):
        scratch += [DMA((n,)), DMA((n,))]
    specs = [ANY] * 3 + [VMEM] * 2 + [ANY] * 2, [VMEM] * 6
    return call(last_kernel, outs, scratch, 1, (wo, pgs, turned, b_out, b_in, nrm, nin), 1 << 32, specs)


def copy_kernel(*refs):
    count = len(refs) // 2
    for source, target in zip(refs[:count], refs[count:]):
        target[...] = source[...]


def result_of(arrays):
    outs = [jax.ShapeDtypeStruct(a.shape, a.dtype) for a in arrays]
    return call(copy_kernel, outs, [], None, arrays, 1 << 20)


def per_device(vision_feats, ln_gain, ln_bias, w_in, b_in, w_out, lm_grad, image_counts, token_pos):
    layers, ny = lax.axis_size("seq_0"), lax.axis_size("img_0")
    grads, hid, slope, nrm, nin, hg, turned, b_out_part = main(
        image_counts,
        token_pos,
        vision_feats[0],
        w_out,
        w_in,
        b_in.reshape(2, -1),
        lm_grad[0],
        ln_gain[None],
        ln_bias[None],
        layers,
    )
    w_out_part, pgs, b_in_part = products(image_counts, token_pos, grads, hid, slope, hg)
    quarter = w_out_part.shape[1]
    w_out_part = w_out_part.reshape(2, ny, 2, -1, quarter)
    sums = last(w_out_part, pgs, turned, b_out_part, b_in_part, nrm, nin, layers)
    w_out_grad, w_in_grad, gain, bias, b_out, b_in_grad = result_of(sums)
    return (w_in_grad, b_in_grad.reshape(-1), w_out_grad, b_out.reshape(-1), gain.reshape(-1), bias.reshape(-1))


def solution(mesh):
    finer = Mesh(
        mesh.devices.reshape(8, 2, 4, 2, mesh.shape["fsdp"]),
        ("seq_0", "seq_1", "img_0", "img_1", "fsdp"),
    )
    placed = (
        P(IMG, SEQ_FSDP, None),
        P(),
        P(),
        P("fsdp", SEQ),
        P(SEQ),
        P(SEQ, "fsdp"),
        P(IMG, SEQ, "fsdp"),
        P(IMG, None),
        P(IMG, None),
    )
    return jax.shard_map(
        per_device,
        mesh=finer,
        in_specs=placed,
        out_specs=(P(IMG_FSDP, SEQ), P(), P(SEQ_IMG, "fsdp"), P(), P(), P()),
        check_vma=False,
    )
```
